8 devices in a mesh: heads: 1 (over z), cp_outer: 2 (over y), cp: 4 (over x, core).
Axes of the slice: x: 2, y: 2, z: 1, core: 2. Of those that a mesh axis runs over, the one named last changes fastest.
Arguments:
- q_segs: bfloat16 [32, 256, 24, 128], P(None, ('cp_outer', 'cp'), 'heads')
- k_prefix: bfloat16 [8448, 8, 128], P(('cp_outer', 'cp'), 'heads')
- v_prefix: bfloat16 [8448, 8, 128], P(('cp_outer', 'cp'), 'heads')
- o_segs: bfloat16 [32, 256, 24, 128], P(None, ('cp_outer', 'cp'), 'heads')
- do_segs: bfloat16 [32, 256, 24, 128], P(None, ('cp_outer', 'cp'), 'heads')
- lse_segs: float32 [32, 256, 24], P(None, ('cp_outer', 'cp'), 'heads')
Outputs:
- output 1: bfloat16 [32, 256, 24, 128], P(None, ('cp_outer', 'cp'), 'heads')
- output 2: float32 [8448, 8, 128], P(('cp_outer', 'cp'), 'heads')
- output 3: float32 [8448, 8, 128], P(('cp_outer', 'cp'), 'heads')
All inputs are finite; a program needn't handle non-finite values.
Results may differ from the reference program's by a relative error of at most 0.001.
Values are sent between devices in bfloat16 or wider.
A program may use at most 1 GiB of HBM per device.

```python
import jax
import jax.numpy as jnp
from jax import lax

SEGMENTS = 32
SEG_LEN = 256
PREFIX0 = 256
CP_BLOCKS = 8
Q_HEADS = 24
KV_HEADS = 8
HEAD_DIM = 128

GROUP = Q_HEADS // KV_HEADS
Q_ROWS = SEG_LEN // CP_BLOCKS
PREFIX_LEN = PREFIX0 + SEGMENTS * SEG_LEN
K_ROWS = PREFIX_LEN // CP_BLOCKS
SCALE = HEAD_DIM ** -0.5


def key_blocks(array_in):
    return array_in.reshape((CP_BLOCKS, K_ROWS) + array_in.shape[1:])


def query_blocks(array_in):
    return array_in.reshape((SEGMENTS * CP_BLOCKS, Q_ROWS) + array_in.shape[2:])


def heads_first(stat_rows):
    return jnp.transpose(stat_rows.reshape(Q_ROWS, KV_HEADS, GROUP), (1, 2, 0))[..., None]


def block_scores(q_four, k_rows, q_blk, k_blk):
    q_pos = PREFIX0 + q_blk * Q_ROWS + jnp.arange(Q_ROWS)
    k_pos = k_blk * K_ROWS + jnp.arange(K_ROWS)
    visible = q_pos[:, None] >= k_pos[None, :]
    scores = jnp.einsum("qhgd,khd->hgqk", q_four, k_rows.astype(jnp.float32)) * SCALE
    return jnp.where(visible, scores, -jnp.inf)


def forward_stats(q_segs, k_prefix, v_prefix):
    k_split = key_blocks(k_prefix)
    v_split = key_blocks(v_prefix)
    blk_ids = jnp.arange(CP_BLOCKS)

    def one_block(block_in):
        q_rows, q_blk = block_in
        q_four = q_rows.astype(jnp.float32).reshape(Q_ROWS, KV_HEADS, GROUP, HEAD_DIM)

        def lse_step(run_lse, key_in):
            k_rows, k_blk = key_in
            scores = block_scores(q_four, k_rows, q_blk, k_blk)
            return jnp.logaddexp(run_lse, jax.nn.logsumexp(scores, axis=-1)), None

        init_lse = jnp.full((KV_HEADS, GROUP, Q_ROWS), -jnp.inf, jnp.float32)
        row_lse, _ = lax.scan(lse_step, init_lse, (k_split, blk_ids))

        def out_step(out_acc, key_in):
            k_rows, v_rows, k_blk = key_in
            p_block = jnp.exp(block_scores(q_four, k_rows, q_blk, k_blk) - row_lse[..., None])
            return out_acc + jnp.einsum("hgqk,khd->qhgd", p_block, v_rows.astype(jnp.float32)), None

        init_out = jnp.zeros((Q_ROWS, KV_HEADS, GROUP, HEAD_DIM), jnp.float32)
        out_rows, _ = lax.scan(out_step, init_out, (k_split, v_split, blk_ids))
        lse_rows = jnp.transpose(row_lse, (2, 0, 1)).reshape(Q_ROWS, Q_HEADS)
        return out_rows.reshape(Q_ROWS, Q_HEADS, HEAD_DIM), lse_rows

    out_blocks, lse_blocks = lax.map(one_block, (query_blocks(q_segs), jnp.arange(SEGMENTS * CP_BLOCKS)))
    return (out_blocks.reshape(SEGMENTS, SEG_LEN, Q_HEADS, HEAD_DIM),
            lse_blocks.reshape(SEGMENTS, SEG_LEN, Q_HEADS))


def setup_inputs(seed: int = 0, part: int = 0) -> dict:
    base_key = jax.random.fold_in(jax.random.key(seed), part)
    key_q, key_k, key_vm, key_vn, key_do = jax.random.split(base_key, 5)
    q_shape = (SEGMENTS, SEG_LEN, Q_HEADS, HEAD_DIM)
    k_shape = (PREFIX_LEN, KV_HEADS, HEAD_DIM)
    q_segs = jax.random.normal(key_q, q_shape, jnp.float32).astype(jnp.bfloat16)
    k_prefix = jax.random.normal(key_k, k_shape, jnp.float32).astype(jnp.bfloat16)
    v_mean = jax.random.normal(key_vm, (KV_HEADS, HEAD_DIM), jnp.float32)
    v_noise = jax.random.normal(key_vn, k_shape, jnp.float32)
    v_prefix = (v_mean + 0.5 * v_noise).astype(jnp.bfloat16)
    out_exact, lse_segs = forward_stats(q_segs, k_prefix, v_prefix)
    do_noise = jax.random.normal(key_do, q_shape, jnp.float32)
    do_segs = (do_noise + 0.5 * out_exact).astype(jnp.bfloat16)
    return {"q_segs": q_segs, "k_prefix": k_prefix, "v_prefix": v_prefix,
            "o_segs": out_exact.astype(jnp.bfloat16), "do_segs": do_segs, "lse_segs": lse_segs}


def reference(q_segs, k_prefix, v_prefix, o_segs, do_segs, lse_segs):
    delta_segs = jnp.sum(do_segs.astype(jnp.float32) * o_segs.astype(jnp.float32), axis=-1)
    k_split = key_blocks(k_prefix)
    v_split = key_blocks(v_prefix)
    blk_ids = jnp.arange(CP_BLOCKS)

    def query_step(grad_pair, query_in):
        dk_acc, dv_acc = grad_pair
        q_rows, do_rows, lse_rows, delta_rows, q_blk = query_in
        q_four = q_rows.astype(jnp.float32).reshape(Q_ROWS, KV_HEADS, GROUP, HEAD_DIM)
        do_four = do_rows.astype(jnp.float32).reshape(Q_ROWS, KV_HEADS, GROUP, HEAD_DIM)
        lse_four = heads_first(lse_rows)
        delta_four = heads_first(delta_rows)

        def key_step(dq_acc, key_in):
            k_rows, v_rows, k_blk = key_in
            p_block = jnp.exp(block_scores(q_four, k_rows, q_blk, k_blk) - lse_four)
            dp_block = jnp.einsum("qhgd,khd->hgqk", do_four, v_rows.astype(jnp.float32))
            ds_block = p_block * (dp_block - delta_four)
            p_low = p_block.astype(jnp.bfloat16).astype(jnp.float32)
            ds_low = ds_block.astype(jnp.bfloat16).astype(jnp.float32)
            dq_part = jnp.einsum("hgqk,khd->qhgd", ds_low, k_rows.astype(jnp.float32))
            dk_part = jnp.einsum("hgqk,qhgd->khd", ds_low, q_four) * SCALE
            dv_part = jnp.einsum("hgqk,qhgd->khd", p_low, do_four)
            return dq_acc + dq_part, (dk_part, dv_part)

        dq_init = jnp.zeros((Q_ROWS, KV_HEADS, GROUP, HEAD_DIM), jnp.float32)
        dq_sum, (dk_parts, dv_parts) = lax.scan(key_step, dq_init, (k_split, v_split, blk_ids))
        dq_rows = (dq_sum * SCALE).reshape(Q_ROWS, Q_HEADS, HEAD_DIM).astype(jnp.bfloat16)
        return (dk_acc + dk_parts, dv_acc + dv_parts), dq_rows

    grad_init = (jnp.zeros((CP_BLOCKS, K_ROWS, KV_HEADS, HEAD_DIM), jnp.float32),
                 jnp.zeros((CP_BLOCKS, K_ROWS, KV_HEADS, HEAD_DIM), jnp.float32))
    query_in = (query_blocks(q_segs), query_blocks(do_segs), query_blocks(lse_segs),
                query_blocks(delta_segs), jnp.arange(SEGMENTS * CP_BLOCKS))
    (dk_acc, dv_acc), dq_blocks = lax.scan(query_step, grad_init, query_in)
    return (dq_blocks.reshape(SEGMENTS, SEG_LEN, Q_HEADS, HEAD_DIM),
            dk_acc.reshape(PREFIX_LEN, KV_HEADS, HEAD_DIM),
            dv_acc.reshape(PREFIX_LEN, KV_HEADS, HEAD_DIM))
```

```python
import functools

import jax
import jax.numpy as jnp
from jax import lax
from jax.experimental import pallas as pl
from jax.experimental.pallas import tpu as pltpu
from jax.sharding import PartitionSpec as P

MESH = pl.DeviceIdType.MESH
SEQ_AXES = ("cp_outer", "cp")
BF16 = jnp.bfloat16
F32 = jnp.float32
LOG2E = 1.4426950408889634
TILE = 256
WIDE = 4
AHEAD = 6


def dot(a, b, ca, cb):
    return lax.dot_general(a, b, (((ca,), (cb,)), ((), ())), preferred_element_type=F32)


def attn_kernel(dims, q_h, do_h, k_h, v_h, st_h, dq_o, dk_o, dv_o,
                q_b, do_b, k_b, v_b, st_b, col_b, k_t, q_t, do_t, dq_a, dk_a, dv_a, dk_s, dv_s,
                in_send, out_send, st_recv, kv_recv, row_recv, out_recv):
    n_dev, inner, n_segs, group, q_rows, head_dim, k_rows, late = dims
    scale = head_dim ** -0.5
    me = lax.axis_index("cp_outer") * inner + lax.axis_index("cp")
    n_tiles = n_segs + 1
    n_wide = n_tiles // WIDE
    first_late = n_segs - late
    late_tile = first_late + 1
    seg_rows = group * TILE

    def peer(i):
        return lax.rem(me + i, n_dev)

    def device(p):
        return (0, lax.div(p, inner), lax.rem(p, inner))

    barrier = pltpu.get_barrier_semaphore()
    for i in range(1, n_dev):
        pl.semaphore_signal(barrier, inc=1, device_id=device(peer(i)), device_id_type=MESH)
    pl.semaphore_wait(barrier, n_dev - 1)

    def send(i, src, dst, send_sem, recv_sem):
        if i == 0:
            pltpu.make_async_copy(src, dst, recv_sem).start()
        else:
            pltpu.make_async_remote_copy(src_ref=src, dst_ref=dst, send_sem=send_sem, recv_sem=recv_sem,
                                         device_id=device(peer(i)), device_id_type=MESH).start()

    def arrived(ref, sem):
        pltpu.make_async_copy(ref, ref, sem).wait()

    def send_kv():
        for i in range(n_dev):
            p = peer(i)
            rows = pl.ds(pl.multiple_of(me * k_rows, 32), k_rows)
            send(i, k_h.at[p], k_b.at[rows], in_send.at[1], kv_recv.at[0, me])
            send(i, v_h.at[p], v_b.at[rows], in_send.at[2], kv_recv.at[1, me])

    def send_pair(r):
        segs = pl.ds(2 * r, 2)
        rows = pl.ds(pl.multiple_of(me * q_rows, q_rows), q_rows)
        for i in range(n_dev):
            p = peer(i)
            send(i, q_h.at[p, segs], q_b.at[segs, :, rows], in_send.at[3], row_recv.at[0, r])
            send(i, do_h.at[p, segs], do_b.at[segs, :, rows], in_send.at[4], row_recv.at[1, r])

        @pl.when((me > 0) & (r == lax.max(2 * me - 3, 0)))
        def _():
            send_kv()

    for i in range(n_dev):
        send(i, st_h.at[peer(i)], st_b.at[me], in_send.at[0], st_recv)

    @pl.when(me == 0)
    def _():
        send_kv()

    @pl.loop(0, AHEAD)
    def _(r):
        send_pair(r)

    @pl.loop(0, n_tiles)
    def _(i):
        dk_a[i] = jnp.zeros((head_dim, TILE), F32)
        dv_a[i] = jnp.zeros((head_dim, TILE), F32)

    arrived(st_b, st_recv)

    @pl.loop(0, n_segs // 4)
    def _(g):
        for b in range(n_dev):
            block = st_b[b, :, pl.ds(pl.multiple_of(g * 128, 128), 128)].T
            for s in range(4):
                col_b[4 * g + s, pl.ds(b * q_rows, q_rows), 0:8] = block[s * q_rows:(s + 1) * q_rows]

    def grads(j, slot, first, n, masked):
        keys = pl.ds(pl.multiple_of(first * TILE, TILE), n * TILE)
        k_blk = k_b[keys, :]
        v_blk = v_b[keys, :]
        if masked:
            visible = (lax.broadcasted_iota(jnp.int32, (TILE, TILE), 0)
                       >= lax.broadcasted_iota(jnp.int32, (TILE, TILE), 1))
        p_low = []
        ds_low = []
        for h in range(group):
            s = dot(q_b[j, h], k_blk, 1, 1)
            dp = dot(do_b[j, h], v_blk, 1, 1)
            p = jnp.exp2(s * (scale * LOG2E) - col_b[j, :, h:h + 1])
            if masked:
                p = jnp.where(visible, p, 0.0)
            ds = p * (dp - col_b[j, :, group + h:group + h + 1])
            p_low.append(p.astype(BF16))
            ds_low.append(ds.astype(BF16))
        p_all = jnp.concatenate(p_low, 0)
        ds_all = jnp.concatenate(ds_low, 0)
        for t in range(n):
            cols = slice(t * TILE, (t + 1) * TILE)
            dv_a[first + t] += dot(do_t[slot], p_all[:, cols], 1, 0)
            dk_a[first + t] += dot(q_t[slot], ds_all[:, cols], 1, 0)
        for h in range(group):
            acc = dq_a[slot, h]
            for t in range(n):
                acc = acc + dot(k_t[first + t], ds_low[h][:, t * TILE:(t + 1) * TILE], 1, 1)
            dq_a[slot, h] = acc

    def open_row(j, slot):
        @pl.when(lax.rem(j, 2) == 0)
        def _():
            segs = pl.ds(pl.multiple_of(j, 2), 2)
            pair = lax.div(j, 2)
            arrived(q_b.at[segs], row_recv.at[0, pair])
            arrived(do_b.at[segs], row_recv.at[1, pair])

            @pl.when(pair + AHEAD < n_segs // 2)
            def _():
                send_pair(pair + AHEAD)

        @pl.when((j == 0) | ((lax.rem(j, 4) == 3) & (j < n_segs - 1)))
        def _():
            owner = lax.div(j + 1, 4)
            rows = pl.ds(pl.multiple_of(owner * k_rows, 32), k_rows)
            arrived(k_b.at[rows], kv_recv.at[0, owner])
            arrived(v_b.at[rows], kv_recv.at[1, owner])

        def turn_keys(t):
            k_t[t] = k_b[pl.ds(pl.multiple_of(t * TILE, TILE), TILE), :].T

        @pl.when(j == 0)
        def _():
            turn_keys(0)

        turn_keys(j + 1)
        q_t[slot] = q_b[j].reshape(seg_rows, head_dim).T
        do_t[slot] = do_b[j].reshape(seg_rows, head_dim).T
        dq_a[slot] = jnp.zeros((group, head_dim, TILE), F32)

    def span(j, slot, lo, hi):
        n = hi - lo

        @pl.loop(0, lax.div(n, WIDE))
        def _(c):
            grads(j, slot, lo + c * WIDE, WIDE, False)

        @pl.loop(hi - lax.rem(n, WIDE), hi)
        def _(t):
            grads(j, slot, t, 1, False)

        grads(j, slot, hi, 1, True)

    def close_row(j, slot):
        for h in range(group):
            q_b[j, h] = (dq_a[slot, h].T * scale).astype(BF16)
        for i in range(n_dev):
            p = peer(i)
            rows = pl.ds(pl.multiple_of(p * q_rows, q_rows), q_rows)
            send(i, q_b.at[j, :, rows], dq_o.at[me, j], out_send.at[0], out_recv.at[0])

    def close_tile(t):
        keys = pl.ds(pl.multiple_of(t * TILE, TILE), TILE)
        dk_s[keys, :] = dk_a[t].T * scale
        dv_s[keys, :] = dv_a[t].T

    def send_piece(r):
        owner = lax.div(r * 32, k_rows)
        src = pl.ds(pl.multiple_of(r * 32, 32), 32)
        dst = pl.ds(pl.multiple_of(r * 32 - owner * k_rows, 32), 32)

        @pl.when(owner == me)
        def _():
            pltpu.make_async_copy(dk_s.at[src], dk_o.at[me, dst], out_recv.at[1]).start()
            pltpu.make_async_copy(dv_s.at[src], dv_o.at[me, dst], out_recv.at[2]).start()

        @pl.when(owner != me)
        def _():
            for s, d, n in ((dk_s, dk_o, 1), (dv_s, dv_o, 2)):
                pltpu.make_async_remote_copy(src_ref=s.at[src], dst_ref=d.at[me, dst], send_sem=out_send.at[n],
                                             recv_sem=out_recv.at[n], device_id=device(owner),
                                             device_id_type=MESH).start()

    @pl.loop(0, first_late)
    def _(j):
        open_row(j, 0)
        span(j, 0, 0, j + 1)
        close_row(j, 0)

    @pl.loop(first_late, n_segs)
    def _(j):
        open_row(j, j - first_late)
        span(j, j - first_late, late_tile, j + 1)

    @pl.loop(late_tile, n_tiles)
    def _(t):
        close_tile(t)

    @pl.loop(0, n_wide)
    def _(i):
        c = lax.rem(me + i, n_wide)

        @pl.when(c * WIDE < late_tile)
        def _():
            @pl.loop(first_late, n_segs)
            def _(j):
                grads(j, j - first_late, c * WIDE, WIDE, False)

            @pl.loop(c * WIDE, c * WIDE + WIDE)
            def _(t):
                close_tile(t)

        @pl.loop(0, WIDE * TILE // 32)
        def _(r):
            send_piece(c * (WIDE * TILE // 32) + r)

    @pl.loop(0, TILE // 32)
    def _(r):
        send_piece(n_wide * (WIDE * TILE // 32) + r)

    @pl.loop(first_late, n_segs)
    def _(j):
        close_row(j, j - first_late)

    rest = n_dev - 1
    for n, ref in enumerate((st_h, k_h, v_h, q_h, do_h)):
        arrived(ref.at[pl.ds(0, rest)], in_send.at[n])
    for n, ref in enumerate((dq_o, dk_o, dv_o)):
        arrived(ref.at[pl.ds(0, rest)], out_send.at[n])
        arrived(ref, out_recv.at[n])


def solution(mesh):
    outer, inner = mesh.shape["cp_outer"], mesh.shape["cp"]
    n_dev = outer * inner
    seq_spec = P(None, SEQ_AXES, "heads", None)
    stat_spec = P(None, SEQ_AXES, "heads")
    kv_spec = P(SEQ_AXES, "heads", None)

    def local_grads(q, k, v, o, do, lse):
        n_segs, q_rows, q_heads, head_dim = q.shape
        k_rows, kv_heads, _ = k.shape
        group = q_heads // kv_heads
        late = 9
        n_tiles = n_segs + 1
        keys = n_dev * k_rows

        def by_head(x):
            return x.reshape(n_segs, q_rows, kv_heads, group, head_dim).transpose(2, 0, 3, 1, 4)

        def stat(x):
            return x.reshape(n_segs, q_rows, kv_heads, group).transpose(2, 3, 0, 1).reshape(
                kv_heads, group, n_segs * q_rows)

        delta = jnp.sum(do.astype(F32) * o.astype(F32), axis=-1)
        stats = jnp.concatenate(
            [stat(lse * LOG2E), stat(delta), jnp.zeros((kv_heads, 8 - 2 * group, n_segs * q_rows), F32)], axis=1)
        dims = (n_dev, inner, n_segs, group, q_rows, head_dim, k_rows, late)
        hbm = pl.BlockSpec(memory_space=pl.ANY)
        row = pltpu.VMEM((n_segs, group, TILE, head_dim), BF16)
        key = pltpu.VMEM((keys, head_dim), BF16)
        turned = pltpu.VMEM((late, head_dim, group * TILE), BF16)
        key_sum = pltpu.VMEM((n_tiles, head_dim, TILE), F32)
        key_out = pltpu.VMEM((keys, head_dim), F32)
        dma = pltpu.SemaphoreType.DMA
        dq, dk, dv = pl.pallas_call(
            functools.partial(attn_kernel, dims),
            out_shape=(jax.ShapeDtypeStruct((kv_heads, n_segs, group, q_rows, head_dim), BF16),
                       jax.ShapeDtypeStruct((kv_heads, k_rows, head_dim), F32),
                       jax.ShapeDtypeStruct((kv_heads, k_rows, head_dim), F32)),
            in_specs=[hbm] * 5,
            out_specs=(hbm,) * 3,
            scratch_shapes=[
                row, row, key, key,
                pltpu.VMEM((n_dev, 8, n_segs * q_rows), F32),
                pltpu.VMEM((n_segs, TILE, 128), F32),
                pltpu.VMEM((n_tiles, head_dim, TILE), BF16),
                turned, turned,
                pltpu.VMEM((late, group, head_dim, TILE), F32),
                key_sum, key_sum, key_out, key_out,
                dma((5,)), dma((3,)), dma, dma((2, n_dev)), dma((2, n_segs // 2)), dma((3,))],
            compiler_params=pltpu.CompilerParams(
                collective_id=0, has_side_effects=True, vmem_limit_bytes=67043328),
            cost_estimate=pl.CostEstimate(flops=1680 * 5 * 2 * 256 * 256 * 128, bytes_accessed=64 << 20,
                                          transcendentals=1680 * 65536),
            name="attn_grads",
        )(by_head(q), by_head(do), k.transpose(1, 0, 2), v.transpose(1, 0, 2), stats)
        dq = dq.transpose(1, 3, 0, 2, 4).reshape(n_segs, q_rows, q_heads, head_dim)
        return dq, dk.transpose(1, 0, 2), dv.transpose(1, 0, 2)

    return jax.shard_map(local_grads, mesh=mesh,
                         in_specs=(seq_spec, kv_spec, kv_spec, seq_spec, seq_spec, stat_spec),
                         out_specs=(seq_spec, kv_spec, kv_spec), check_vma=False)
```

```python
import functools

import jax
import jax.numpy as jnp
from jax import lax
from jax.experimental import pallas as pl
from jax.experimental.pallas import tpu as pltpu
from jax.sharding import PartitionSpec as P

MESH = pl.DeviceIdType.MESH
SEQ_AXES = ("cp_outer", "cp")
BF16 = jnp.bfloat16
F32 = jnp.float32
LOG2E = 1.4426950408889634
TILE = 256
WIDE = 4
RING = 8
PIECE = 32
CHUNK = 96


def dot(a, b, ca, cb):
    return lax.dot_general(a, b, (((ca,), (cb,)), ((), ())), preferred_element_type=F32)


def attn_kernel(dims, q_n, do_n, o_n, k_n, v_n, ls_n, dq_o, dk_o, dv_o,
                nat, nat_k, ls_v, stg, o_s, kv_s, st_s, q_b, do_b, k_b, v_b, st_b,
                k_t, v_t, q_t, do_t, dq_a, dk_a, dv_a, col, p_c, d_c,
                nat_sem, natk_sem, ls_sem, row_send, kv_send, st_send, out_send,
                row_recv, kv_recv, st_recv, out_recv):
    n_dev, inner, n_segs, group, q_rows, head_dim, k_rows, late = dims
    scale = head_dim ** -0.5
    me = lax.axis_index("cp_outer") * inner + lax.axis_index("cp")
    n_pairs = n_segs // 2
    n_tiles = n_segs + 1
    first_late = n_segs - late
    late_tile = first_late
    n_cols = late_tile // WIDE
    pieces = k_rows // PIECE
    rest = n_dev - 1
    my_rows = pl.ds(pl.multiple_of(me * q_rows, q_rows), q_rows)

    def peer(i):
        return lax.rem(me + i, n_dev)

    def device(p):
        return (0, lax.div(p, inner), lax.rem(p, inner))

    def remote(src, dst, send_sem, recv_sem, p):
        pltpu.make_async_remote_copy(src_ref=src, dst_ref=dst, send_sem=send_sem, recv_sem=recv_sem,
                                     device_id=device(p), device_id_type=MESH).start()

    def arrived(ref, sem):
        pltpu.make_async_copy(ref, ref, sem).wait()

    def fetch(r):
        for a, src in enumerate((q_n, do_n, o_n)):
            pltpu.make_async_copy(src.at[pl.ds(r * 2 * q_rows, 2 * q_rows)], nat.at[lax.rem(r, 2), a],
                                  nat_sem.at[lax.rem(r, 2), a]).start()

    def fetch_keys(c):
        for a, src in enumerate((k_n, v_n)):
            pltpu.make_async_copy(src.at[pl.ds(c * CHUNK, CHUNK)], nat_k.at[lax.rem(c, 2), a],
                                  natk_sem.at[lax.rem(c, 2), a]).start()

    def send_keys():
        fetch_keys(0)

        @pl.loop(0, k_rows // CHUNK)
        def _(c):
            buf = lax.rem(c, 2)
            rows = pl.ds(pl.multiple_of(c * CHUNK, CHUNK), CHUNK)
            dst = pl.ds(pl.multiple_of(me * k_rows + c * CHUNK, 32), CHUNK)
            for a in range(2):
                arrived(nat_k.at[buf, a], natk_sem.at[buf, a])

            @pl.when(c + 1 < k_rows // CHUNK)
            def _():
                fetch_keys(c + 1)

            for a, land in enumerate((k_b, v_b)):
                kv_s[a, :, rows] = jnp.transpose(nat_k[buf, a], (1, 0, 2))
                land[dst, :] = kv_s[a, me, rows]
            for i in range(1, n_dev):
                p = peer(i)
                for a, land in enumerate((k_b, v_b)):
                    remote(kv_s.at[a, p, rows], land.at[dst], kv_send.at[a], kv_recv.at[a, me], p)

    def send_pair(r):
        buf, slot = lax.rem(r, 2), lax.rem(r, RING)
        segs = pl.ds(2 * r, 2)
        for a in range(3):
            arrived(nat.at[buf, a], nat_sem.at[buf, a])

        @pl.when(r + 1 < n_pairs)
        def _():
            fetch(r + 1)

        @pl.when(r >= RING)
        def _():
            for a in range(2):
                arrived(stg.at[slot, a, pl.ds(0, rest)], row_send.at[a, slot])

        for u in range(4):
            half = slice(16 * (u % 2), 16 * (u % 2) + 16)
            for a in range(3):
                block = jnp.transpose(nat[buf, a, 16 * u:16 * u + 16], (1, 0, 2)).reshape(n_dev, group, 16, head_dim)
                if a < 2:
                    stg[slot, a, :, u // 2, :, half] = block
                else:
                    o_s[:, u // 2, :, half] = block
        for s in range(2):
            q_b[2 * r + s, :, my_rows] = stg[slot, 0, me, s]
            do_b[2 * r + s, :, my_rows] = stg[slot, 1, me, s]
        for i in range(1, n_dev):
            p = peer(i)
            for a, land in enumerate((q_b, do_b)):
                remote(stg.at[slot, a, p], land.at[segs, :, my_rows], row_send.at[a, slot], row_recv.at[a, r], p)

        ones = jnp.ones((8, head_dim), BF16)
        blank = jnp.zeros((1, 128 - group * q_rows), F32)
        for p in range(n_dev):
            for s in range(2):
                rows = group * q_rows
                prod = (stg[slot, 1, p, s].reshape(rows, head_dim).astype(F32)
                        * o_s[p, s].reshape(rows, head_dim).astype(F32))
                hi = prod.astype(BF16)
                prod = prod - hi.astype(F32)
                mid = prod.astype(BF16)
                low = (prod - mid.astype(F32)).astype(BF16)
                delta = (dot(ones, hi, 1, 1) + dot(ones, mid, 1, 1)) + dot(ones, low, 1, 1)
                st_s[r, p, 0:1, 128 * s:128 * s + 128] = jnp.concatenate([delta[0:1], blank], 1)
            st_s[r, p, 1:2, :] = ls_v[r, p:p + 1, :]
        st_b[r, me] = st_s[r, me]
        for i in range(1, n_dev):
            p = peer(i)
            remote(st_s.at[r, p], st_b.at[r, me], st_send, st_recv.at[r], p)

        @pl.when(r == lax.max(2 * me - 3, 0))
        def _():
            send_keys()

    pltpu.make_async_copy(ls_n, ls_v, ls_sem).start()
    fetch(0)
    barrier = pltpu.get_barrier_semaphore()
    for i in range(1, n_dev):
        pl.semaphore_signal(barrier, inc=1, device_id=device(peer(i)), device_id_type=MESH)
    pl.semaphore_wait(barrier, rest)
    arrived(ls_v, ls_sem)

    @pl.loop(0, RING)
    def _(r):
        send_pair(r)

    @pl.loop(0, 2 * n_tiles)
    def _(i):
        dk_a[i] = jnp.zeros((head_dim, 128), F32)
        dv_a[i] = jnp.zeros((head_dim, 128), F32)

    q_t[1] = jnp.zeros(q_t.shape[1:], BF16)
    do_t[1] = jnp.zeros(do_t.shape[1:], BF16)
    dq_a[1] = jnp.zeros(dq_a.shape[1:], F32)
    p_c[...] = jnp.zeros(p_c.shape, BF16)
    d_c[...] = jnp.zeros(d_c.shape, BF16)

    def products(j, slot, tiles, old_slot, old_tile, masked=False):
        if masked:
            visible = (lax.broadcasted_iota(jnp.int32, (TILE, TILE), 0)
                       >= lax.broadcasted_iota(jnp.int32, (TILE, TILE), 1))
        old = [(p_c[h], d_c[h]) for h in range(group)]
        for t in tiles:
            new = []
            dv_sum = dk_sum = None
            for h in range(group):
                p_old, d_old = old[h]
                lanes = slice(h * TILE, (h + 1) * TILE)
                if t is not None:
                    s = dot(q_b[j, h], k_t[t], 1, 0)
                part = dot(do_t[old_slot, :, lanes], p_old, 1, 0)
                dv_sum = part if dv_sum is None else dv_sum + part
                if t is not None:
                    dp = dot(do_b[j, h], v_t[t], 1, 0)
                part = dot(q_t[old_slot, :, lanes], d_old, 1, 0)
                dk_sum = part if dk_sum is None else dk_sum + part
                dq_a[old_slot, h] += dot(k_t[old_tile], d_old, 1, 1)
                if t is not None:
                    p = jnp.exp2(s * (scale * LOG2E) - col[slot, :, 2 * h + 1:2 * h + 2])
                    if masked:
                        p = jnp.where(visible, p, 0.0)
                    ds = p * (dp - col[slot, :, 2 * h:2 * h + 1])
                    new.append((p.astype(BF16), ds.astype(BF16)))
            for acc, total in ((dv_a, dv_sum), (dk_a, dk_sum)):
                acc[2 * old_tile] += total[:, :128]
                acc[2 * old_tile + 1] += total[:, 128:]
            old, old_slot, old_tile = new, slot, t
        if old:
            for h in range(group):
                p_c[h], d_c[h] = old[h]

    def open_row(j, slot):
        pair, s = lax.div(j, 2), lax.rem(j, 2)

        @pl.when(s == 0)
        def _():
            segs = pl.ds(pl.multiple_of(j, 2), 2)
            for a, land in enumerate((q_b, do_b)):
                arrived(land.at[segs, :, pl.ds(0, rest * q_rows)], row_recv.at[a, pair])
            arrived(st_b.at[pair, pl.ds(0, rest)], st_recv.at[pair])

            @pl.when(pair + RING < n_pairs)
            def _():
                send_pair(pair + RING)

        owner = lax.div(j + 1, 4)

        @pl.when(((j == 0) | ((lax.rem(j, 4) == 3) & (j < n_segs - 1))) & (owner != me))
        def _():
            rows = pl.ds(pl.multiple_of(owner * k_rows, 32), k_rows)
            for a, land in enumerate((k_b, v_b)):
                arrived(land.at[rows], kv_recv.at[a, owner])

        def turn_keys(t):
            rows = pl.ds(pl.multiple_of(t * TILE, TILE), TILE)
            k_t[t] = k_b[rows, :].T
            v_t[t] = v_b[rows, :].T

        @pl.when(j == 0)
        def _():
            turn_keys(0)

        turn_keys(j + 1)
        q_t[slot] = q_b[j].reshape(group * TILE, head_dim).T
        do_t[slot] = do_b[j].reshape(group * TILE, head_dim).T
        dq_a[slot] = jnp.zeros((group, head_dim, TILE), F32)
        for b in range(n_dev):
            stats = st_b[pair, b, :, pl.ds(pl.multiple_of(s * 128, 128), 128)]
            turned = jnp.concatenate([stats, jnp.zeros((6, 128), F32)], 0).T
            for h in range(group):
                col[slot, b * q_rows:(b + 1) * q_rows, 2 * h:2 * h + 2] = turned[h * q_rows:(h + 1) * q_rows, 0:2]

    def close_row(j, slot):
        for h in range(group):
            q_b[j, h] = (dq_a[slot, h].T * scale).astype(BF16)
        pltpu.make_async_copy(q_b.at[j, :, my_rows], dq_o.at[j, me], out_recv.at[0]).start()
        for i in range(1, n_dev):
            p = peer(i)
            rows = pl.ds(pl.multiple_of(p * q_rows, q_rows), q_rows)
            remote(q_b.at[j, :, rows], dq_o.at[j, me], out_send.at[0], out_recv.at[0], p)

    def close_tile(t):
        for b in range(2):
            dk_a[2 * t + b] = dk_a[2 * t + b].T * scale
            dv_a[2 * t + b] = dv_a[2 * t + b].T

    def send_piece(r):
        owner = lax.div(r, pieces)
        block = lax.div(r, 4)
        rows = pl.ds(pl.multiple_of(lax.rem(r, 4) * PIECE, PIECE), PIECE)
        for n, src, dst in ((1, dk_a, dk_o), (2, dv_a, dv_o)):
            @pl.when(owner == me)
            def _():
                pltpu.make_async_copy(src.at[block, rows], dst.at[r - owner * pieces, me], out_recv.at[n]).start()

            @pl.when(owner != me)
            def _():
                remote(src.at[block, rows], dst.at[r - owner * pieces, me], out_send.at[n], out_recv.at[n], owner)

    def row(j, slot, old_slot, lo, close):
        n = j + 1 - lo

        @pl.loop(0, lax.div(n, WIDE))
        def _(c):
            t = lo + c * WIDE
            products(j, slot, [t + w for w in range(WIDE)],
                     jnp.where(c == 0, old_slot, slot), jnp.where(c == 0, j, t - 1))

        @pl.loop(j + 1 - lax.rem(n, WIDE), j + 1)
        def _(t):
            products(j, slot, [t], jnp.where(t == lo, old_slot, slot), jnp.where(t == lo, j, t - 1))

        close()
        products(j, slot, [j + 1], slot, j, masked=True)

    @pl.loop(0, first_late)
    def _(j):
        slot = lax.rem(j, 2)
        open_row(j, slot)

        def close():
            @pl.when(j > 0)
            def _():
                close_row(j - 1, 1 - slot)

        row(j, slot, 1 - slot, 0, close)

    @pl.loop(first_late, n_segs)
    def _(j):
        slot = j - first_late + 2
        open_row(j, slot)

        def close():
            @pl.when(j == first_late)
            def _():
                close_row(j - 1, 1)

        row(j, slot, slot - 1, late_tile, close)

    late_pieces = (n_tiles - late_tile) * (TILE // PIECE)
    share = late_pieces // n_cols
    wide_pieces = WIDE * TILE // PIECE

    def close_wide(c):
        @pl.loop(c * WIDE, c * WIDE + WIDE)
        def _(t):
            close_tile(t)

        @pl.loop(c * wide_pieces, (c + 1) * wide_pieces)
        def _(r):
            send_piece(r)

    @pl.loop(0, n_cols)
    def _(i):
        c = lax.rem(me + i, n_cols)
        done = lax.rem(me + i + n_cols - 1, n_cols)

        @pl.loop(first_late, n_segs)
        def _(j):
            slot = j - first_late + 2
            first = j == first_late
            products(j, slot, [c * WIDE + w for w in range(WIDE)],
                     jnp.where(first, late + 1, slot - 1),
                     jnp.where(first, jnp.where(i == 0, n_segs, done * WIDE + WIDE - 1), c * WIDE + WIDE - 1))

            @pl.when(first & (i == 0))
            def _():
                @pl.loop(late_tile, n_tiles)
                def _(t):
                    close_tile(t)

            @pl.when(first & (i > 0))
            def _():
                close_wide(done)

            @pl.when(first)
            def _():
                @pl.loop(0, share)
                def _(r):
                    send_piece(late_tile * (TILE // PIECE) + lax.rem(i * share + r + me * (late_pieces // n_dev),
                                                                      late_pieces))

            @pl.when((i == n_cols - 1) & jnp.logical_not(first))
            def _():
                close_row(j - 1, slot - 1)

    last = lax.rem(me + n_cols - 1, n_cols)
    products(0, 0, [None], late + 1, last * WIDE + WIDE - 1)
    close_row(n_segs - 1, late + 1)
    close_wide(last)

    @pl.loop(0, RING)
    def _(slot):
        for a in range(2):
            arrived(stg.at[slot, a, pl.ds(0, rest)], row_send.at[a, slot])

    for a in range(2):
        arrived(kv_s.at[a, pl.ds(0, rest)], kv_send.at[a])
    arrived(st_s.at[:, pl.ds(0, rest)], st_send)
    for n, ref in enumerate((dq_o, dk_o, dv_o)):
        arrived(ref.at[:, pl.ds(0, rest)], out_send.at[n])
        arrived(ref, out_recv.at[n])


def ungroup_kernel(dq_i, dk_i, dv_i, dq_o, dk_o, dv_o):
    @pl.when(pl.program_id(0) < pl.num_programs(0) - 1)
    def _():
        dq_o[...] = jnp.transpose(dq_i[0], (1, 0, 2))

    dk_o[...] = jnp.transpose(dk_i[0], (1, 0, 2))
    dv_o[...] = jnp.transpose(dv_i[0], (1, 0, 2))


def solution(mesh):
    outer, inner = mesh.shape["cp_outer"], mesh.shape["cp"]
    n_dev = outer * inner
    seq_spec = P(None, SEQ_AXES, "heads", None)
    stat_spec = P(None, SEQ_AXES, "heads")
    kv_spec = P(SEQ_AXES, "heads", None)

    def local_grads(q, k, v, o, do, lse):
        n_segs, q_rows, q_heads, head_dim = q.shape
        k_rows, kv_heads, _ = k.shape
        group = q_heads // kv_heads
        late = 8
        n_tiles = n_segs + 1
        n_pairs = n_segs // 2
        pieces = k_rows // PIECE
        keys = n_dev * k_rows

        def flat(x):
            return x.reshape(n_segs * q_rows, q_heads, head_dim)

        stats = (lse * LOG2E).reshape(n_pairs, 2, q_rows, kv_heads, group).transpose(0, 3, 1, 4, 2)
        stats = jnp.pad(stats.reshape(n_pairs, kv_heads, 2, group * q_rows),
                        ((0, 0), (0, 0), (0, 0), (0, 128 - group * q_rows)))
        stats = stats.reshape(n_pairs, kv_heads, 256)
        dims = (n_dev, inner, n_segs, group, q_rows, head_dim, k_rows, late)
        hbm = pl.BlockSpec(memory_space=pl.ANY)
        vmem = pltpu.VMEM
        row = vmem((n_segs, group, TILE, head_dim), BF16)
        key = vmem((keys, head_dim), BF16)
        key_t = vmem((n_tiles, head_dim, TILE), BF16)
        row_t = vmem((late + 2, head_dim, group * TILE), BF16)
        key_sum = vmem((2 * n_tiles, head_dim, 128), F32)
        stat = vmem((n_pairs, n_dev, 2, 256), F32)
        carried = vmem((group, TILE, TILE), BF16)
        dma = pltpu.SemaphoreType.DMA
        kv_out = jax.ShapeDtypeStruct((pieces, kv_heads, PIECE, head_dim), F32)
        dq, dk, dv = pl.pallas_call(
            functools.partial(attn_kernel, dims),
            out_shape=(jax.ShapeDtypeStruct((n_segs, kv_heads, group, q_rows, head_dim), BF16), kv_out, kv_out),
            in_specs=[hbm] * 6,
            out_specs=(hbm,) * 3,
            scratch_shapes=[
                vmem((2, 3, 2 * q_rows, q_heads, head_dim), BF16),
                vmem((2, 2, CHUNK, kv_heads, head_dim), BF16),
                vmem((n_pairs, kv_heads, 256), F32),
                vmem((RING, 2, kv_heads, 2, group, q_rows, head_dim), BF16),
                vmem((kv_heads, 2, group, q_rows, head_dim), BF16),
                vmem((2, kv_heads, k_rows, head_dim), BF16),
                stat, row, row, key, key, stat,
                key_t, key_t, row_t, row_t,
                vmem((late + 2, group, head_dim, TILE), F32),
                key_sum, key_sum,
                vmem((late + 2, TILE, 8), F32),
                carried, carried,
                dma((2, 3)), dma((2, 2)), dma, dma((2, RING)), dma((2,)), dma, dma((3,)),
                dma((2, n_pairs)), dma((2, n_dev)), dma((n_pairs,)), dma((3,))],
            compiler_params=pltpu.CompilerParams(
                collective_id=0, has_side_effects=True, vmem_limit_bytes=67043328),
            cost_estimate=pl.CostEstimate(flops=1680 * 5 * 2 * 256 * 256 * 128, bytes_accessed=64 << 20,
                                          transcendentals=1680 * 65536),
            name="attn_grads",
        )(flat(q), flat(do), flat(o), k, v, stats)

        last = n_segs - 1
        kv_in = pl.BlockSpec((1, kv_heads, PIECE, head_dim), lambda i: (i, 0, 0, 0))
        kv_back = pl.BlockSpec((PIECE, kv_heads, head_dim), lambda i: (i, 0, 0))
        dq, dk, dv = pl.pallas_call(
            ungroup_kernel,
            grid=(pieces,),
            out_shape=(jax.ShapeDtypeStruct((n_segs * q_rows, q_heads, head_dim), BF16),
                       jax.ShapeDtypeStruct((k_rows, kv_heads, head_dim), F32),
                       jax.ShapeDtypeStruct((k_rows, kv_heads, head_dim), F32)),
            in_specs=[pl.BlockSpec((1, q_heads, q_rows, head_dim), lambda i: (jnp.minimum(i, last), 0, 0, 0)),
                      kv_in, kv_in],
            out_specs=(pl.BlockSpec((q_rows, q_heads, head_dim), lambda i: (jnp.minimum(i, last), 0, 0)),
                       kv_back, kv_back),
            name="ungroup",
        )(dq.reshape(n_segs, q_heads, q_rows, head_dim), dk, dv)
        return dq.reshape(n_segs, q_rows, q_heads, head_dim), dk, dv

    return jax.shard_map(local_grads, mesh=mesh,
                         in_specs=(seq_spec, kv_spec, kv_spec, seq_spec, seq_spec, stat_spec),
                         out_specs=(seq_spec, kv_spec, kv_spec), check_vma=False)
```

```python
import functools

import jax
import jax.numpy as jnp
from jax import lax
from jax.experimental import pallas as pl
from jax.experimental.pallas import tpu as pltpu
from jax.sharding import PartitionSpec as P

MESH = pl.DeviceIdType.MESH
SEQ_AXES = ("cp_outer", "cp")
BF16 = jnp.bfloat16
F32 = jnp.float32
LOG2E = 1.4426950408889634
TILE = 256
WIDE = 4
PIECE = 32
CHUNK = 96


def dot(a, b, ca, cb):
    return lax.dot_general(a, b, (((ca,), (cb,)), ((), ())), preferred_element_type=F32)


def attn_kernel(dims, q_n, do_n, o_n, k_n, v_n, ls_n, dq_o, dk_o, dv_o, box, mir_kv, mir_q, mir_k, mir_v,
                nat, nat_k, ls_v, stg, o_s, kv_s, st_s, qd_b, k_b, v_b, st_b,
                k_t, v_t, q_t, do_t, dq_a, dk_a, dv_a, col, p_c, d_c,
                nat_sem, natk_sem, ls_sem, box_own, box_send, box_recv, pair_send, pair_d2d,
                kv_send, kv_d2d, kv_mir, kv_mir_recv, st_send, dq_send, dq_d2d, dq_mir, dq_mir_recv,
                dkv_send, dkv_d2d, dkv_mir, dkv_mir_recv, row_recv, kv_recv, st_recv, out_recv):
    n_dev, inner, n_segs, group, q_rows, head_dim, k_rows, late = dims
    scale = head_dim ** -0.5
    outer_at, inner_at = lax.axis_index("cp_outer"), lax.axis_index("cp")
    me = outer_at * inner + inner_at
    core = lax.rem(inner_at, 2)
    mate = me + 1 - 2 * core
    n_pairs = n_segs // 2
    n_tiles = n_segs + 1
    first_late = n_segs - late
    late_tile = first_late
    n_cols = late_tile // WIDE
    pieces = k_rows // PIECE
    rest = n_dev - 1
    early_pairs = first_late // 2

    def chip_cores(flip_outer, flip_inner):
        y = 1 - outer_at if flip_outer else outer_at
        x = (inner - 2) - (inner_at - core) if flip_inner else inner_at - core
        return [y * inner + x + c for c in range(2)]

    along = chip_cores(False, True) + chip_cores(True, False)
    across = chip_cores(True, True)

    def sent_by_me(send_all):
        @pl.when(core == 0)
        def _():
            send_all(along)

        @pl.when(core == 1)
        def _():
            send_all(across)

    def rows_of(p):
        return pl.ds(pl.multiple_of(p * q_rows, q_rows), q_rows)

    def device(p):
        return (0, lax.div(p, inner), lax.rem(p, inner))

    def remote(src, dst, send_sem, recv_sem, p):
        pltpu.make_async_remote_copy(src_ref=src, dst_ref=dst, send_sem=send_sem, recv_sem=recv_sem,
                                     device_id=device(p), device_id_type=MESH).start()

    def arrived(ref, sem):
        pltpu.make_async_copy(ref, ref, sem).wait()

    def wait_sent(whole, half, sem):
        @pl.when(core == 0)
        def _():
            arrived(whole, sem)

        @pl.when(core == 1)
        def _():
            arrived(half, sem)

    def pair_at(k):
        return jnp.where(k < early_pairs, early_pairs - 1 - k, k)

    def fetch(k):
        r = pair_at(k)
        for a, src in enumerate((q_n, do_n, o_n)):
            pltpu.make_async_copy(src.at[pl.ds(r * 2 * q_rows, 2 * q_rows)], nat.at[lax.rem(k, 2), a],
                                  nat_sem.at[lax.rem(k, 2), a]).start()

    def fetch_keys(c):
        for a, src in enumerate((k_n, v_n)):
            pltpu.make_async_copy(src.at[pl.ds(c * CHUNK, CHUNK)], nat_k.at[lax.rem(c, 2), a],
                                  natk_sem.at[lax.rem(c, 2), a]).start()

    def send_keys(src, owner):
        dst = pl.ds(pl.multiple_of(owner * k_rows, 32), k_rows)

        def send_all(to):
            for p in to:
                for a, land in enumerate((k_b, v_b)):
                    remote(src.at[a, p], land.at[dst], kv_send.at[a], kv_recv.at[a], p)

        sent_by_me(send_all)

    def stage_keys():
        @pl.loop(0, k_rows // CHUNK)
        def _(c):
            buf = lax.rem(c, 2)
            rows = pl.ds(pl.multiple_of(c * CHUNK, CHUNK), CHUNK)
            dst = pl.ds(pl.multiple_of(me * k_rows + c * CHUNK, 32), CHUNK)
            for a in range(2):
                arrived(nat_k.at[buf, a], natk_sem.at[buf, a])

            @pl.when(c + 1 < k_rows // CHUNK)
            def _():
                fetch_keys(c + 1)

            for a, land in enumerate((k_b, v_b)):
                kv_s[a, :, rows] = jnp.transpose(nat_k[buf, a], (1, 0, 2))
                land[dst, :] = kv_s[a, me, rows]

        send_keys(kv_s, me)
        dst = pl.ds(pl.multiple_of(me * k_rows, 32), k_rows)
        for a, land in enumerate((k_b, v_b)):
            remote(kv_s.at[a, mate], land.at[dst], kv_d2d.at[a], kv_recv.at[a], mate)
            remote(kv_s.at[a], mir_kv.at[a], kv_mir.at[a], kv_mir_recv.at[a], mate)

    def forward_keys():
        for a in range(2):
            arrived(mir_kv.at[a], kv_mir_recv.at[a])
        send_keys(mir_kv, mate)

    def stage_pair(k):
        buf = lax.rem(k, 2)
        r = pair_at(k)
        for a in range(3):
            arrived(nat.at[buf, a], nat_sem.at[buf, a])

        @pl.when(k + 1 < n_pairs)
        def _():
            fetch(k + 1)

        for u in range(4):
            half = slice(16 * (u % 2), 16 * (u % 2) + 16)
            for a in range(3):
                block = jnp.transpose(nat[buf, a, 16 * u:16 * u + 16], (1, 0, 2)).reshape(n_dev, group, 16, head_dim)
                if a < 2:
                    stg[buf, :, u // 2, a, :, half] = block
                else:
                    o_s[:, u // 2, :, half] = block
        segs = pl.ds(2 * r, 2)
        for s in range(2):
            qd_b[2 * r + s, :, :, rows_of(me)] = stg[buf, me, s]
        pltpu.make_async_copy(stg.at[buf], box.at[core, k], box_own.at[buf]).start()
        remote(stg.at[buf], box.at[core, k], box_send.at[buf], box_recv.at[k], mate)
        remote(stg.at[buf, mate], qd_b.at[segs, :, :, rows_of(me)], pair_d2d.at[buf], row_recv.at[r], mate)

        ones = jnp.ones((8, head_dim), BF16)
        rows = group * q_rows
        blank = jnp.zeros((1, 128 - rows), F32)
        for p in range(n_dev):
            for s in range(2):
                prod = (stg[buf, p, s, 1].reshape(rows, head_dim).astype(F32)
                        * o_s[p, s].reshape(rows, head_dim).astype(F32))
                hi = prod.astype(BF16)
                prod = prod - hi.astype(F32)
                mid = prod.astype(BF16)
                low = (prod - mid.astype(F32)).astype(BF16)
                delta = (dot(ones, hi, 1, 1) + dot(ones, mid, 1, 1)) + dot(ones, low, 1, 1)
                st_s[r, p, 0:1, 128 * s:128 * s + 128] = jnp.concatenate([delta[0:1], blank], 1)
            st_s[r, p, 1:2, :] = ls_v[r, p:p + 1, :]
        st_b[r, me] = st_s[r, me]
        for p in along + across + [mate]:
            remote(st_s.at[r, p], st_b.at[r, me], st_send, st_recv.at[r], p)

    def ship_pair(k):
        buf = lax.rem(k, 2)
        r = pair_at(k)
        segs = pl.ds(2 * r, 2)
        arrived(stg.at[buf], box_own.at[buf])
        arrived(stg.at[buf], box_send.at[buf])
        arrived(stg.at[buf, 0], pair_d2d.at[buf])
        arrived(box.at[0, k], box_recv.at[k])

        def send_all(to):
            for src in range(2):
                for p in to:
                    remote(box.at[src, k, p], qd_b.at[segs, :, :, rows_of(me - core + src)], pair_send, row_recv.at[r], p)

        sent_by_me(send_all)

    pltpu.make_async_copy(ls_n, ls_v, ls_sem).start()
    fetch_keys(0)
    fetch(0)
    barrier = pltpu.get_barrier_semaphore()
    for p in along + across + [mate]:
        pl.semaphore_signal(barrier, inc=1, device_id=device(p), device_id_type=MESH)
    pl.semaphore_wait(barrier, rest)
    arrived(ls_v, ls_sem)
    stage_keys()

    @pl.loop(0, n_pairs)
    def _(k):
        stage_pair(k)

        @pl.when(k == 1)
        def _():
            forward_keys()

        @pl.when(k > 0)
        def _():
            ship_pair(k - 1)

    ship_pair(n_pairs - 1)

    @pl.loop(0, 2 * n_tiles)
    def _(i):
        dk_a[i] = jnp.zeros((head_dim, 128), F32)
        dv_a[i] = jnp.zeros((head_dim, 128), F32)

    q_t[0] = jnp.zeros(q_t.shape[1:], BF16)
    do_t[0] = jnp.zeros(do_t.shape[1:], BF16)
    dq_a[0] = jnp.zeros(dq_a.shape[1:], F32)
    p_c[...] = jnp.zeros(p_c.shape, BF16)
    d_c[...] = jnp.zeros(d_c.shape, BF16)

    for a, land in enumerate((k_b, v_b)):
        arrived(land.at[pl.ds(0, rest * k_rows)], kv_recv.at[a])

    @pl.loop(0, n_tiles)
    def _(t):
        rows = pl.ds(pl.multiple_of(t * TILE, TILE), TILE)
        k_t[t] = k_b[rows, :].T
        v_t[t] = v_b[rows, :].T

    def products(j, slot, tiles, old_slot, old_tile, masked=False):
        if masked:
            visible = (lax.broadcasted_iota(jnp.int32, (TILE, TILE), 0)
                       >= lax.broadcasted_iota(jnp.int32, (TILE, TILE), 1))
        old = [(p_c[h], d_c[h]) for h in range(group)]
        for t in tiles:
            new = []
            dv_sum = dk_sum = None
            for h in range(group):
                p_old, d_old = old[h]
                lanes = slice(h * TILE, (h + 1) * TILE)
                if t is not None:
                    s = dot(qd_b[j, 0, h], k_t[t], 1, 0)
                part = dot(do_t[old_slot, :, lanes], p_old, 1, 0)
                dv_sum = part if dv_sum is None else dv_sum + part
                if t is not None:
                    dp = dot(qd_b[j, 1, h], v_t[t], 1, 0)
                part = dot(q_t[old_slot, :, lanes], d_old, 1, 0)
                dk_sum = part if dk_sum is None else dk_sum + part
                dq_a[old_slot, h] += dot(k_t[old_tile], d_old, 1, 1)
                if t is not None:
                    p = jnp.exp2(s * (scale * LOG2E) - col[slot, :, 2 * h + 1:2 * h + 2])
                    if masked:
                        p = jnp.where(visible, p, 0.0)
                    ds = p * (dp - col[slot, :, 2 * h:2 * h + 1])
                    new.append((p.astype(BF16), ds.astype(BF16)))
            for acc, total in ((dv_a, dv_sum), (dk_a, dk_sum)):
                acc[2 * old_tile] += total[:, :128]
                acc[2 * old_tile + 1] += total[:, 128:]
            old, old_slot, old_tile = new, slot, t
        if old:
            for h in range(group):
                p_c[h], d_c[h] = old[h]

    def open_row(j, slot, first):
        pair, s = lax.div(j, 2), lax.rem(j, 2)

        @pl.when(s == first)
        def _():
            arrived(qd_b.at[pl.ds(2 * pair, 2), :, :, pl.ds(0, rest * q_rows)], row_recv.at[pair])
            arrived(st_b.at[pair, pl.ds(0, rest)], st_recv.at[pair])

        q_t[slot] = qd_b[j, 0].reshape(group * TILE, head_dim).T
        do_t[slot] = qd_b[j, 1].reshape(group * TILE, head_dim).T
        dq_a[slot] = jnp.zeros((group, head_dim, TILE), F32)
        for b in range(n_dev):
            stats = st_b[pair, b, :, pl.ds(pl.multiple_of(s * 128, 128), 128)]
            turned = jnp.concatenate([stats, jnp.zeros((6, 128), F32)], 0).T
            for h in range(group):
                col[slot, b * q_rows:(b + 1) * q_rows, 2 * h:2 * h + 2] = turned[h * q_rows:(h + 1) * q_rows, 0:2]

    def forward_row(j):
        arrived(mir_q.at[j], dq_mir_recv.at[j])

        def send_all(to):
            for p in to:
                remote(mir_q.at[j, :, rows_of(p)], dq_o.at[j, mate], dq_send, out_recv.at[0], p)

        sent_by_me(send_all)

    def close_row(j, slot, before):
        for h in range(group):
            qd_b[j, 0, h] = (dq_a[slot, h].T * scale).astype(BF16)
        remote(qd_b.at[j, 0], mir_q.at[j], dq_mir, dq_mir_recv.at[j], mate)
        remote(qd_b.at[j, 0, :, rows_of(mate)], dq_o.at[j, me], dq_d2d, out_recv.at[0], mate)
        pltpu.make_async_copy(qd_b.at[j, 0, :, rows_of(me)], dq_o.at[j, me], out_recv.at[0]).start()

        def send_all(to):
            for p in to:
                remote(qd_b.at[j, 0, :, rows_of(p)], dq_o.at[j, me], dq_send, out_recv.at[0], p)

        sent_by_me(send_all)

        @pl.when(before >= 0)
        def _():
            forward_row(before)

    flat_sums = [ref.reshape(2 * n_tiles * 128 // PIECE, PIECE, head_dim) for ref in (dk_a, dv_a)]
    flat_mirs = [ref.reshape(2 * n_tiles * 128 // PIECE, PIECE, head_dim) for ref in (mir_k, mir_v)]
    per_tile = TILE // PIECE

    def ship_tile(t, src_dev, mine):
        def part(p, n):
            owner = lax.div(p, pieces)
            src, dst = pl.ds(p, n), pl.ds(p - owner * pieces, n)
            on_chip = lax.div(owner, 2) == lax.div(me, 2)
            both = (lax.div(owner, inner) != outer_at) & (lax.div(lax.rem(owner, inner), 2) != lax.div(inner_at, 2))
            mine_to_send = jnp.where(both, 1, 0) == core
            for n_out, out in enumerate((dk_o, dv_o)):
                ref = (flat_sums if mine else flat_mirs)[n_out]
                if mine:
                    @pl.when(owner == me)
                    def _():
                        pltpu.make_async_copy(ref.at[src], out.at[dst, src_dev], out_recv.at[1 + n_out]).start()

                    @pl.when(owner == mate)
                    def _():
                        remote(ref.at[src], out.at[dst, src_dev], dkv_d2d.at[n_out], out_recv.at[1 + n_out], mate)

                @pl.when(jnp.logical_not(on_chip) & mine_to_send)
                def _():
                    remote(ref.at[src], out.at[dst, src_dev], dkv_send.at[n_out], out_recv.at[1 + n_out], owner)

        first = t * per_tile
        whole = lax.div(first, pieces) == lax.div(first + per_tile - 1, pieces)

        @pl.when(whole)
        def _():
            part(first, per_tile)

        @pl.when(jnp.logical_not(whole))
        def _():
            @pl.loop(0, per_tile)
            def _(i):
                part(first + i, 1)

    def close_tiles(lo, n, step, mir):
        @pl.loop(0, n)
        def _(w):
            t = lo + w * step
            for b in range(2):
                dk_a[2 * t + b] = dk_a[2 * t + b].T * scale
                dv_a[2 * t + b] = dv_a[2 * t + b].T
            for a, (src, dst) in enumerate(((dk_a, mir_k), (dv_a, mir_v))):
                remote(src.at[pl.ds(2 * t, 2)], dst.at[pl.ds(2 * t, 2)], dkv_mir.at[a], dkv_mir_recv.at[a, mir], mate)

    def row(j, slot, old_slot, old_tile, lo, close):
        n = j + 1 - lo

        @pl.loop(0, lax.div(n, WIDE))
        def _(c):
            t = lo + c * WIDE
            products(j, slot, [t + w for w in range(WIDE)],
                     jnp.where(c == 0, old_slot, slot), jnp.where(c == 0, old_tile, t - 1))

        @pl.loop(j + 1 - lax.rem(n, WIDE), j + 1)
        def _(t):
            products(j, slot, [t], jnp.where(t == lo, old_slot, slot), jnp.where(t == lo, old_tile, t - 1))

        close()
        products(j, slot, [j + 1], slot, j, masked=True)

    @pl.loop(0, first_late)
    def _(i):
        j = first_late - 1 - i
        slot = lax.rem(j, 2)
        open_row(j, slot, 1)

        def close():
            @pl.when(i > 0)
            def _():
                close_row(j + 1, 1 - slot, jnp.where(i > 1, j + 2, -1))

        row(j, slot, 1 - slot, j + 2, 0, close)

    @pl.loop(first_late, n_segs)
    def _(j):
        slot = j - first_late + 2
        first = j == first_late
        open_row(j, slot, 0)

        def close():
            @pl.when(first)
            def _():
                close_row(0, 0, 1)

        row(j, slot, jnp.where(first, 0, slot - 1), jnp.where(first, 1, j), late_tile, close)

    n_late = n_tiles - late_tile

    def column(dev, i):
        return lax.rem(dev + i, n_cols)

    def ship_column(dev, i, mine):
        @pl.loop(0, WIDE)
        def _(w):
            ship_tile(column(dev, i) + w * n_cols, dev, mine)

    def ship_late(dev, i, mine):
        @pl.loop(lax.div(i * n_late, n_cols), lax.div((i + 1) * n_late, n_cols))
        def _(n):
            ship_tile(late_tile + lax.rem(n + dev, n_late), dev, mine)

    def forward_column(i):
        for a, ref in enumerate((mir_k, mir_v)):
            arrived(ref.at[pl.ds(0, 2 * WIDE)], dkv_mir_recv.at[a, i])
        ship_column(mate, i, False)

    @pl.loop(0, n_cols)
    def _(i):
        c = column(me, i)

        @pl.loop(first_late, n_segs)
        def _(j):
            slot = j - first_late + 2
            first = j == first_late
            middle = j == first_late + late // 2
            last_tile = c + (WIDE - 1) * n_cols
            products(j, slot, [c + w * n_cols for w in range(WIDE)],
                     jnp.where(first, late + 1, slot - 1),
                     jnp.where(first, jnp.where(i == 0, n_segs, column(me, i + n_cols - 1) + (WIDE - 1) * n_cols),
                               last_tile))

            @pl.when(first & (i == 0))
            def _():
                close_tiles(late_tile, n_late, 1, n_cols)

            @pl.when(first & (i > 0))
            def _():
                close_tiles(column(me, i - 1), WIDE, n_cols, i - 1)
                ship_column(me, i - 1, True)

            @pl.when(first)
            def _():
                ship_late(me, i, True)

            @pl.when(middle & (i == 0))
            def _():
                for a, ref in enumerate((mir_k, mir_v)):
                    arrived(ref.at[pl.ds(0, 2 * n_late)], dkv_mir_recv.at[a, n_cols])

            @pl.when(middle & (i > 0))
            def _():
                forward_column(i - 1)

            @pl.when(middle)
            def _():
                ship_late(mate, i, False)

            @pl.when((i == n_cols - 1) & jnp.logical_not(first))
            def _():
                close_row(j - 1, slot - 1, jnp.where(j - 1 == first_late, 0, j - 2))

    products(0, 0, [None], late + 1, column(me, n_cols - 1) + (WIDE - 1) * n_cols)
    close_tiles(column(me, n_cols - 1), WIDE, n_cols, n_cols - 1)
    close_row(n_segs - 1, late + 1, n_segs - 2)
    ship_column(me, n_cols - 1, True)
    forward_row(n_segs - 1)
    forward_column(n_cols - 1)

    half = pl.ds(0, n_dev // 2)
    one = pl.ds(0, 1)
    wait_sent(box.at[0], box.at[0, :, half], pair_send)
    for a in range(2):
        wait_sent(kv_s.at[a], kv_s.at[a, half], kv_send.at[a])
        arrived(kv_s.at[a, one], kv_d2d.at[a])
        arrived(kv_s.at[a], kv_mir.at[a])
    arrived(st_s.at[:, pl.ds(0, rest)], st_send)
    wait_sent(dq_o, dq_o.at[:, half], dq_send)
    arrived(dq_o.at[:, one], dq_d2d)
    arrived(mir_q, dq_mir)
    for a, (out, ref) in enumerate(((dk_o, dk_a), (dv_o, dv_a))):
        wait_sent(out, out.at[:, half], dkv_send.at[a])
        arrived(out.at[:, one], dkv_d2d.at[a])
        arrived(ref, dkv_mir.at[a])
    for n, ref in enumerate((dq_o, dk_o, dv_o)):
        arrived(ref, out_recv.at[n])


def ungroup_kernel(n_q, dq_i, dk_i, dv_i, dq_o, dk_o, dv_o):
    @pl.when(pl.program_id(0) < n_q)
    def _():
        rows = dq_i.shape[2]
        for i in range(dq_i.shape[0]):
            dq_o[i * rows:(i + 1) * rows] = jnp.transpose(dq_i[i], (1, 0, 2))

    rows = dk_i.shape[2]
    for i in range(dk_i.shape[0]):
        dk_o[i * rows:(i + 1) * rows] = jnp.transpose(dk_i[i], (1, 0, 2))
        dv_o[i * rows:(i + 1) * rows] = jnp.transpose(dv_i[i], (1, 0, 2))


def solution(mesh):
    outer, inner = mesh.shape["cp_outer"], mesh.shape["cp"]
    n_dev = outer * inner
    seq_spec = P(None, SEQ_AXES, "heads", None)
    stat_spec = P(None, SEQ_AXES, "heads")
    kv_spec = P(SEQ_AXES, "heads", None)

    def local_grads(q, k, v, o, do, lse):
        n_segs, q_rows, q_heads, head_dim = q.shape
        k_rows, kv_heads, _ = k.shape
        group = q_heads // kv_heads
        late = 8
        n_tiles = n_segs + 1
        n_pairs = n_segs // 2
        pieces = k_rows // PIECE
        keys = n_dev * k_rows

        def flat(x):
            return x.reshape(n_segs * q_rows, q_heads, head_dim)

        stats = (lse * LOG2E).reshape(n_pairs, 2, q_rows, kv_heads, group).transpose(0, 3, 1, 4, 2)
        stats = jnp.pad(stats.reshape(n_pairs, kv_heads, 2, group * q_rows),
                        ((0, 0), (0, 0), (0, 0), (0, 128 - group * q_rows)))
        stats = stats.reshape(n_pairs, kv_heads, 256)
        dims = (n_dev, inner, n_segs, group, q_rows, head_dim, k_rows, late)
        hbm = pl.BlockSpec(memory_space=pl.ANY)
        vmem = pltpu.VMEM
        key = vmem((keys, head_dim), BF16)
        key_t = vmem((n_tiles, head_dim, TILE), BF16)
        row_t = vmem((late + 2, head_dim, group * TILE), BF16)
        key_sum = vmem((2 * n_tiles, head_dim, 128), F32)
        stat = vmem((n_pairs, n_dev, 2, 256), F32)
        carried = vmem((group, TILE, TILE), BF16)
        dma = pltpu.SemaphoreType.DMA
        n_cols = (n_segs - late) // WIDE
        kv_out = jax.ShapeDtypeStruct((pieces, kv_heads, PIECE, head_dim), F32)
        sums = jax.ShapeDtypeStruct((2 * n_tiles, 128, head_dim), F32)
        pair = (kv_heads, 2, 2, group, q_rows, head_dim)
        dq, dk, dv = pl.pallas_call(
            functools.partial(attn_kernel, dims),
            out_shape=(jax.ShapeDtypeStruct((n_segs, kv_heads, group, q_rows, head_dim), BF16), kv_out, kv_out,
                       jax.ShapeDtypeStruct((2, n_pairs) + pair, BF16),
                       jax.ShapeDtypeStruct((2, kv_heads, k_rows, head_dim), BF16),
                       jax.ShapeDtypeStruct((n_segs, group, TILE, head_dim), BF16), sums, sums),
            in_specs=[hbm] * 6,
            out_specs=(hbm,) * 8,
            scratch_shapes=[
                vmem((2, 3, 2 * q_rows, q_heads, head_dim), BF16),
                vmem((2, 2, CHUNK, kv_heads, head_dim), BF16),
                vmem((n_pairs, kv_heads, 256), F32),
                vmem((2,) + pair, BF16),
                vmem((kv_heads, 2, group, q_rows, head_dim), BF16),
                vmem((2, kv_heads, k_rows, head_dim), BF16),
                stat, vmem((n_segs, 2, group, TILE, head_dim), BF16), key, key, stat,
                key_t, key_t, row_t, row_t,
                vmem((late + 2, group, head_dim, TILE), F32),
                key_sum, key_sum,
                vmem((late + 2, TILE, 8), F32),
                carried, carried,
                dma((2, 3)), dma((2, 2)), dma, dma((2,)), dma((2,)), dma((n_pairs,)), dma, dma((2,)),
                dma((2,)), dma((2,)), dma((2,)), dma((2,)), dma, dma, dma, dma, dma((n_segs,)),
                dma((2,)), dma((2,)), dma((2,)), dma((2, n_cols + 1)), dma((n_pairs,)), dma((2,)), dma((n_pairs,)),
                dma((3,))],
            compiler_params=pltpu.CompilerParams(
                collective_id=0, has_side_effects=True, vmem_limit_bytes=67043328),
            cost_estimate=pl.CostEstimate(flops=1680 * 5 * 2 * 256 * 256 * 128, bytes_accessed=64 << 20,
                                          transcendentals=1680 * 65536),
            name="attn_grads",
        )(flat(q), flat(do), flat(o), k, v, stats)[:3]

        q_step, k_step = 4, 3
        n_q = n_segs // q_step
        kv_in = pl.BlockSpec((k_step, kv_heads, PIECE, head_dim), lambda i: (i, 0, 0, 0))
        kv_back = pl.BlockSpec((k_step * PIECE, kv_heads, head_dim), lambda i: (i, 0, 0))
        dq, dk, dv = pl.pallas_call(
            functools.partial(ungroup_kernel, n_q),
            grid=(pieces // k_step,),
            out_shape=(jax.ShapeDtypeStruct((n_segs * q_rows, q_heads, head_dim), BF16),
                       jax.ShapeDtypeStruct((k_rows, kv_heads, head_dim), F32),
                       jax.ShapeDtypeStruct((k_rows, kv_heads, head_dim), F32)),
            in_specs=[pl.BlockSpec((q_step, q_heads, q_rows, head_dim), lambda i: (jnp.minimum(i, n_q - 1), 0, 0, 0)),
                      kv_in, kv_in],
            out_specs=(pl.BlockSpec((q_step * q_rows, q_heads, head_dim), lambda i: (jnp.minimum(i, n_q - 1), 0, 0)),
                       kv_back, kv_back),
            name="ungroup",
        )(dq.reshape(n_segs, q_heads, q_rows, head_dim), dk, dv)
        return dq.reshape(n_segs, q_rows, q_heads, head_dim), dk, dv

    return jax.shard_map(local_grads, mesh=mesh,
                         in_specs=(seq_spec, kv_spec, kv_spec, seq_spec, seq_spec, stat_spec),
                         out_specs=(seq_spec, kv_spec, kv_spec), check_vma=False)
```

```python
import functools

import jax
import jax.numpy as jnp
from jax import lax
from jax.experimental import pallas as pl
from jax.experimental.pallas import tpu as pltpu
from jax.sharding import PartitionSpec as P

MESH = pl.DeviceIdType.MESH
SEQ_AXES = ("cp_outer", "cp")
BF16 = jnp.bfloat16
F32 = jnp.float32
LOG2E = 1.4426950408889634
TILE = 256
WIDE = 8
HALF = 4
ORDER = "SVPKSQPVSKPQVKQ"
PIECE = 32
CHUNK = 96


def dot(a, b, ca, cb):
    return lax.dot_general(a, b, (((ca,), (cb,)), ((), ())), preferred_element_type=F32)


def attn_kernel(dims, q_n, do_n, o_n, k_n, v_n, ls_n, dq_o, dk_o, dv_o, box, mir_kv, mir_q, mir_k, mir_v,
                nat, nat_k, ls_v, stg, o_s, kv_s, st_s, qd_b, k_b, v_b, st_b,
                k_t, v_t, q_t, do_t, dq_a, dk_a, dv_a, aug, aug_k, p_c, d_c, turn,
                nat_sem, natk_sem, ls_sem, box_own, box_send, box_recv, pair_send, pair_d2d,
                kv_send, kv_d2d, kv_mir, kv_mir_recv, st_send, dq_send, dq_d2d, dq_mir, dq_mir_recv,
                dkv_send, dkv_d2d, dkv_mir, dkv_mir_recv, row_recv, kv_recv, st_recv, out_recv):
    n_dev, inner, n_segs, group, q_rows, head_dim, k_rows, late = dims
    scale = head_dim ** -0.5
    outer_at, inner_at = lax.axis_index("cp_outer"), lax.axis_index("cp")
    me = outer_at * inner + inner_at
    core = lax.rem(inner_at, 2)
    mate = me + 1 - 2 * core
    n_pairs = n_segs // 2
    n_tiles = n_segs + 1
    first_late = n_segs - late
    late_tile = first_late
    n_cols = late_tile // HALF
    pieces = k_rows // PIECE
    rest = n_dev - 1
    early_pairs = first_late // 2

    def chip_cores(flip_outer, flip_inner):
        y = 1 - outer_at if flip_outer else outer_at
        x = (inner - 2) - (inner_at - core) if flip_inner else inner_at - core
        return [y * inner + x + c for c in range(2)]

    along = chip_cores(False, True) + chip_cores(True, False)
    across = chip_cores(True, True)

    def sent_by_me(send_all):
        @pl.when(core == 0)
        def _():
            send_all(along)

        @pl.when(core == 1)
        def _():
            send_all(across)

    def rows_of(p):
        return pl.ds(pl.multiple_of(p * q_rows, q_rows), q_rows)

    def device(p):
        return (0, lax.div(p, inner), lax.rem(p, inner))

    def remote(src, dst, send_sem, recv_sem, p):
        pltpu.make_async_remote_copy(src_ref=src, dst_ref=dst, send_sem=send_sem, recv_sem=recv_sem,
                                     device_id=device(p), device_id_type=MESH).start()

    def arrived(ref, sem):
        pltpu.make_async_copy(ref, ref, sem).wait()

    def wait_sent(whole, half, sem):
        @pl.when(core == 0)
        def _():
            arrived(whole, sem)

        @pl.when(core == 1)
        def _():
            arrived(half, sem)

    def pair_at(k):
        return jnp.where(k < early_pairs, early_pairs - 1 - k, k)

    def fetch(k):
        r = pair_at(k)
        for a, src in enumerate((q_n, do_n, o_n)):
            pltpu.make_async_copy(src.at[pl.ds(r * 2 * q_rows, 2 * q_rows)], nat.at[lax.rem(k, 2), a],
                                  nat_sem.at[lax.rem(k, 2), a]).start()

    def fetch_keys(c):
        for a, src in enumerate((k_n, v_n)):
            pltpu.make_async_copy(src.at[pl.ds(c * CHUNK, CHUNK)], nat_k.at[lax.rem(c, 2), a],
                                  natk_sem.at[lax.rem(c, 2), a]).start()

    def send_keys(src, owner, lo, n):
        rows = pl.ds(lo, n)
        dst = pl.ds(pl.multiple_of(owner * k_rows + lo, 32), n)

        def send_all(to):
            for p in to:
                for a, land in enumerate((k_b, v_b)):
                    remote(src.at[a, p, rows], land.at[dst], kv_send.at[a], kv_recv.at[a], p)

        sent_by_me(send_all)

    def stage_keys(first, n):
        @pl.loop(first, first + n)
        def _(c):
            buf = lax.rem(c, 2)
            rows = pl.ds(pl.multiple_of(c * CHUNK, CHUNK), CHUNK)
            dst = pl.ds(pl.multiple_of(me * k_rows + c * CHUNK, 32), CHUNK)
            for a in range(2):
                arrived(nat_k.at[buf, a], natk_sem.at[buf, a])

            @pl.when(c + 1 < k_rows // CHUNK)
            def _():
                fetch_keys(c + 1)

            for a, land in enumerate((k_b, v_b)):
                kv_s[a, :, rows] = jnp.transpose(nat_k[buf, a], (1, 0, 2))
                land[dst, :] = kv_s[a, me, rows]

        lo, rows = first * CHUNK, n * CHUNK
        send_keys(kv_s, me, lo, rows)
        src = pl.ds(lo, rows)
        dst = pl.ds(pl.multiple_of(me * k_rows + lo, 32), rows)
        for a, land in enumerate((k_b, v_b)):
            remote(kv_s.at[a, mate, src], land.at[dst], kv_d2d.at[a], kv_recv.at[a], mate)
            remote(kv_s.at[a, :, src], mir_kv.at[a, :, src], kv_mir.at[a], kv_mir_recv.at[a], mate)

    def forward_keys():
        for a in range(2):
            arrived(mir_kv.at[a], kv_mir_recv.at[a])
        send_keys(mir_kv, mate, 0, k_rows)

    def stage_pair(k):
        buf = lax.rem(k, 2)
        r = pair_at(k)
        for a in range(3):
            arrived(nat.at[buf, a], nat_sem.at[buf, a])

        @pl.when(k + 1 < n_pairs)
        def _():
            fetch(k + 1)

        for u in range(4):
            half = slice(16 * (u % 2), 16 * (u % 2) + 16)
            for a in range(3):
                block = jnp.transpose(nat[buf, a, 16 * u:16 * u + 16], (1, 0, 2)).reshape(n_dev, group, 16, head_dim)
                if a < 2:
                    stg[buf, :, u // 2, a, :, half] = block
                else:
                    o_s[:, u // 2, :, half] = block
        segs = pl.ds(2 * r, 2)
        for s in range(2):
            qd_b[2 * r + s, :, :, rows_of(me)] = stg[buf, me, s]
        pltpu.make_async_copy(stg.at[buf], box.at[core, k], box_own.at[buf]).start()
        remote(stg.at[buf], box.at[core, k], box_send.at[buf], box_recv.at[k], mate)
        remote(stg.at[buf, mate], qd_b.at[segs, :, :, rows_of(me)], pair_d2d.at[buf], row_recv.at[r], mate)

        ones = jnp.ones((8, head_dim), BF16)
        rows = group * q_rows
        blank = jnp.zeros((1, 128 - rows), F32)
        for p in range(n_dev):
            for s in range(2):
                prod = (stg[buf, p, s, 1].reshape(rows, head_dim).astype(F32)
                        * o_s[p, s].reshape(rows, head_dim).astype(F32))
                hi = prod.astype(BF16)
                prod = prod - hi.astype(F32)
                mid = prod.astype(BF16)
                low = (prod - mid.astype(F32)).astype(BF16)
                delta = (dot(ones, hi, 1, 1) + dot(ones, mid, 1, 1)) + dot(ones, low, 1, 1)
                lse = [ls_v[2 * r + s, p * group + h:p * group + h + 1, :] for h in range(group)]
                st_s[r, p, 0:1, 128 * s:128 * s + 128] = jnp.concatenate([delta[0:1], blank], 1)
                st_s[r, p, 1:2, 128 * s:128 * s + 128] = jnp.concatenate(lse + [blank], 1) * (1 / scale)
        st_b[r, me] = st_s[r, me]
        for p in along + across + [mate]:
            remote(st_s.at[r, p], st_b.at[r, me], st_send, st_recv.at[r], p)

    def ship_pair(k):
        buf = lax.rem(k, 2)
        r = pair_at(k)
        segs = pl.ds(2 * r, 2)
        arrived(stg.at[buf], box_own.at[buf])
        arrived(stg.at[buf], box_send.at[buf])
        arrived(stg.at[buf, 0], pair_d2d.at[buf])
        arrived(box.at[0, k], box_recv.at[k])

        def send_all(to):
            for src in range(2):
                for p in to:
                    remote(box.at[src, k, p], qd_b.at[segs, :, :, rows_of(me - core + src)], pair_send, row_recv.at[r], p)

        sent_by_me(send_all)

    pltpu.make_async_copy(ls_n, ls_v, ls_sem).start()
    fetch_keys(0)
    fetch(0)
    barrier = pltpu.get_barrier_semaphore()
    for p in along + across + [mate]:
        pl.semaphore_signal(barrier, inc=1, device_id=device(p), device_id_type=MESH)
    pl.semaphore_wait(barrier, rest)
    arrived(ls_v, ls_sem)
    chunks = k_rows // CHUNK
    stage_keys(0, chunks // 2)
    stage_keys(chunks // 2, chunks - chunks // 2)

    @pl.loop(0, n_pairs)
    def _(k):
        stage_pair(k)

        @pl.when(k == 1)
        def _():
            forward_keys()

        @pl.when(k > 0)
        def _():
            ship_pair(k - 1)

    ship_pair(n_pairs - 1)

    @pl.loop(0, 2 * n_tiles)
    def _(i):
        dk_a[i] = jnp.zeros((head_dim, 128), F32)
        dv_a[i] = jnp.zeros((head_dim, 128), F32)

    q_t[0] = jnp.zeros(q_t.shape[1:], BF16)
    do_t[0] = jnp.zeros(do_t.shape[1:], BF16)
    dq_a[0] = jnp.zeros(dq_a.shape[1:], F32)
    p_c[...] = jnp.zeros(p_c.shape, BF16)
    d_c[...] = jnp.zeros(d_c.shape, BF16)
    turn[1] = jnp.zeros(turn.shape[1:], BF16)
    aug[...] = jnp.zeros(aug.shape, BF16)
    place = lax.broadcasted_iota(jnp.int32, (head_dim, TILE), 0)
    for a in range(2):
        aug_k[a] = jnp.where((place < 6) & (lax.rem(place, 2) == 1 - a), -1.0, 0.0).astype(BF16)

    for a, land in enumerate((k_b, v_b)):
        arrived(land.at[pl.ds(0, rest * k_rows)], kv_recv.at[a])

    @pl.loop(0, n_tiles)
    def _(t):
        rows = pl.ds(pl.multiple_of(t * TILE, TILE), TILE)
        k_t[t] = k_b[rows, :].T
        v_t[t] = v_b[rows, :].T

    def products(items, old_slot, old_tile, masked=False):
        n = len(items)
        old = [(p_c[h], d_c[h]) for h in range(group)]
        old_turn = 1
        for w, item in enumerate(items):
            new = [None] * group
            new_turn = 1 if w == n - 1 else 0 if (n - 1 - w) % 2 else 2
            sums = {"V": None, "K": None}
            raw = {"S": [None] * group, "P": [None] * group}
            count = dict.fromkeys("SPVKQ", 0)
            kept = [turn[old_turn, h] for h in range(group)] if new_turn == old_turn else None
            for step in ORDER:
                h = count[step]
                count[step] += 1
                if step in "SP":
                    if item is None:
                        continue
                    j, slot, t = item
                    a = "SP".index(step)
                    rows = jnp.concatenate([qd_b[j, a, h], aug[slot, h]], 1)
                    cols = jnp.concatenate([(k_t, v_t)[a][t], aug_k[a]], 0)
                    raw[step][h] = dot(rows, cols, 1, 0)
                    if raw["S"][h] is not None and raw["P"][h] is not None:
                        p = jnp.exp2(raw["S"][h] * (scale * LOG2E))
                        if masked and w == n - 1:
                            visible = (lax.broadcasted_iota(jnp.int32, (TILE, TILE), 0)
                                       >= lax.broadcasted_iota(jnp.int32, (TILE, TILE), 1))
                            p = jnp.where(visible, p, 0.0)
                        ds = (p * raw["P"][h]).astype(BF16)
                        new[h] = (p.astype(BF16), ds)
                        turn[new_turn, h] = ds.T
                elif step == "Q":
                    right = turn[old_turn, h] if kept is None else kept[h]
                    dq_a[old_slot, h] += dot(k_t[old_tile], right, 1, 0)
                else:
                    lanes = slice(h * TILE, (h + 1) * TILE)
                    left = (do_t if step == "V" else q_t)[old_slot, :, lanes]
                    part = dot(left, old[h]["VK".index(step)], 1, 0)
                    sums[step] = part if sums[step] is None else sums[step] + part
            for acc, total in ((dv_a, sums["V"]), (dk_a, sums["K"])):
                acc[2 * old_tile] += total[:, :128]
                acc[2 * old_tile + 1] += total[:, 128:]
            if item is None:
                return
            old, old_turn, old_slot, old_tile = new, new_turn, slot, t
        for h in range(group):
            p_c[h], d_c[h] = old[h]

    def open_row(j, slot, opens_pair):
        pair, s = lax.div(j, 2), lax.rem(j, 2)

        @pl.when(opens_pair)
        def _():
            arrived(qd_b.at[pl.ds(2 * pair, 2), :, :, pl.ds(0, rest * q_rows)], row_recv.at[pair])
            arrived(st_b.at[pair, pl.ds(0, rest)], st_recv.at[pair])

        q_t[slot] = qd_b[j, 0].reshape(group * TILE, head_dim).T
        do_t[slot] = qd_b[j, 1].reshape(group * TILE, head_dim).T
        dq_a[slot] = jnp.zeros((group, head_dim, TILE), F32)
        for b in range(n_dev):
            stats = st_b[pair, b, :, pl.ds(pl.multiple_of(s * 128, 128), 128)]
            hi = stats.astype(BF16).astype(F32)
            mid = (stats - hi).astype(BF16).astype(F32)
            parts = jnp.concatenate([hi, mid, (stats - hi) - mid, jnp.zeros((2, 128), F32)], 0).T.astype(BF16)
            for h in range(group):
                aug[slot, h, b * q_rows:(b + 1) * q_rows, 0:8] = parts[h * q_rows:(h + 1) * q_rows]

    def forward_row(j):
        arrived(mir_q.at[j], dq_mir_recv.at[j])

        def send_all(to):
            for p in to:
                remote(mir_q.at[j, :, rows_of(p)], dq_o.at[j, mate], dq_send, out_recv.at[0], p)

        sent_by_me(send_all)

    def close_row(j, slot, before):
        for h in range(group):
            qd_b[j, 0, h] = (dq_a[slot, h].T * scale).astype(BF16)
        remote(qd_b.at[j, 0], mir_q.at[j], dq_mir, dq_mir_recv.at[j], mate)
        remote(qd_b.at[j, 0, :, rows_of(mate)], dq_o.at[j, me], dq_d2d, out_recv.at[0], mate)
        pltpu.make_async_copy(qd_b.at[j, 0, :, rows_of(me)], dq_o.at[j, me], out_recv.at[0]).start()

        def send_all(to):
            for p in to:
                remote(qd_b.at[j, 0, :, rows_of(p)], dq_o.at[j, me], dq_send, out_recv.at[0], p)

        sent_by_me(send_all)

        @pl.when(before >= 0)
        def _():
            forward_row(before)

    flat_sums = [ref.reshape(2 * n_tiles * 128 // PIECE, PIECE, head_dim) for ref in (dk_a, dv_a)]
    flat_mirs = [ref.reshape(2 * n_tiles * 128 // PIECE, PIECE, head_dim) for ref in (mir_k, mir_v)]
    per_tile = TILE // PIECE

    def ship_tile(t, src_dev, mine):
        def part(p, n):
            owner = lax.div(p, pieces)
            src, dst = pl.ds(p, n), pl.ds(p - owner * pieces, n)
            on_chip = lax.div(owner, 2) == lax.div(me, 2)
            both = (lax.div(owner, inner) != outer_at) & (lax.div(lax.rem(owner, inner), 2) != lax.div(inner_at, 2))
            mine_to_send = jnp.where(both, 1, 0) == core
            for n_out, out in enumerate((dk_o, dv_o)):
                ref = (flat_sums if mine else flat_mirs)[n_out]
                if mine:
                    @pl.when(owner == me)
                    def _():
                        pltpu.make_async_copy(ref.at[src], out.at[dst, src_dev], out_recv.at[1 + n_out]).start()

                    @pl.when(owner == mate)
                    def _():
                        remote(ref.at[src], out.at[dst, src_dev], dkv_d2d.at[n_out], out_recv.at[1 + n_out], mate)

                @pl.when(jnp.logical_not(on_chip) & mine_to_send)
                def _():
                    remote(ref.at[src], out.at[dst, src_dev], dkv_send.at[n_out], out_recv.at[1 + n_out], owner)

        first = t * per_tile
        whole = lax.div(first, pieces) == lax.div(first + per_tile - 1, pieces)

        @pl.when(whole)
        def _():
            part(first, per_tile)

        @pl.when(jnp.logical_not(whole))
        def _():
            @pl.loop(0, per_tile)
            def _(i):
                part(first + i, 1)

    def close_tiles(lo, n, step, mir):
        @pl.loop(0, n)
        def _(w):
            t = lo + w * step
            for b in range(2):
                dk_a[2 * t + b] = dk_a[2 * t + b].T * scale
                dv_a[2 * t + b] = dv_a[2 * t + b].T
            for a, (src, dst) in enumerate(((dk_a, mir_k), (dv_a, mir_v))):
                remote(src.at[pl.ds(2 * t, 2)], dst.at[pl.ds(2 * t, 2)], dkv_mir.at[a], dkv_mir_recv.at[a, mir], mate)

    @pl.loop(0, n_segs)
    def _(i):
        early = i < first_late
        j = jnp.where(early, first_late - 1 - i, i)
        slot = jnp.where(early, lax.rem(j, 2), i - first_late + 2)
        lo = jnp.where(early, 0, late_tile)
        before = jnp.where(early, j + 1, jnp.where(i == first_late, 0, j - 1))
        old_slot = jnp.where(early, 1 - slot, jnp.where(i == first_late, 0, slot - 1))
        open_row(j, slot, lax.rem(i, 2) == 0)
        n = j + 1 - lo

        def tiles(t, n):
            return [(j, slot, t + w) for w in range(n)]

        def after(t):
            return jnp.where(t == lo, old_slot, slot), jnp.where(t == lo, before + 1, t - 1)

        wide_end = lo + lax.div(n, WIDE) * WIDE
        half_end = lo + lax.div(n, HALF) * HALF

        @pl.loop(0, lax.div(n, WIDE))
        def _(c):
            t = lo + c * WIDE
            products(tiles(t, WIDE), *after(t))

        @pl.when(half_end > wide_end)
        def _():
            products(tiles(wide_end, HALF), *after(wide_end))

        for r in range(HALF):
            @pl.when(lax.rem(n, HALF) == r)
            def _():
                products(tiles(half_end, r + 1), *after(half_end), masked=True)

        @pl.when((i > 0) & (i <= first_late))
        def _():
            close_row(before, old_slot, jnp.where(i > 1, before + 1, -1))

    n_late = n_tiles - late_tile

    def column(dev, i):
        return lax.rem(dev + i, n_cols)

    def ship_column(dev, i, mine):
        @pl.loop(0, HALF)
        def _(w):
            ship_tile(column(dev, i) + w * n_cols, dev, mine)

    def ship_late(dev, i, mine):
        @pl.loop(lax.div(i * n_late, n_cols), lax.div((i + 1) * n_late, n_cols))
        def _(n):
            ship_tile(late_tile + lax.rem(n + dev, n_late), dev, mine)

    def forward_column(i):
        for a, ref in enumerate((mir_k, mir_v)):
            arrived(ref.at[pl.ds(0, 2 * HALF)], dkv_mir_recv.at[a, i])
        ship_column(mate, i, False)

    @pl.loop(0, n_cols)
    def _(i):
        c = column(me, i)

        @pl.loop(0, late // 2)
        def _(pair):
            j = first_late + 2 * pair
            slot = 2 * pair + 2
            first = pair == 0
            middle = pair == late // 4
            last_tile = c + (HALF - 1) * n_cols
            products([(j + u, slot + u, c + w * n_cols) for u in range(2) for w in range(HALF)],
                     jnp.where(first, late + 1, slot - 1),
                     jnp.where(first, jnp.where(i == 0, n_segs, column(me, i + n_cols - 1) + (HALF - 1) * n_cols),
                               last_tile))

            @pl.when(first & (i == 0))
            def _():
                close_tiles(late_tile, n_late, 1, n_cols)

            @pl.when(first & (i > 0))
            def _():
                close_tiles(column(me, i - 1), HALF, n_cols, i - 1)
                ship_column(me, i - 1, True)

            @pl.when(first)
            def _():
                ship_late(me, i, True)

            @pl.when(middle & (i == 0))
            def _():
                for a, ref in enumerate((mir_k, mir_v)):
                    arrived(ref.at[pl.ds(0, 2 * n_late)], dkv_mir_recv.at[a, n_cols])

            @pl.when(middle & (i > 0))
            def _():
                forward_column(i - 1)

            @pl.when(middle)
            def _():
                ship_late(mate, i, False)

            @pl.when(i == n_cols - 1)
            def _():
                @pl.when(jnp.logical_not(first))
                def _():
                    close_row(j - 1, slot - 1, j - 2)

                close_row(j, slot, jnp.where(first, 0, j - 1))

    products([None], late + 1, column(me, n_cols - 1) + (HALF - 1) * n_cols)
    close_tiles(column(me, n_cols - 1), HALF, n_cols, n_cols - 1)
    close_row(n_segs - 1, late + 1, n_segs - 2)
    ship_column(me, n_cols - 1, True)
    forward_row(n_segs - 1)
    forward_column(n_cols - 1)

    half = pl.ds(0, n_dev // 2)
    one = pl.ds(0, 1)
    wait_sent(box.at[0], box.at[0, :, half], pair_send)
    for a in range(2):
        wait_sent(kv_s.at[a], kv_s.at[a, half], kv_send.at[a])
        arrived(kv_s.at[a, one], kv_d2d.at[a])
        arrived(kv_s.at[a], kv_mir.at[a])
    arrived(st_s.at[:, pl.ds(0, rest)], st_send)
    wait_sent(dq_o, dq_o.at[:, half], dq_send)
    arrived(dq_o.at[:, one], dq_d2d)
    arrived(mir_q, dq_mir)
    for a, (out, ref) in enumerate(((dk_o, dk_a), (dv_o, dv_a))):
        wait_sent(out, out.at[:, half], dkv_send.at[a])
        arrived(out.at[:, one], dkv_d2d.at[a])
        arrived(ref, dkv_mir.at[a])
    for n, ref in enumerate((dq_o, dk_o, dv_o)):
        arrived(ref, out_recv.at[n])


def ungroup_kernel(q_step, k_step, dq_i, dk_i, dv_i, dq_o, dk_o, dv_o, q_in, k_in, v_in, q_out, k_out, v_out,
                   q_sem, k_sem, v_sem, q_done, k_done, v_done):
    groups = ((dq_i, q_in, q_out, dq_o, q_step, q_sem, q_done), (dk_i, k_in, k_out, dk_o, k_step, k_sem, k_done),
              (dv_i, v_in, v_out, dv_o, k_step, v_sem, v_done))

    def part(n, i, step):
        return pl.ds(i * step * n, step * n)

    for src, held, _, _, step, sem, _ in groups:
        @pl.loop(0, src.shape[0] // step)
        def _(i):
            pltpu.make_async_copy(src.at[part(1, i, step)], held.at[part(1, i, step)], sem.at[i]).start()

    for src, held, turned, dst, step, sem, done in groups:
        rows = src.shape[2]

        @pl.loop(0, src.shape[0] // step)
        def _(i):
            block = held.at[part(1, i, step)]
            pltpu.make_async_copy(block, block, sem.at[i]).wait()
            for u in range(step):
                at = pl.ds(pl.multiple_of((i * step + u) * rows, rows), rows)
                turned[at] = jnp.transpose(held[i * step + u], (1, 0, 2))
            pltpu.make_async_copy(turned.at[part(rows, i, step)], dst.at[part(rows, i, step)], done.at[i]).start()

    for src, _, turned, _, step, _, done in groups:
        rows = src.shape[2]

        @pl.loop(0, src.shape[0] // step)
        def _(i):
            block = turned.at[part(rows, i, step)]
            pltpu.make_async_copy(block, block, done.at[i]).wait()


def solution(mesh):
    outer, inner = mesh.shape["cp_outer"], mesh.shape["cp"]
    n_dev = outer * inner
    seq_spec = P(None, SEQ_AXES, "heads", None)
    stat_spec = P(None, SEQ_AXES, "heads")
    kv_spec = P(SEQ_AXES, "heads", None)

    def local_grads(q, k, v, o, do, lse):
        n_segs, q_rows, q_heads, head_dim = q.shape
        k_rows, kv_heads, _ = k.shape
        group = q_heads // kv_heads
        late = 8
        n_tiles = n_segs + 1
        n_pairs = n_segs // 2
        pieces = k_rows // PIECE
        keys = n_dev * k_rows

        def flat(x):
            return x.reshape(n_segs * q_rows, q_heads, head_dim)

        dims = (n_dev, inner, n_segs, group, q_rows, head_dim, k_rows, late)
        hbm = pl.BlockSpec(memory_space=pl.ANY)
        vmem = pltpu.VMEM
        key = vmem((keys, head_dim), BF16)
        key_t = vmem((n_tiles, head_dim, TILE), BF16)
        row_t = vmem((late + 2, head_dim, group * TILE), BF16)
        key_sum = vmem((2 * n_tiles, head_dim, 128), F32)
        stat = vmem((n_pairs, n_dev, 2, 256), F32)
        carried = vmem((group, TILE, TILE), BF16)
        dma = pltpu.SemaphoreType.DMA
        n_cols = (n_segs - late) // HALF
        kv_out = jax.ShapeDtypeStruct((pieces, kv_heads, PIECE, head_dim), F32)
        sums = jax.ShapeDtypeStruct((2 * n_tiles, 128, head_dim), F32)
        pair = (kv_heads, 2, 2, group, q_rows, head_dim)
        dq, dk, dv = pl.pallas_call(
            functools.partial(attn_kernel, dims),
            out_shape=(jax.ShapeDtypeStruct((n_segs, kv_heads, group, q_rows, head_dim), BF16), kv_out, kv_out,
                       jax.ShapeDtypeStruct((2, n_pairs) + pair, BF16),
                       jax.ShapeDtypeStruct((2, kv_heads, k_rows, head_dim), BF16),
                       jax.ShapeDtypeStruct((n_segs, group, TILE, head_dim), BF16), sums, sums),
            in_specs=[hbm] * 6,
            out_specs=(hbm,) * 8,
            scratch_shapes=[
                vmem((2, 3, 2 * q_rows, q_heads, head_dim), BF16),
                vmem((2, 2, CHUNK, kv_heads, head_dim), BF16),
                vmem((n_segs, q_heads, q_rows), F32),
                vmem((2,) + pair, BF16),
                vmem((kv_heads, 2, group, q_rows, head_dim), BF16),
                vmem((2, kv_heads, k_rows, head_dim), BF16),
                stat, vmem((n_segs, 2, group, TILE, head_dim), BF16), key, key, stat,
                key_t, key_t, row_t, row_t,
                vmem((late + 2, group, head_dim, TILE), F32),
                key_sum, key_sum,
                vmem((late + 2, group, TILE, head_dim), BF16), vmem((2, head_dim, TILE), BF16),
                carried, carried, vmem((3, group, TILE, TILE), BF16),
                dma((2, 3)), dma((2, 2)), dma, dma((2,)), dma((2,)), dma((n_pairs,)), dma, dma((2,)),
                dma((2,)), dma((2,)), dma((2,)), dma((2,)), dma, dma, dma, dma, dma((n_segs,)),
                dma((2,)), dma((2,)), dma((2,)), dma((2, n_cols + 1)), dma((n_pairs,)), dma((2,)), dma((n_pairs,)),
                dma((3,))],
            compiler_params=pltpu.CompilerParams(
                collective_id=0, has_side_effects=True, vmem_limit_bytes=67043328),
            cost_estimate=pl.CostEstimate(flops=1680 * 5 * 2 * 256 * 256 * 128, bytes_accessed=64 << 20,
                                          transcendentals=1680 * 65536),
            name="attn_grads",
        )(flat(q), flat(do), flat(o), k, v, lse.transpose(0, 2, 1))[:3]

        q_step, k_step = 4, 3
        q_rows_out = jax.ShapeDtypeStruct((n_segs * q_rows, q_heads, head_dim), BF16)
        k_rows_out = jax.ShapeDtypeStruct((k_rows, kv_heads, head_dim), F32)
        q_sems, k_sems = dma((n_segs // q_step,)), dma((pieces // k_step,))
        q_blocks, k_blocks = vmem((n_segs, q_heads, q_rows, head_dim), BF16), vmem(kv_out.shape, F32)
        q_turned, k_turned = vmem(q_rows_out.shape, BF16), vmem(k_rows_out.shape, F32)
        dq, dk, dv = pl.pallas_call(
            functools.partial(ungroup_kernel, q_step, k_step),
            out_shape=(q_rows_out, k_rows_out, k_rows_out),
            in_specs=[hbm] * 3,
            out_specs=(hbm,) * 3,
            scratch_shapes=[q_blocks, k_blocks, k_blocks, q_turned, k_turned, k_turned,
                            q_sems, k_sems, k_sems, q_sems, k_sems, k_sems],
            compiler_params=pltpu.CompilerParams(vmem_limit_bytes=67043328),
            name="ungroup",
        )(dq.reshape(n_segs, q_heads, q_rows, head_dim), dk, dv)
        return dq.reshape(n_segs, q_rows, q_heads, head_dim), dk, dv

    return jax.shard_map(local_grads, mesh=mesh,
                         in_specs=(seq_spec, kv_spec, kv_spec, seq_spec, seq_spec, stat_spec),
                         out_specs=(seq_spec, kv_spec, kv_spec), check_vma=False)
```

```python
import functools

import jax
import jax.numpy as jnp
from jax import lax
from jax.experimental import pallas as pl
from jax.experimental.pallas import tpu as pltpu
from jax.sharding import PartitionSpec as P

MESH = pl.DeviceIdType.MESH
SEQ_AXES = ("cp_outer", "cp")
BF16 = jnp.bfloat16
F32 = jnp.float32
LOG2E = 1.4426950408889634
TILE = 256
WIDE = 8
HALF = 4
ORDER = "SVPKSQPVSKPQVKQ"
PIECE = 32
CHUNK = 96


def dot(a, b, ca, cb):
    return lax.dot_general(a, b, (((ca,), (cb,)), ((), ())), preferred_element_type=F32)


def attn_kernel(dims, q_n, do_n, o_n, k_n, v_n, ls_n, dq_o, dk_o, dv_o, box, mir_kv, mir_q, mir_k, mir_v,
                nat, nat_k, ls_v, stg, o_s, kv_s, st_s, qd_b, k_b, v_b, st_b,
                k_t, v_t, q_t, do_t, dq_a, dk_a, dv_a, aug, aug_k, p_c, d_c, turn,
                nat_sem, natk_sem, ls_sem, box_own, box_send, box_recv, pair_send, pair_d2d,
                kv_send, kv_d2d, kv_mir, kv_mir_recv, st_send, dq_send, dq_d2d, dq_mir, dq_mir_recv,
                dkv_send, dkv_d2d, dkv_mir, dkv_mir_recv, row_recv, kv_recv, st_recv, out_recv):
    n_dev, inner, n_segs, group, q_rows, head_dim, k_rows, late = dims
    scale = head_dim ** -0.5
    outer_at, inner_at = lax.axis_index("cp_outer"), lax.axis_index("cp")
    me = outer_at * inner + inner_at
    core = lax.rem(inner_at, 2)
    mate = me + 1 - 2 * core
    n_pairs = n_segs // 2
    n_tiles = n_segs + 1
    first_late = n_segs - late
    late_tile = first_late
    n_cols = late_tile // HALF
    pieces = k_rows // PIECE
    rest = n_dev - 1
    middle_row = first_late // 2

    def chip_cores(flip_outer, flip_inner):
        y = 1 - outer_at if flip_outer else outer_at
        x = (inner - 2) - (inner_at - core) if flip_inner else inner_at - core
        return [y * inner + x + c for c in range(2)]

    along = chip_cores(False, True) + chip_cores(True, False)
    across = chip_cores(True, True)

    def sent_by_me(send_all):
        @pl.when(core == 0)
        def _():
            send_all(along)

        @pl.when(core == 1)
        def _():
            send_all(across)

    def rows_of(p):
        return pl.ds(pl.multiple_of(p * q_rows, q_rows), q_rows)

    def device(p):
        return (0, lax.div(p, inner), lax.rem(p, inner))

    def remote(src, dst, send_sem, recv_sem, p):
        pltpu.make_async_remote_copy(src_ref=src, dst_ref=dst, send_sem=send_sem, recv_sem=recv_sem,
                                     device_id=device(p), device_id_type=MESH).start()

    def arrived(ref, sem):
        pltpu.make_async_copy(ref, ref, sem).wait()

    def wait_sent(whole, half, sem):
        @pl.when(core == 0)
        def _():
            arrived(whole, sem)

        @pl.when(core == 1)
        def _():
            arrived(half, sem)

    def row_at(i):
        return jnp.where(i < middle_row, first_late - 1 - i,
                         jnp.where(i < middle_row + late, first_late - middle_row + i, n_segs - 1 - i))

    def pair_at(k):
        return lax.div(row_at(2 * k), 2)

    def fetch(k):
        r = pair_at(k)
        for a, src in enumerate((q_n, do_n, o_n)):
            pltpu.make_async_copy(src.at[pl.ds(r * 2 * q_rows, 2 * q_rows)], nat.at[lax.rem(k, 2), a],
                                  nat_sem.at[lax.rem(k, 2), a]).start()

    def fetch_keys(c):
        for a, src in enumerate((k_n, v_n)):
            pltpu.make_async_copy(src.at[pl.ds(c * CHUNK, CHUNK)], nat_k.at[lax.rem(c, 2), a],
                                  natk_sem.at[lax.rem(c, 2), a]).start()

    def send_keys(src, owner, lo, n):
        rows = pl.ds(lo, n)
        dst = pl.ds(pl.multiple_of(owner * k_rows + lo, 32), n)

        def send_all(to):
            for p in to:
                for a, land in enumerate((k_b, v_b)):
                    remote(src.at[a, p, rows], land.at[dst], kv_send.at[a], kv_recv.at[a], p)

        sent_by_me(send_all)

    def stage_keys(first, n):
        @pl.loop(first, first + n)
        def _(c):
            buf = lax.rem(c, 2)
            rows = pl.ds(pl.multiple_of(c * CHUNK, CHUNK), CHUNK)
            dst = pl.ds(pl.multiple_of(me * k_rows + c * CHUNK, 32), CHUNK)
            for a in range(2):
                arrived(nat_k.at[buf, a], natk_sem.at[buf, a])

            @pl.when(c + 1 < k_rows // CHUNK)
            def _():
                fetch_keys(c + 1)

            for a, land in enumerate((k_b, v_b)):
                kv_s[a, :, rows] = jnp.transpose(nat_k[buf, a], (1, 0, 2))
                land[dst, :] = kv_s[a, me, rows]

    def ship_keys(first, n):
        lo, rows = first * CHUNK, n * CHUNK
        send_keys(kv_s, me, lo, rows)
        src = pl.ds(lo, rows)
        dst = pl.ds(pl.multiple_of(me * k_rows + lo, 32), rows)
        for a, land in enumerate((k_b, v_b)):
            remote(kv_s.at[a, mate, src], land.at[dst], kv_d2d.at[a], kv_recv.at[a], mate)
            remote(kv_s.at[a, :, src], mir_kv.at[a, :, src], kv_mir.at[a], kv_mir_recv.at[a], mate)

    def forward_keys():
        for a in range(2):
            arrived(mir_kv.at[a], kv_mir_recv.at[a])
        send_keys(mir_kv, mate, 0, k_rows)

    def stage_pair(k):
        buf = lax.rem(k, 2)
        r = pair_at(k)
        for a in range(3):
            arrived(nat.at[buf, a], nat_sem.at[buf, a])

        @pl.when(k + 1 < n_pairs)
        def _():
            fetch(k + 1)

        for u in range(4):
            half = slice(16 * (u % 2), 16 * (u % 2) + 16)
            for a in range(3):
                block = jnp.transpose(nat[buf, a, 16 * u:16 * u + 16], (1, 0, 2)).reshape(n_dev, group, 16, head_dim)
                if a < 2:
                    stg[buf, :, u // 2, a, :, half] = block
                else:
                    o_s[:, u // 2, :, half] = block
        segs = pl.ds(2 * r, 2)
        for s in range(2):
            qd_b[2 * r + s, :, :, rows_of(me)] = stg[buf, me, s]
        pltpu.make_async_copy(stg.at[buf], box.at[core, k], box_own.at[buf]).start()
        remote(stg.at[buf], box.at[core, k], box_send.at[buf], box_recv.at[k], mate)
        remote(stg.at[buf, mate], qd_b.at[segs, :, :, rows_of(me)], pair_d2d.at[buf], row_recv.at[r], mate)

        ones = jnp.ones((8, head_dim), BF16)
        rows = group * q_rows
        blank = jnp.zeros((1, 128 - rows), F32)
        for p in range(n_dev):
            for s in range(2):
                prod = (stg[buf, p, s, 1].reshape(rows, head_dim).astype(F32)
                        * o_s[p, s].reshape(rows, head_dim).astype(F32))
                hi = prod.astype(BF16)
                prod = prod - hi.astype(F32)
                mid = prod.astype(BF16)
                low = (prod - mid.astype(F32)).astype(BF16)
                delta = (dot(ones, hi, 1, 1) + dot(ones, mid, 1, 1)) + dot(ones, low, 1, 1)
                lse = [ls_v[2 * r + s, p * group + h:p * group + h + 1, :] for h in range(group)]
                st_s[r, p, 0:1, 128 * s:128 * s + 128] = jnp.concatenate([delta[0:1], blank], 1)
                st_s[r, p, 1:2, 128 * s:128 * s + 128] = jnp.concatenate(lse + [blank], 1) * (1 / scale)
        st_b[r, me] = st_s[r, me]
        for p in along + across + [mate]:
            remote(st_s.at[r, p], st_b.at[r, me], st_send, st_recv.at[r], p)

    def ship_pair(k):
        buf = lax.rem(k, 2)
        r = pair_at(k)
        segs = pl.ds(2 * r, 2)
        arrived(stg.at[buf], box_own.at[buf])
        arrived(stg.at[buf], box_send.at[buf])
        arrived(stg.at[buf, 0], pair_d2d.at[buf])
        arrived(box.at[0, k], box_recv.at[k])

        def send_all(to):
            for src in range(2):
                for p in to:
                    remote(box.at[src, k, p], qd_b.at[segs, :, :, rows_of(me - core + src)], pair_send, row_recv.at[r], p)

        sent_by_me(send_all)

    pltpu.make_async_copy(ls_n, ls_v, ls_sem).start()
    fetch_keys(0)
    fetch(0)
    barrier = pltpu.get_barrier_semaphore()
    for p in along + across + [mate]:
        pl.semaphore_signal(barrier, inc=1, device_id=device(p), device_id_type=MESH)
    chunks = k_rows // CHUNK
    stage_keys(0, 2)
    pl.semaphore_wait(barrier, rest)
    ship_keys(0, 2)
    stage_keys(2, chunks - 2)
    ship_keys(2, chunks - 2)
    arrived(ls_v, ls_sem)

    @pl.loop(0, n_pairs)
    def _(k):
        stage_pair(k)

        @pl.when(k == 1)
        def _():
            forward_keys()

        @pl.when(k > 0)
        def _():
            ship_pair(k - 1)

    ship_pair(n_pairs - 1)

    @pl.loop(0, 2 * n_tiles)
    def _(i):
        dk_a[i] = jnp.zeros((head_dim, 128), F32)
        dv_a[i] = jnp.zeros((head_dim, 128), F32)

    q_t[0] = jnp.zeros(q_t.shape[1:], BF16)
    do_t[0] = jnp.zeros(do_t.shape[1:], BF16)
    dq_a[0] = jnp.zeros(dq_a.shape[1:], F32)
    p_c[...] = jnp.zeros(p_c.shape, BF16)
    d_c[...] = jnp.zeros(d_c.shape, BF16)
    turn[1] = jnp.zeros(turn.shape[1:], BF16)
    aug[...] = jnp.zeros(aug.shape, BF16)
    place = lax.broadcasted_iota(jnp.int32, (head_dim, TILE), 0)
    for a in range(2):
        aug_k[a] = jnp.where((place < 6) & (lax.rem(place, 2) == 1 - a), -1.0, 0.0).astype(BF16)

    for a, land in enumerate((k_b, v_b)):
        arrived(land.at[pl.ds(0, rest * k_rows)], kv_recv.at[a])

    @pl.loop(0, n_tiles)
    def _(t):
        rows = pl.ds(pl.multiple_of(t * TILE, TILE), TILE)
        k_t[t] = k_b[rows, :].T
        v_t[t] = v_b[rows, :].T

    def products(items, old_slot, old_tile, masked=False):
        n = len(items)
        old = [(p_c[h], d_c[h]) for h in range(group)]
        old_turn = 1
        for w, item in enumerate(items):
            new = [None] * group
            new_turn = 1 if w == n - 1 else 0 if (n - 1 - w) % 2 else 2
            sums = {"V": None, "K": None}
            raw = {"S": [None] * group, "P": [None] * group}
            count = dict.fromkeys("SPVKQ", 0)
            kept = [turn[old_turn, h] for h in range(group)] if new_turn == old_turn else None
            for step in ORDER:
                h = count[step]
                count[step] += 1
                if step in "SP":
                    if item is None:
                        continue
                    j, slot, t = item
                    a = "SP".index(step)
                    rows = jnp.concatenate([qd_b[j, a, h], aug[slot, h]], 1)
                    cols = jnp.concatenate([(k_t, v_t)[a][t], aug_k[a]], 0)
                    raw[step][h] = dot(rows, cols, 1, 0)
                    if raw["S"][h] is not None and raw["P"][h] is not None:
                        p = jnp.exp2(raw["S"][h] * (scale * LOG2E))
                        if masked and w == n - 1:
                            visible = (lax.broadcasted_iota(jnp.int32, (TILE, TILE), 0)
                                       >= lax.broadcasted_iota(jnp.int32, (TILE, TILE), 1))
                            p = jnp.where(visible, p, 0.0)
                        ds = (p * raw["P"][h]).astype(BF16)
                        new[h] = (p.astype(BF16), ds)
                        turn[new_turn, h] = ds.T
                elif step == "Q":
                    right = turn[old_turn, h] if kept is None else kept[h]
                    dq_a[old_slot, h] += dot(k_t[old_tile], right, 1, 0)
                else:
                    lanes = slice(h * TILE, (h + 1) * TILE)
                    left = (do_t if step == "V" else q_t)[old_slot, :, lanes]
                    part = dot(left, old[h]["VK".index(step)], 1, 0)
                    sums[step] = part if sums[step] is None else sums[step] + part
            for acc, total in ((dv_a, sums["V"]), (dk_a, sums["K"])):
                acc[2 * old_tile] += total[:, :128]
                acc[2 * old_tile + 1] += total[:, 128:]
            if item is None:
                return
            old, old_turn, old_slot, old_tile = new, new_turn, slot, t
        for h in range(group):
            p_c[h], d_c[h] = old[h]

    def open_row(j, slot, opens_pair):
        pair, s = lax.div(j, 2), lax.rem(j, 2)

        @pl.when(opens_pair)
        def _():
            arrived(qd_b.at[pl.ds(2 * pair, 2), :, :, pl.ds(0, rest * q_rows)], row_recv.at[pair])
            arrived(st_b.at[pair, pl.ds(0, rest)], st_recv.at[pair])

        q_t[slot] = qd_b[j, 0].reshape(group * TILE, head_dim).T
        do_t[slot] = qd_b[j, 1].reshape(group * TILE, head_dim).T
        dq_a[slot] = jnp.zeros((group, head_dim, TILE), F32)
        for b in range(n_dev):
            stats = st_b[pair, b, :, pl.ds(pl.multiple_of(s * 128, 128), 128)]
            hi = stats.astype(BF16).astype(F32)
            mid = (stats - hi).astype(BF16).astype(F32)
            parts = jnp.concatenate([hi, mid, (stats - hi) - mid, jnp.zeros((2, 128), F32)], 0).T.astype(BF16)
            for h in range(group):
                aug[slot, h, b * q_rows:(b + 1) * q_rows, 0:8] = parts[h * q_rows:(h + 1) * q_rows]

    def forward_row(j):
        arrived(mir_q.at[j], dq_mir_recv.at[j])

        def send_all(to):
            for p in to:
                remote(mir_q.at[j, :, rows_of(p)], dq_o.at[j, mate], dq_send, out_recv.at[0], p)

        sent_by_me(send_all)

    def close_row(j, slot, before):
        for h in range(group):
            qd_b[j, 0, h] = (dq_a[slot, h].T * scale).astype(BF16)
        remote(qd_b.at[j, 0], mir_q.at[j], dq_mir, dq_mir_recv.at[j], mate)
        remote(qd_b.at[j, 0, :, rows_of(mate)], dq_o.at[j, me], dq_d2d, out_recv.at[0], mate)
        pltpu.make_async_copy(qd_b.at[j, 0, :, rows_of(me)], dq_o.at[j, me], out_recv.at[0]).start()

        def send_all(to):
            for p in to:
                remote(qd_b.at[j, 0, :, rows_of(p)], dq_o.at[j, me], dq_send, out_recv.at[0], p)

        sent_by_me(send_all)

        @pl.when(before >= 0)
        def _():
            forward_row(before)

    flat_sums = [ref.reshape(2 * n_tiles * 128 // PIECE, PIECE, head_dim) for ref in (dk_a, dv_a)]
    flat_mirs = [ref.reshape(2 * n_tiles * 128 // PIECE, PIECE, head_dim) for ref in (mir_k, mir_v)]
    per_tile = TILE // PIECE

    def ship_tile(t, src_dev, mine):
        def part(p, n):
            owner = lax.div(p, pieces)
            src, dst = pl.ds(p, n), pl.ds(p - owner * pieces, n)
            on_chip = lax.div(owner, 2) == lax.div(me, 2)
            both = (lax.div(owner, inner) != outer_at) & (lax.div(lax.rem(owner, inner), 2) != lax.div(inner_at, 2))
            mine_to_send = jnp.where(both, 1, 0) == core
            for n_out, out in enumerate((dk_o, dv_o)):
                ref = (flat_sums if mine else flat_mirs)[n_out]
                if mine:
                    @pl.when(owner == me)
                    def _():
                        pltpu.make_async_copy(ref.at[src], out.at[dst, src_dev], out_recv.at[1 + n_out]).start()

                    @pl.when(owner == mate)
                    def _():
                        remote(ref.at[src], out.at[dst, src_dev], dkv_d2d.at[n_out], out_recv.at[1 + n_out], mate)

                @pl.when(jnp.logical_not(on_chip) & mine_to_send)
                def _():
                    remote(ref.at[src], out.at[dst, src_dev], dkv_send.at[n_out], out_recv.at[1 + n_out], owner)

        first = t * per_tile
        whole = lax.div(first, pieces) == lax.div(first + per_tile - 1, pieces)

        @pl.when(whole)
        def _():
            part(first, per_tile)

        @pl.when(jnp.logical_not(whole))
        def _():
            @pl.loop(0, per_tile)
            def _(i):
                part(first + i, 1)

    def close_tiles(lo, n, step, mir):
        @pl.loop(0, n)
        def _(w):
            t = lo + w * step
            for b in range(2):
                dk_a[2 * t + b] = dk_a[2 * t + b].T * scale
                dv_a[2 * t + b] = dv_a[2 * t + b].T
            for a, (src, dst) in enumerate(((dk_a, mir_k), (dv_a, mir_v))):
                remote(src.at[pl.ds(2 * t, 2)], dst.at[pl.ds(2 * t, 2)], dkv_mir.at[a], dkv_mir_recv.at[a, mir], mate)

    n_late = n_tiles - late_tile

    def column(dev, i):
        return lax.rem(dev + i, n_cols)

    def ship_column(dev, i, mine):
        @pl.loop(0, HALF)
        def _(w):
            ship_tile(column(dev, i) + w * n_cols, dev, mine)

    def ship_late(dev, n, mine):
        ship_tile(late_tile + lax.rem(n + dev, n_late), dev, mine)

    def forward_column(i):
        for a, ref in enumerate((mir_k, mir_v)):
            arrived(ref.at[pl.ds(0, 2 * HALF)], dkv_mir_recv.at[a, i])
        ship_column(mate, i, False)

    late_end = middle_row + late

    @pl.loop(0, n_segs)
    def _(i):
        j = row_at(i)
        before = jnp.where(i == 0, first_late, row_at(jnp.maximum(i - 1, 0)))
        early = j < first_late
        early_before = (before < first_late) | (i == 0)
        slot = jnp.where(early, lax.rem(j, 2), j - first_late + 2)
        old_slot = jnp.where(early_before, lax.rem(before, 2), before - first_late + 2)
        lo = jnp.where(early, 0, late_tile)
        open_row(j, slot, lax.rem(i, 2) == 0)
        n = j + 1 - lo

        def tiles(t, n):
            return [(j, slot, t + w) for w in range(n)]

        def after(t):
            return jnp.where(t == lo, old_slot, slot), jnp.where(t == lo, before + 1, t - 1)

        wide_end = lo + lax.div(n, WIDE) * WIDE
        half_end = lo + lax.div(n, HALF) * HALF

        @pl.loop(0, lax.div(n, WIDE))
        def _(c):
            t = lo + c * WIDE
            products(tiles(t, WIDE), *after(t))

        @pl.when(half_end > wide_end)
        def _():
            products(tiles(wide_end, HALF), *after(wide_end))

        for r in range(HALF):
            @pl.when(lax.rem(n, HALF) == r)
            def _():
                products(tiles(half_end, r + 1), *after(half_end), masked=True)

        @pl.when((i > 0) & early_before)
        def _():
            close_row(before, old_slot, jnp.where(i > 1, before + 1, -1))

        @pl.when(i == late_end)
        def _():
            close_tiles(late_tile, n_late, 1, n_cols)

        @pl.when(i == late_end + 1)
        def _():
            for a, ref in enumerate((mir_k, mir_v)):
                arrived(ref.at[pl.ds(0, 2 * n_late)], dkv_mir_recv.at[a, n_cols])

        @pl.when(i >= late_end)
        def _():
            turn_of = lax.div(i - late_end, 2)

            @pl.when(lax.rem(i, 2) == 0)
            def _():
                ship_late(me, turn_of, True)

            @pl.when(lax.rem(i, 2) == 1)
            def _():
                ship_late(mate, turn_of, False)

    @pl.loop(0, n_cols)
    def _(i):
        c = column(me, i)

        @pl.loop(0, late // 2)
        def _(pair):
            j = first_late + 2 * pair
            slot = 2 * pair + 2
            first = pair == 0
            middle = pair == late // 4
            last_tile = c + (HALF - 1) * n_cols
            products([(j + u, slot + u, c + w * n_cols) for u in range(2) for w in range(HALF)],
                     jnp.where(first, jnp.where(i == 0, 0, late + 1), slot - 1),
                     jnp.where(first, jnp.where(i == 0, 1, column(me, i + n_cols - 1) + (HALF - 1) * n_cols),
                               last_tile))

            @pl.when(first & (i == 0))
            def _():
                close_row(0, 0, 1)

            @pl.when(first & (i > 0))
            def _():
                close_tiles(column(me, i - 1), HALF, n_cols, i - 1)
                ship_column(me, i - 1, True)

            shipped = (n_segs - late_end) // 2

            @pl.when(first & (i < n_late - shipped))
            def _():
                ship_late(me, shipped + i, True)

            @pl.when(middle & (i > 0))
            def _():
                forward_column(i - 1)

            @pl.when(middle & (i < n_late - shipped))
            def _():
                ship_late(mate, shipped + i, False)

            @pl.when(i == n_cols - 1)
            def _():
                @pl.when(jnp.logical_not(first))
                def _():
                    close_row(j - 1, slot - 1, j - 2)

                close_row(j, slot, jnp.where(first, 0, j - 1))

    products([None], late + 1, column(me, n_cols - 1) + (HALF - 1) * n_cols)
    close_tiles(column(me, n_cols - 1), HALF, n_cols, n_cols - 1)
    close_row(n_segs - 1, late + 1, n_segs - 2)
    ship_column(me, n_cols - 1, True)
    forward_row(n_segs - 1)
    forward_column(n_cols - 1)

    half = pl.ds(0, n_dev // 2)
    one = pl.ds(0, 1)
    wait_sent(box.at[0], box.at[0, :, half], pair_send)
    for a in range(2):
        wait_sent(kv_s.at[a], kv_s.at[a, half], kv_send.at[a])
        arrived(kv_s.at[a, one], kv_d2d.at[a])
        arrived(kv_s.at[a], kv_mir.at[a])
    arrived(st_s.at[:, pl.ds(0, rest)], st_send)
    wait_sent(dq_o, dq_o.at[:, half], dq_send)
    arrived(dq_o.at[:, one], dq_d2d)
    arrived(mir_q, dq_mir)
    for a, (out, ref) in enumerate(((dk_o, dk_a), (dv_o, dv_a))):
        wait_sent(out, out.at[:, half], dkv_send.at[a])
        arrived(out.at[:, one], dkv_d2d.at[a])
        arrived(ref, dkv_mir.at[a])
    for n, ref in enumerate((dq_o, dk_o, dv_o)):
        arrived(ref, out_recv.at[n])


def ungroup_kernel(q_step, k_step, dq_i, dk_i, dv_i, dq_o, dk_o, dv_o, q_in, k_in, v_in, q_out, k_out, v_out,
                   q_sem, k_sem, v_sem, q_done, k_done, v_done):
    groups = ((dq_i, q_in, q_out, dq_o, q_step, q_sem, q_done), (dk_i, k_in, k_out, dk_o, k_step, k_sem, k_done),
              (dv_i, v_in, v_out, dv_o, k_step, v_sem, v_done))

    def part(n, i, step):
        return pl.ds(i * step * n, step * n)

    for src, held, _, _, step, sem, _ in groups:
        @pl.loop(0, src.shape[0] // step)
        def _(i):
            pltpu.make_async_copy(src.at[part(1, i, step)], held.at[part(1, i, step)], sem.at[i]).start()

    for src, held, turned, dst, step, sem, done in groups:
        rows = src.shape[2]

        @pl.loop(0, src.shape[0] // step)
        def _(i):
            block = held.at[part(1, i, step)]
            pltpu.make_async_copy(block, block, sem.at[i]).wait()
            for u in range(step):
                at = pl.ds(pl.multiple_of((i * step + u) * rows, rows), rows)
                turned[at] = jnp.transpose(held[i * step + u], (1, 0, 2))
            pltpu.make_async_copy(turned.at[part(rows, i, step)], dst.at[part(rows, i, step)], done.at[i]).start()

    for src, _, turned, _, step, _, done in groups:
        rows = src.shape[2]

        @pl.loop(0, src.shape[0] // step)
        def _(i):
            block = turned.at[part(rows, i, step)]
            pltpu.make_async_copy(block, block, done.at[i]).wait()


def solution(mesh):
    outer, inner = mesh.shape["cp_outer"], mesh.shape["cp"]
    n_dev = outer * inner
    seq_spec = P(None, SEQ_AXES, "heads", None)
    stat_spec = P(None, SEQ_AXES, "heads")
    kv_spec = P(SEQ_AXES, "heads", None)

    def local_grads(q, k, v, o, do, lse):
        n_segs, q_rows, q_heads, head_dim = q.shape
        k_rows, kv_heads, _ = k.shape
        group = q_heads // kv_heads
        late = 8
        n_tiles = n_segs + 1
        n_pairs = n_segs // 2
        pieces = k_rows // PIECE
        keys = n_dev * k_rows

        def flat(x):
            return x.reshape(n_segs * q_rows, q_heads, head_dim)

        dims = (n_dev, inner, n_segs, group, q_rows, head_dim, k_rows, late)
        hbm = pl.BlockSpec(memory_space=pl.ANY)
        vmem = pltpu.VMEM
        key = vmem((keys, head_dim), BF16)
        key_t = vmem((n_tiles, head_dim, TILE), BF16)
        row_t = vmem((late + 2, head_dim, group * TILE), BF16)
        key_sum = vmem((2 * n_tiles, head_dim, 128), F32)
        stat = vmem((n_pairs, n_dev, 2, 256), F32)
        carried = vmem((group, TILE, TILE), BF16)
        dma = pltpu.SemaphoreType.DMA
        n_cols = (n_segs - late) // HALF
        kv_out = jax.ShapeDtypeStruct((pieces, kv_heads, PIECE, head_dim), F32)
        sums = jax.ShapeDtypeStruct((2 * n_tiles, 128, head_dim), F32)
        pair = (kv_heads, 2, 2, group, q_rows, head_dim)
        dq, dk, dv = pl.pallas_call(
            functools.partial(attn_kernel, dims),
            out_shape=(jax.ShapeDtypeStruct((n_segs, kv_heads, group, q_rows, head_dim), BF16), kv_out, kv_out,
                       jax.ShapeDtypeStruct((2, n_pairs) + pair, BF16),
                       jax.ShapeDtypeStruct((2, kv_heads, k_rows, head_dim), BF16),
                       jax.ShapeDtypeStruct((n_segs, group, TILE, head_dim), BF16), sums, sums),
            in_specs=[hbm] * 6,
            out_specs=(hbm,) * 8,
            scratch_shapes=[
                vmem((2, 3, 2 * q_rows, q_heads, head_dim), BF16),
                vmem((2, 2, CHUNK, kv_heads, head_dim), BF16),
                vmem((n_segs, q_heads, q_rows), F32),
                vmem((2,) + pair, BF16),
                vmem((kv_heads, 2, group, q_rows, head_dim), BF16),
                vmem((2, kv_heads, k_rows, head_dim), BF16),
                stat, vmem((n_segs, 2, group, TILE, head_dim), BF16), key, key, stat,
                key_t, key_t, row_t, row_t,
                vmem((late + 2, group, head_dim, TILE), F32),
                key_sum, key_sum,
                vmem((late + 2, group, TILE, head_dim), BF16), vmem((2, head_dim, TILE), BF16),
                carried, carried, vmem((3, group, TILE, TILE), BF16),
                dma((2, 3)), dma((2, 2)), dma, dma((2,)), dma((2,)), dma((n_pairs,)), dma, dma((2,)),
                dma((2,)), dma((2,)), dma((2,)), dma((2,)), dma, dma, dma, dma, dma((n_segs,)),
                dma((2,)), dma((2,)), dma((2,)), dma((2, n_cols + 1)), dma((n_pairs,)), dma((2,)), dma((n_pairs,)),
                dma((3,))],
            compiler_params=pltpu.CompilerParams(
                collective_id=0, has_side_effects=True, vmem_limit_bytes=67043328),
            cost_estimate=pl.CostEstimate(flops=1680 * 5 * 2 * 256 * 256 * 128, bytes_accessed=64 << 20,
                                          transcendentals=1680 * 65536),
            name="attn_grads",
        )(flat(q), flat(do), flat(o), k, v, lse.transpose(0, 2, 1))[:3]

        q_step, k_step = 4, 3
        q_rows_out = jax.ShapeDtypeStruct((n_segs * q_rows, q_heads, head_dim), BF16)
        k_rows_out = jax.ShapeDtypeStruct((k_rows, kv_heads, head_dim), F32)
        q_sems, k_sems = dma((n_segs // q_step,)), dma((pieces // k_step,))
        q_blocks, k_blocks = vmem((n_segs, q_heads, q_rows, head_dim), BF16), vmem(kv_out.shape, F32)
        q_turned, k_turned = vmem(q_rows_out.shape, BF16), vmem(k_rows_out.shape, F32)
        dq, dk, dv = pl.pallas_call(
            functools.partial(ungroup_kernel, q_step, k_step),
            out_shape=(q_rows_out, k_rows_out, k_rows_out),
            in_specs=[hbm] * 3,
            out_specs=(hbm,) * 3,
            scratch_shapes=[q_blocks, k_blocks, k_blocks, q_turned, k_turned, k_turned,
                            q_sems, k_sems, k_sems, q_sems, k_sems, k_sems],
            compiler_params=pltpu.CompilerParams(vmem_limit_bytes=67043328),
            name="ungroup",
        )(dq.reshape(n_segs, q_heads, q_rows, head_dim), dk, dv)
        return dq.reshape(n_segs, q_rows, q_heads, head_dim), dk, dv

    return jax.shard_map(local_grads, mesh=mesh,
                         in_specs=(seq_spec, kv_spec, kv_spec, seq_spec, seq_spec, stat_spec),
                         out_specs=(seq_spec, kv_spec, kv_spec), check_vma=False)
```

```python
import functools

import jax
import jax.numpy as jnp
from jax import lax
from jax.experimental import pallas as pl
from jax.experimental.pallas import tpu as pltpu
from jax.sharding import PartitionSpec as P

MESH = pl.DeviceIdType.MESH
SEQ_AXES = ("cp_outer", "cp")
BF16 = jnp.bfloat16
F32 = jnp.float32
LOG2E = 1.4426950408889634
TILE = 256
WIDE = 8
HALF = 4
ORDER = "SVPKSQPVSKPQVKQ"
PIECE = 32
CHUNK = 96
MAIN_VMEM = 48 << 20


def dot(a, b, ca, cb):
    return lax.dot_general(a, b, (((ca,), (cb,)), ((), ())), preferred_element_type=F32)


def attn_kernel(dims, q_n, do_n, o_n, k_n, v_n, ls_n, dq_o, dk_o, dv_o, box, mir_kv, mir_q, mir_k, mir_v,
                nat, nat_k, ls_v, stg, o_s, st_s, qd_b, k_b, v_b, st_b,
                k_t, v_t, q_t, do_t, dq_a, dk_a, dv_a, aug, aug_k, p_c, d_c, turn,
                nat_sem, natk_sem, ls_sem, box_own, box_send, box_recv, pair_send, pair_d2d,
                kv_send, kv_fwd, kv_d2d, kv_mir, kv_mir_recv, st_send, dq_send, dq_d2d, dq_mir, dq_mir_recv,
                dkv_send, dkv_d2d, dkv_mir, dkv_mir_recv, row_recv, kv_recv, st_recv, out_recv):
    n_dev, inner, n_segs, group, q_rows, head_dim, k_rows, late = dims
    scale = head_dim ** -0.5
    outer_at, inner_at = lax.axis_index("cp_outer"), lax.axis_index("cp")
    me = outer_at * inner + inner_at
    core = lax.rem(inner_at, 2)
    mate = me + 1 - 2 * core
    n_pairs = n_segs // 2
    n_tiles = n_segs + 1
    first_late = n_segs - late
    late_tile = first_late
    n_cols = late_tile // HALF
    pieces = k_rows // PIECE
    rest = n_dev - 1
    middle_row = first_late // 2

    kv_s = [ref.reshape(n_dev, k_rows, head_dim) for ref in (k_t, v_t)]

    def chip_cores(flip_outer, flip_inner):
        y = 1 - outer_at if flip_outer else outer_at
        x = (inner - 2) - (inner_at - core) if flip_inner else inner_at - core
        return [y * inner + x + c for c in range(2)]

    along = chip_cores(False, True) + chip_cores(True, False)
    across = chip_cores(True, True)

    def sent_by_me(send_all):
        @pl.when(core == 0)
        def _():
            send_all(along)

        @pl.when(core == 1)
        def _():
            send_all(across)

    def rows_of(p):
        return pl.ds(pl.multiple_of(p * q_rows, q_rows), q_rows)

    def device(p):
        return (0, lax.div(p, inner), lax.rem(p, inner))

    def remote(src, dst, send_sem, recv_sem, p):
        pltpu.make_async_remote_copy(src_ref=src, dst_ref=dst, send_sem=send_sem, recv_sem=recv_sem,
                                     device_id=device(p), device_id_type=MESH).start()

    def arrived(ref, sem):
        pltpu.make_async_copy(ref, ref, sem).wait()

    def wait_sent(whole, half, sem):
        @pl.when(core == 0)
        def _():
            arrived(whole, sem)

        @pl.when(core == 1)
        def _():
            arrived(half, sem)

    def row_at(i):
        return jnp.where(i < middle_row, first_late - 1 - i,
                         jnp.where(i < middle_row + late, first_late - middle_row + i, n_segs - 1 - i))

    def pair_at(k):
        return lax.div(row_at(2 * k), 2)

    def fetch(k):
        r = pair_at(k)
        for a, src in enumerate((q_n, do_n, o_n)):
            pltpu.make_async_copy(src.at[pl.ds(r * 2 * q_rows, 2 * q_rows)], nat.at[lax.rem(k, 2), a],
                                  nat_sem.at[lax.rem(k, 2), a]).start()

    def fetch_keys(c):
        for a, src in enumerate((k_n, v_n)):
            pltpu.make_async_copy(src.at[pl.ds(c * CHUNK, CHUNK)], nat_k.at[lax.rem(c, 2), a],
                                  natk_sem.at[lax.rem(c, 2), a]).start()

    def send_keys(src, owner, lo, n, sem):
        rows = pl.ds(lo, n)
        dst = pl.ds(pl.multiple_of(owner * k_rows + lo, 32), n)

        def send_all(to):
            for p in to:
                for a, land in enumerate((k_b, v_b)):
                    remote(src[a].at[p, rows], land.at[dst], sem.at[a], kv_recv.at[a], p)

        sent_by_me(send_all)

    def stage_keys(first, n):
        @pl.loop(first, first + n)
        def _(c):
            buf = lax.rem(c, 2)
            rows = pl.ds(pl.multiple_of(c * CHUNK, CHUNK), CHUNK)
            dst = pl.ds(pl.multiple_of(me * k_rows + c * CHUNK, 32), CHUNK)
            for a in range(2):
                arrived(nat_k.at[buf, a], natk_sem.at[buf, a])

            @pl.when(c + 1 < k_rows // CHUNK)
            def _():
                fetch_keys(c + 1)

            for a, land in enumerate((k_b, v_b)):
                block = jnp.transpose(nat_k[buf, a], (1, 0, 2))
                kv_s[a][:, rows] = block
                land[dst, :] = kv_s[a][me, rows]

    def ship_keys(first, n):
        lo, rows = first * CHUNK, n * CHUNK
        send_keys(kv_s, me, lo, rows, kv_send)
        src = pl.ds(lo, rows)
        dst = pl.ds(pl.multiple_of(me * k_rows + lo, 32), rows)
        for a, land in enumerate((k_b, v_b)):
            remote(kv_s[a].at[mate, src], land.at[dst], kv_d2d.at[a], kv_recv.at[a], mate)
            remote(kv_s[a].at[:, src], mir_kv.at[a, :, src], kv_mir.at[a], kv_mir_recv.at[a], mate)

    def forward_keys():
        for a in range(2):
            arrived(mir_kv.at[a], kv_mir_recv.at[a])
        send_keys([mir_kv.at[a] for a in range(2)], mate, 0, k_rows, kv_fwd)

    def stage_pair(k):
        buf = lax.rem(k, 2)
        r = pair_at(k)
        for a in range(3):
            arrived(nat.at[buf, a], nat_sem.at[buf, a])

        @pl.when(k + 1 < n_pairs)
        def _():
            fetch(k + 1)

        for u in range(4):
            half = slice(16 * (u % 2), 16 * (u % 2) + 16)
            for a in range(3):
                block = jnp.transpose(nat[buf, a, 16 * u:16 * u + 16], (1, 0, 2)).reshape(n_dev, group, 16, head_dim)
                if a < 2:
                    stg[buf, :, u // 2, a, :, half] = block
                else:
                    o_s[:, u // 2, :, half] = block
        segs = pl.ds(2 * r, 2)
        for s in range(2):
            qd_b[2 * r + s, :, :, rows_of(me)] = stg[buf, me, s]
        pltpu.make_async_copy(stg.at[buf], box.at[core, k], box_own.at[buf]).start()
        remote(stg.at[buf], box.at[core, k], box_send.at[buf], box_recv.at[k], mate)
        remote(stg.at[buf, mate], qd_b.at[segs, :, :, rows_of(me)], pair_d2d.at[buf], row_recv.at[r], mate)

        ones = jnp.ones((8, head_dim), BF16)
        rows = group * q_rows
        blank = jnp.zeros((1, 128 - rows), F32)
        for p in range(n_dev):
            for s in range(2):
                prod = (stg[buf, p, s, 1].reshape(rows, head_dim).astype(F32)
                        * o_s[p, s].reshape(rows, head_dim).astype(F32))
                hi = prod.astype(BF16)
                prod = prod - hi.astype(F32)
                mid = prod.astype(BF16)
                low = (prod - mid.astype(F32)).astype(BF16)
                delta = (dot(ones, hi, 1, 1) + dot(ones, mid, 1, 1)) + dot(ones, low, 1, 1)
                lse = [ls_v[2 * r + s, p * group + h:p * group + h + 1, :] for h in range(group)]
                st_s[r, p, 0:1, 128 * s:128 * s + 128] = jnp.concatenate([delta[0:1], blank], 1)
                st_s[r, p, 1:2, 128 * s:128 * s + 128] = jnp.concatenate(lse + [blank], 1) * (1 / scale)
        st_b[r, me] = st_s[r, me]
        for p in along + across + [mate]:
            remote(st_s.at[r, p], st_b.at[r, me], st_send, st_recv.at[r], p)

    def ship_pair(k):
        buf = lax.rem(k, 2)
        r = pair_at(k)
        segs = pl.ds(2 * r, 2)
        arrived(stg.at[buf], box_own.at[buf])
        arrived(stg.at[buf], box_send.at[buf])
        arrived(stg.at[buf, 0], pair_d2d.at[buf])
        arrived(box.at[0, k], box_recv.at[k])

        def send_all(to):
            for src in range(2):
                for p in to:
                    remote(box.at[src, k, p], qd_b.at[segs, :, :, rows_of(me - core + src)], pair_send, row_recv.at[r], p)

        sent_by_me(send_all)

    pltpu.make_async_copy(ls_n, ls_v, ls_sem).start()
    fetch_keys(0)
    fetch(0)
    barrier = pltpu.get_barrier_semaphore()
    for p in along + across + [mate]:
        pl.semaphore_signal(barrier, inc=1, device_id=device(p), device_id_type=MESH)
    chunks = k_rows // CHUNK
    stage_keys(0, 2)
    pl.semaphore_wait(barrier, rest)
    ship_keys(0, 2)
    stage_keys(2, chunks - 2)
    ship_keys(2, chunks - 2)
    arrived(ls_v, ls_sem)

    @pl.loop(0, n_pairs)
    def _(k):
        stage_pair(k)

        @pl.when(k == 1)
        def _():
            forward_keys()

        @pl.when(k > 0)
        def _():
            ship_pair(k - 1)

    ship_pair(n_pairs - 1)

    @pl.loop(0, 2 * n_tiles)
    def _(i):
        dk_a[i] = jnp.zeros((head_dim, 128), F32)
        dv_a[i] = jnp.zeros((head_dim, 128), F32)

    q_t[0] = jnp.zeros(q_t.shape[1:], BF16)
    do_t[0] = jnp.zeros(do_t.shape[1:], BF16)
    dq_a[0] = jnp.zeros(dq_a.shape[1:], F32)
    p_c[...] = jnp.zeros(p_c.shape, BF16)
    d_c[...] = jnp.zeros(d_c.shape, BF16)
    turn[1] = jnp.zeros(turn.shape[1:], BF16)
    aug[...] = jnp.zeros(aug.shape, BF16)
    place = lax.broadcasted_iota(jnp.int32, (head_dim, TILE), 0)
    for a in range(2):
        aug_k[a] = jnp.where((place < 6) & (lax.rem(place, 2) == 1 - a), -1.0, 0.0).astype(BF16)

    for a, land in enumerate((k_b, v_b)):
        arrived(land.at[pl.ds(0, rest * k_rows)], kv_recv.at[a])

    half = pl.ds(0, n_dev // 2)
    quarter = pl.ds(0, n_dev // 4)
    one = pl.ds(0, 1)
    for a in range(2):
        wait_sent(kv_s[a].at[half], kv_s[a].at[quarter], kv_send.at[a])
        arrived(kv_s[a].at[one], kv_d2d.at[a])
        arrived(kv_s[a], kv_mir.at[a])

    @pl.loop(0, n_tiles)
    def _(t):
        for b in range(2):
            rows = pl.ds(pl.multiple_of(t * TILE + b * 128, 128), 128)
            k_t[2 * t + b] = k_b[rows, :].T
            v_t[2 * t + b] = v_b[rows, :].T

    def tile_of(ref, t):
        return jnp.concatenate([ref[2 * t], ref[2 * t + 1]], 1)

    def products(items, old_slot, old_tile, masked=False):
        n = len(items)
        old = [(p_c[h], d_c[h]) for h in range(group)]
        old_turn = 1
        for w, item in enumerate(items):
            new = [None] * group
            new_turn = 1 if w == n - 1 else 0 if (n - 1 - w) % 2 else 2
            sums = {"V": None, "K": None}
            raw = {"S": [None] * group, "P": [None] * group}
            count = dict.fromkeys("SPVKQ", 0)
            kept = [turn[old_turn, h] for h in range(group)] if new_turn == old_turn else None
            for step in ORDER:
                h = count[step]
                count[step] += 1
                if step in "SP":
                    if item is None:
                        continue
                    j, slot, t = item
                    a = "SP".index(step)
                    rows = jnp.concatenate([qd_b[j, a, h], aug[slot, h]], 1)
                    cols = jnp.concatenate([tile_of((k_t, v_t)[a], t), aug_k[a]], 0)
                    raw[step][h] = dot(rows, cols, 1, 0)
                    if raw["S"][h] is not None and raw["P"][h] is not None:
                        p = jnp.exp2(raw["S"][h] * (scale * LOG2E))
                        if masked and w == n - 1:
                            visible = (lax.broadcasted_iota(jnp.int32, (TILE, TILE), 0)
                                       >= lax.broadcasted_iota(jnp.int32, (TILE, TILE), 1))
                            p = jnp.where(visible, p, 0.0)
                        ds = (p * raw["P"][h]).astype(BF16)
                        new[h] = (p.astype(BF16), ds)
                        turn[new_turn, h] = ds.T
                elif step == "Q":
                    right = turn[old_turn, h] if kept is None else kept[h]
                    dq_a[old_slot, h] += dot(tile_of(k_t, old_tile), right, 1, 0)
                else:
                    lanes = slice(h * TILE, (h + 1) * TILE)
                    left = (do_t if step == "V" else q_t)[old_slot, :, lanes]
                    part = dot(left, old[h]["VK".index(step)], 1, 0)
                    sums[step] = part if sums[step] is None else sums[step] + part
            for acc, total in ((dv_a, sums["V"]), (dk_a, sums["K"])):
                acc[2 * old_tile] += total[:, :128]
                acc[2 * old_tile + 1] += total[:, 128:]
            if item is None:
                return
            old, old_turn, old_slot, old_tile = new, new_turn, slot, t
        for h in range(group):
            p_c[h], d_c[h] = old[h]

    def open_row(j, slot, opens_pair):
        pair, s = lax.div(j, 2), lax.rem(j, 2)

        @pl.when(opens_pair)
        def _():
            arrived(qd_b.at[pl.ds(2 * pair, 2), :, :, pl.ds(0, rest * q_rows)], row_recv.at[pair])
            arrived(st_b.at[pair, pl.ds(0, rest)], st_recv.at[pair])

        q_t[slot] = qd_b[j, 0].reshape(group * TILE, head_dim).T
        do_t[slot] = qd_b[j, 1].reshape(group * TILE, head_dim).T
        dq_a[slot] = jnp.zeros((group, head_dim, TILE), F32)
        for b in range(n_dev):
            stats = st_b[pair, b, :, pl.ds(pl.multiple_of(s * 128, 128), 128)]
            hi = stats.astype(BF16).astype(F32)
            mid = (stats - hi).astype(BF16).astype(F32)
            parts = jnp.concatenate([hi, mid, (stats - hi) - mid, jnp.zeros((2, 128), F32)], 0).T.astype(BF16)
            for h in range(group):
                aug[slot, h, b * q_rows:(b + 1) * q_rows, 0:8] = parts[h * q_rows:(h + 1) * q_rows]

    def forward_row(j):
        arrived(mir_q.at[j], dq_mir_recv.at[j])

        def send_all(to):
            for p in to:
                remote(mir_q.at[j, :, rows_of(p)], dq_o.at[j, mate], dq_send, out_recv.at[0], p)

        sent_by_me(send_all)

    def close_row(j, slot, before):
        for h in range(group):
            qd_b[j, 0, h] = (dq_a[slot, h].T * scale).astype(BF16)
        remote(qd_b.at[j, 0], mir_q.at[j], dq_mir, dq_mir_recv.at[j], mate)
        remote(qd_b.at[j, 0, :, rows_of(mate)], dq_o.at[j, me], dq_d2d, out_recv.at[0], mate)
        dq_o[j, me] = qd_b[j, 0, :, rows_of(me)]

        def send_all(to):
            for p in to:
                remote(qd_b.at[j, 0, :, rows_of(p)], dq_o.at[j, me], dq_send, out_recv.at[0], p)

        sent_by_me(send_all)

        @pl.when(before >= 0)
        def _():
            forward_row(before)

    flat_sums = [ref.reshape(2 * n_tiles * 128 // PIECE, PIECE, head_dim) for ref in (dk_a, dv_a)]
    flat_mirs = [ref.reshape(2 * n_tiles * 128 // PIECE, PIECE, head_dim) for ref in (mir_k, mir_v)]
    per_tile = TILE // PIECE

    def ship_tile(t, src_dev, mine):
        def part(p, n):
            owner = lax.div(p, pieces)
            src, dst = pl.ds(p, n), pl.ds(p - owner * pieces, n)
            on_chip = lax.div(owner, 2) == lax.div(me, 2)
            both = (lax.div(owner, inner) != outer_at) & (lax.div(lax.rem(owner, inner), 2) != lax.div(inner_at, 2))
            mine_to_send = jnp.where(both, 1, 0) == core
            for n_out, out in enumerate((dk_o, dv_o)):
                ref = (flat_sums if mine else flat_mirs)[n_out]
                if mine:
                    @pl.when(owner == me)
                    def _():
                        out[dst, src_dev] = ref[src]

                    @pl.when(owner == mate)
                    def _():
                        remote(ref.at[src], out.at[dst, src_dev], dkv_d2d.at[n_out], out_recv.at[1 + n_out], mate)

                @pl.when(jnp.logical_not(on_chip) & mine_to_send)
                def _():
                    remote(ref.at[src], out.at[dst, src_dev], dkv_send.at[n_out], out_recv.at[1 + n_out], owner)

        first = t * per_tile
        whole = lax.div(first, pieces) == lax.div(first + per_tile - 1, pieces)

        @pl.when(whole)
        def _():
            part(first, per_tile)

        @pl.when(jnp.logical_not(whole))
        def _():
            @pl.loop(0, per_tile)
            def _(i):
                part(first + i, 1)

    def close_tiles(lo, n, step, mir):
        @pl.loop(0, n)
        def _(w):
            t = lo + w * step
            for b in range(2):
                dk_a[2 * t + b] = dk_a[2 * t + b].T * scale
                dv_a[2 * t + b] = dv_a[2 * t + b].T
            for a, (src, dst) in enumerate(((dk_a, mir_k), (dv_a, mir_v))):
                remote(src.at[pl.ds(2 * t, 2)], dst.at[pl.ds(2 * t, 2)], dkv_mir.at[a], dkv_mir_recv.at[a, mir], mate)

    n_late = n_tiles - late_tile

    def column(dev, i):
        return lax.rem(dev + i, n_cols)

    def ship_column(dev, i, mine):
        @pl.loop(0, HALF)
        def _(w):
            ship_tile(column(dev, i) + w * n_cols, dev, mine)

    def ship_late(dev, n, mine):
        ship_tile(late_tile + lax.rem(n + dev, n_late), dev, mine)

    def forward_column(i):
        for a, ref in enumerate((mir_k, mir_v)):
            arrived(ref.at[pl.ds(0, 2 * HALF)], dkv_mir_recv.at[a, i])
        ship_column(mate, i, False)

    late_end = middle_row + late

    @pl.loop(0, n_segs)
    def _(i):
        j = row_at(i)
        before = jnp.where(i == 0, first_late, row_at(jnp.maximum(i - 1, 0)))
        early = j < first_late
        early_before = (before < first_late) | (i == 0)
        slot = jnp.where(early, lax.rem(j, 2), j - first_late + 2)
        old_slot = jnp.where(early_before, lax.rem(before, 2), before - first_late + 2)
        lo = jnp.where(early, 0, late_tile)
        open_row(j, slot, lax.rem(i, 2) == 0)
        n = j + 1 - lo

        def tiles(t, n):
            return [(j, slot, t + w) for w in range(n)]

        def after(t):
            return jnp.where(t == lo, old_slot, slot), jnp.where(t == lo, before + 1, t - 1)

        wide_end = lo + lax.div(n, WIDE) * WIDE
        half_end = lo + lax.div(n, HALF) * HALF

        @pl.loop(0, lax.div(n, WIDE))
        def _(c):
            t = lo + c * WIDE
            products(tiles(t, WIDE), *after(t))

        @pl.when(half_end > wide_end)
        def _():
            products(tiles(wide_end, HALF), *after(wide_end))

        for r in range(HALF):
            @pl.when(lax.rem(n, HALF) == r)
            def _():
                products(tiles(half_end, r + 1), *after(half_end), masked=True)

        @pl.when((i > 0) & early_before)
        def _():
            close_row(before, old_slot, jnp.where(i > 1, before + 1, -1))

        @pl.when(i == late_end)
        def _():
            close_tiles(late_tile, n_late, 1, n_cols)

        @pl.when(i == late_end + 1)
        def _():
            for a, ref in enumerate((mir_k, mir_v)):
                arrived(ref.at[pl.ds(0, 2 * n_late)], dkv_mir_recv.at[a, n_cols])

        @pl.when(i >= late_end)
        def _():
            turn_of = lax.div(i - late_end, 2)

            @pl.when(lax.rem(i, 2) == 0)
            def _():
                ship_late(me, turn_of, True)

            @pl.when(lax.rem(i, 2) == 1)
            def _():
                ship_late(mate, turn_of, False)

    @pl.loop(0, n_cols)
    def _(i):
        c = column(me, i)

        @pl.loop(0, late // 2)
        def _(pair):
            j = first_late + 2 * pair
            slot = 2 * pair + 2
            first = pair == 0
            middle = pair == late // 4
            last_tile = c + (HALF - 1) * n_cols
            products([(j + u, slot + u, c + w * n_cols) for u in range(2) for w in range(HALF)],
                     jnp.where(first, jnp.where(i == 0, 0, late + 1), slot - 1),
                     jnp.where(first, jnp.where(i == 0, 1, column(me, i + n_cols - 1) + (HALF - 1) * n_cols),
                               last_tile))

            @pl.when(first & (i == 0))
            def _():
                close_row(0, 0, 1)

            @pl.when(first & (i > 0))
            def _():
                close_tiles(column(me, i - 1), HALF, n_cols, i - 1)
                ship_column(me, i - 1, True)

            shipped = (n_segs - late_end) // 2

            @pl.when(first & (i < n_late - shipped))
            def _():
                ship_late(me, shipped + i, True)

            @pl.when(middle & (i > 0))
            def _():
                forward_column(i - 1)

            @pl.when(middle & (i < n_late - shipped))
            def _():
                ship_late(mate, shipped + i, False)

            @pl.when(i == n_cols - 1)
            def _():
                @pl.when(jnp.logical_not(first))
                def _():
                    close_row(j - 1, slot - 1, j - 2)

                close_row(j, slot, jnp.where(first, 0, j - 1))

    products([None], late + 1, column(me, n_cols - 1) + (HALF - 1) * n_cols)
    close_tiles(column(me, n_cols - 1), HALF, n_cols, n_cols - 1)
    close_row(n_segs - 1, late + 1, n_segs - 2)
    ship_column(me, n_cols - 1, True)
    forward_row(n_segs - 1)
    forward_column(n_cols - 1)

    wait_sent(box.at[0], box.at[0, :, half], pair_send)
    for a in range(2):
        wait_sent(mir_kv.at[a, half], mir_kv.at[a, quarter], kv_fwd.at[a])
    arrived(st_s.at[:, pl.ds(0, rest)], st_send)
    wait_sent(dq_o, dq_o.at[:, half], dq_send)
    arrived(dq_o.at[:, one], dq_d2d)
    arrived(mir_q, dq_mir)
    for a, (out, ref) in enumerate(((dk_o, dk_a), (dv_o, dv_a))):
        wait_sent(out, out.at[:, half], dkv_send.at[a])
        arrived(out.at[:, one], dkv_d2d.at[a])
        arrived(ref, dkv_mir.at[a])
    for n, ref in enumerate((dq_o, dk_o, dv_o)):
        arrived(ref.at[:, pl.ds(0, rest)], out_recv.at[n])


def ungroup_kernel(q_step, k_step, dq_i, dk_i, dv_i, dq_o, dk_o, dv_o, q_out, k_out, v_out, q_done, k_done, v_done):
    groups = ((dq_i, q_out, dq_o, q_step, q_done), (dk_i, k_out, dk_o, k_step, k_done), (dv_i, v_out, dv_o, k_step, v_done))

    for src, turned, dst, step, done in groups:
        rows, width = src.shape[-2], src.shape[-1]

        @pl.loop(0, src.shape[0] // step)
        def _(i):
            for u in range(step):
                at = pl.ds(pl.multiple_of((i * step + u) * rows, rows), rows)
                turned[at] = jnp.transpose(src[i * step + u].reshape(-1, rows, width), (1, 0, 2))
            part = pl.ds(i * step * rows, step * rows)
            pltpu.make_async_copy(turned.at[part], dst.at[part], done.at[i]).start()

    for src, turned, _, step, done in groups:
        rows = src.shape[-2]

        @pl.loop(0, src.shape[0] // step)
        def _(i):
            part = turned.at[pl.ds(i * step * rows, step * rows)]
            pltpu.make_async_copy(part, part, done.at[i]).wait()


def solution(mesh):
    outer, inner = mesh.shape["cp_outer"], mesh.shape["cp"]
    n_dev = outer * inner
    seq_spec = P(None, SEQ_AXES, "heads", None)
    stat_spec = P(None, SEQ_AXES, "heads")
    kv_spec = P(SEQ_AXES, "heads", None)

    def local_grads(q, k, v, o, do, lse):
        n_segs, q_rows, q_heads, head_dim = q.shape
        k_rows, kv_heads, _ = k.shape
        group = q_heads // kv_heads
        late = 8
        n_tiles = n_segs + 1
        n_pairs = n_segs // 2
        pieces = k_rows // PIECE
        keys = n_dev * k_rows

        def flat(x):
            return x.reshape(n_segs * q_rows, q_heads, head_dim)

        dims = (n_dev, inner, n_segs, group, q_rows, head_dim, k_rows, late)
        hbm = pl.BlockSpec(memory_space=pl.ANY)
        vmem = pltpu.VMEM
        key = vmem((keys, head_dim), BF16)
        key_t = vmem((2 * n_tiles, head_dim, 128), BF16)
        row_t = vmem((late + 2, head_dim, group * TILE), BF16)
        key_sum = vmem((2 * n_tiles, head_dim, 128), F32)
        stat = vmem((n_pairs, n_dev, 2, 256), F32)
        carried = vmem((group, TILE, TILE), BF16)
        dma = pltpu.SemaphoreType.DMA
        n_cols = (n_segs - late) // HALF
        q_out = vmem((n_segs, kv_heads, group, q_rows, head_dim), BF16)
        kv_out = vmem((pieces, kv_heads, PIECE, head_dim), F32)
        on_chip = pl.BlockSpec(memory_space=pltpu.VMEM)
        sums = jax.ShapeDtypeStruct((2 * n_tiles, 128, head_dim), F32)
        pair = (kv_heads, 2, 2, group, q_rows, head_dim)
        dq, dk, dv = pl.pallas_call(
            functools.partial(attn_kernel, dims),
            out_shape=(q_out, kv_out, kv_out,
                       jax.ShapeDtypeStruct((2, n_pairs) + pair, BF16),
                       jax.ShapeDtypeStruct((2, kv_heads, k_rows, head_dim), BF16),
                       jax.ShapeDtypeStruct((n_segs, group, TILE, head_dim), BF16), sums, sums),
            in_specs=[hbm] * 6,
            out_specs=(on_chip,) * 3 + (hbm,) * 5,
            scratch_shapes=[
                vmem((2, 3, 2 * q_rows, q_heads, head_dim), BF16),
                vmem((2, 2, CHUNK, kv_heads, head_dim), BF16),
                vmem((n_segs, q_heads, q_rows), F32),
                vmem((2,) + pair, BF16),
                vmem((kv_heads, 2, group, q_rows, head_dim), BF16),
                stat, vmem((n_segs, 2, group, TILE, head_dim), BF16), key, key, stat,
                key_t, key_t, row_t, row_t,
                vmem((late + 2, group, head_dim, TILE), F32),
                key_sum, key_sum,
                vmem((late + 2, group, TILE, head_dim), BF16), vmem((2, head_dim, TILE), BF16),
                carried, carried, vmem((3, group, TILE, TILE), BF16),
                dma((2, 3)), dma((2, 2)), dma, dma((2,)), dma((2,)), dma((n_pairs,)), dma, dma((2,)),
                dma((2,)), dma((2,)), dma((2,)), dma((2,)), dma((2,)), dma, dma, dma, dma, dma((n_segs,)),
                dma((2,)), dma((2,)), dma((2,)), dma((2, n_cols + 1)), dma((n_pairs,)), dma((2,)), dma((n_pairs,)),
                dma((3,))],
            compiler_params=pltpu.CompilerParams(
                collective_id=0, has_side_effects=True, vmem_limit_bytes=MAIN_VMEM),
            cost_estimate=pl.CostEstimate(flops=1680 * 5 * 2 * 256 * 256 * 128, bytes_accessed=64 << 20,
                                          transcendentals=1680 * 65536),
            name="attn_grads",
        )(flat(q), flat(do), flat(o), k, v, lse.transpose(0, 2, 1))[:3]

        q_step, k_step = 4, 3
        q_rows_out = jax.ShapeDtypeStruct((n_segs * q_rows, q_heads, head_dim), BF16)
        k_rows_out = jax.ShapeDtypeStruct((k_rows, kv_heads, head_dim), F32)
        q_sems, k_sems = dma((n_segs // q_step,)), dma((pieces // k_step,))
        q_turned, k_turned = vmem(q_rows_out.shape, BF16), vmem(k_rows_out.shape, F32)
        dq, dk, dv = pl.pallas_call(
            functools.partial(ungroup_kernel, q_step, k_step),
            out_shape=(q_rows_out, k_rows_out, k_rows_out),
            in_specs=[on_chip] * 3,
            out_specs=(hbm,) * 3,
            scratch_shapes=[q_turned, k_turned, k_turned, q_sems, k_sems, k_sems],
            compiler_params=pltpu.CompilerParams(vmem_limit_bytes=24 << 20),
            name="ungroup",
        )(dq, dk, dv)
        return dq.reshape(n_segs, q_rows, q_heads, head_dim), dk, dv

    return jax.shard_map(local_grads, mesh=mesh,
                         in_specs=(seq_spec, kv_spec, kv_spec, seq_spec, seq_spec, stat_spec),
                         out_specs=(seq_spec, kv_spec, kv_spec), check_vma=False)
```

```python
import functools

import jax
import jax.numpy as jnp
from jax import lax
from jax.experimental import pallas as pl
from jax.experimental.pallas import tpu as pltpu
from jax.sharding import PartitionSpec as P

MESH = pl.DeviceIdType.MESH
SEQ_AXES = ("cp_outer", "cp")
BF16 = jnp.bfloat16
F32 = jnp.float32
LOG2E = 1.4426950408889634
TILE = 256
WIDE = 8
HALF = 4
EARLY_SLOTS = 3
ORDER = "SVPKSQPVSKPQVKQ"
PIECE = 32
CHUNK = 96
MAIN_VMEM = 49 << 20


def dot(a, b, ca, cb):
    return lax.dot_general(a, b, (((ca,), (cb,)), ((), ())), preferred_element_type=F32)


def attn_kernel(dims, q_n, do_n, o_n, k_n, v_n, ls_n, dq_o, dk_o, dv_o, box, mir_kv, mir_q, mir_k, mir_v,
                nat, nat_k, ls_v, stg, o_s, st_s, qd_b, k_b, v_b, st_b,
                k_t, v_t, q_t, do_t, dq_a, dk_a, dv_a, aug, aug_k, p_c, d_c, turn,
                nat_sem, natk_sem, ls_sem, box_own, box_send, box_recv, pair_send, pair_d2d,
                kv_send, kv_fwd, kv_d2d, kv_mir, kv_mir_recv, st_send, dq_send, dq_d2d, dq_mir, dq_mir_recv,
                dkv_send, dkv_d2d, dkv_mir, dkv_mir_recv, row_recv, kv_recv, st_recv, out_recv):
    n_dev, inner, n_segs, group, q_rows, head_dim, k_rows, late = dims
    scale = head_dim ** -0.5
    outer_at, inner_at = lax.axis_index("cp_outer"), lax.axis_index("cp")
    me = outer_at * inner + inner_at
    core = lax.rem(inner_at, 2)
    mate = me + 1 - 2 * core
    n_pairs = n_segs // 2
    n_tiles = n_segs + 1
    first_late = n_segs - late
    late_tile = first_late
    n_cols = late_tile // HALF
    pieces = k_rows // PIECE
    rest = n_dev - 1
    middle_row = first_late // 2

    kv_s = [ref.reshape(n_dev, k_rows, head_dim) for ref in (k_t, v_t)]

    def chip_cores(flip_outer, flip_inner):
        y = 1 - outer_at if flip_outer else outer_at
        x = (inner - 2) - (inner_at - core) if flip_inner else inner_at - core
        return [y * inner + x + c for c in range(2)]

    along = chip_cores(False, True) + chip_cores(True, False)
    across = chip_cores(True, True)

    def sent_by_me(send_all):
        @pl.when(core == 0)
        def _():
            send_all(along)

        @pl.when(core == 1)
        def _():
            send_all(across)

    def rows_of(p):
        return pl.ds(pl.multiple_of(p * q_rows, q_rows), q_rows)

    def device(p):
        return (0, lax.div(p, inner), lax.rem(p, inner))

    def remote(src, dst, send_sem, recv_sem, p):
        pltpu.make_async_remote_copy(src_ref=src, dst_ref=dst, send_sem=send_sem, recv_sem=recv_sem,
                                     device_id=device(p), device_id_type=MESH).start()

    def arrived(ref, sem):
        pltpu.make_async_copy(ref, ref, sem).wait()

    def wait_sent(whole, half, sem):
        @pl.when(core == 0)
        def _():
            arrived(whole, sem)

        @pl.when(core == 1)
        def _():
            arrived(half, sem)

    def row_at(i):
        return jnp.where(i < middle_row, first_late - 1 - i,
                         jnp.where(i < middle_row + late, first_late - middle_row + i, n_segs - 1 - i))

    def pair_at(k):
        return lax.div(row_at(2 * k), 2)

    def fetch(k):
        r = pair_at(k)
        for a, src in enumerate((q_n, do_n, o_n)):
            pltpu.make_async_copy(src.at[pl.ds(r * 2 * q_rows, 2 * q_rows)], nat.at[lax.rem(k, 2), a],
                                  nat_sem.at[lax.rem(k, 2), a]).start()

    def fetch_keys(c):
        for a, src in enumerate((k_n, v_n)):
            pltpu.make_async_copy(src.at[pl.ds(c * CHUNK, CHUNK)], nat_k.at[lax.rem(c, 2), a],
                                  natk_sem.at[lax.rem(c, 2), a]).start()

    def send_keys(src, owner, lo, n, sem):
        rows = pl.ds(lo, n)
        dst = pl.ds(pl.multiple_of(owner * k_rows + lo, 32), n)

        def send_all(to):
            for p in to:
                for a, land in enumerate((k_b, v_b)):
                    remote(src[a].at[p, rows], land.at[dst], sem.at[a], kv_recv.at[a], p)

        sent_by_me(send_all)

    def stage_keys(first, n):
        @pl.loop(first, first + n)
        def _(c):
            buf = lax.rem(c, 2)
            rows = pl.ds(pl.multiple_of(c * CHUNK, CHUNK), CHUNK)
            dst = pl.ds(pl.multiple_of(me * k_rows + c * CHUNK, 32), CHUNK)
            for a in range(2):
                arrived(nat_k.at[buf, a], natk_sem.at[buf, a])

            @pl.when(c + 1 < k_rows // CHUNK)
            def _():
                fetch_keys(c + 1)

            for a, land in enumerate((k_b, v_b)):
                block = jnp.transpose(nat_k[buf, a], (1, 0, 2))
                kv_s[a][:, rows] = block
                land[dst, :] = kv_s[a][me, rows]

    def ship_keys(first, n):
        lo, rows = first * CHUNK, n * CHUNK
        send_keys(kv_s, me, lo, rows, kv_send)
        src = pl.ds(lo, rows)
        dst = pl.ds(pl.multiple_of(me * k_rows + lo, 32), rows)
        for a, land in enumerate((k_b, v_b)):
            remote(kv_s[a].at[mate, src], land.at[dst], kv_d2d.at[a], kv_recv.at[a], mate)
            remote(kv_s[a].at[:, src], mir_kv.at[a, :, src], kv_mir.at[a], kv_mir_recv.at[a], mate)

    def forward_keys():
        for a in range(2):
            arrived(mir_kv.at[a], kv_mir_recv.at[a])
        send_keys([mir_kv.at[a] for a in range(2)], mate, 0, k_rows, kv_fwd)

    def stage_pair(k):
        buf = lax.rem(k, 2)
        r = pair_at(k)
        for a in range(3):
            arrived(nat.at[buf, a], nat_sem.at[buf, a])

        @pl.when(k + 1 < n_pairs)
        def _():
            fetch(k + 1)

        for u in range(4):
            half = slice(16 * (u % 2), 16 * (u % 2) + 16)
            for a in range(3):
                block = jnp.transpose(nat[buf, a, 16 * u:16 * u + 16], (1, 0, 2)).reshape(n_dev, group, 16, head_dim)
                if a < 2:
                    stg[buf, :, u // 2, a, :, half] = block
                else:
                    o_s[:, u // 2, :, half] = block
        segs = pl.ds(2 * r, 2)
        for s in range(2):
            qd_b[2 * r + s, :, :, rows_of(me)] = stg[buf, me, s]
        pltpu.make_async_copy(stg.at[buf], box.at[core, k], box_own.at[buf]).start()
        remote(stg.at[buf], box.at[core, k], box_send.at[buf], box_recv.at[k], mate)
        remote(stg.at[buf, mate], qd_b.at[segs, :, :, rows_of(me)], pair_d2d.at[buf], row_recv.at[r], mate)

        ones = jnp.ones((8, head_dim), BF16)
        rows = group * q_rows
        blank = jnp.zeros((1, 128 - rows), F32)
        for p in range(n_dev):
            for s in range(2):
                prod = (stg[buf, p, s, 1].reshape(rows, head_dim).astype(F32)
                        * o_s[p, s].reshape(rows, head_dim).astype(F32))
                hi = prod.astype(BF16)
                prod = prod - hi.astype(F32)
                mid = prod.astype(BF16)
                low = (prod - mid.astype(F32)).astype(BF16)
                delta = (dot(ones, hi, 1, 1) + dot(ones, mid, 1, 1)) + dot(ones, low, 1, 1)
                lse = [ls_v[2 * r + s, p * group + h:p * group + h + 1, :] for h in range(group)]
                st_s[r, p, 0:1, 128 * s:128 * s + 128] = jnp.concatenate([delta[0:1], blank], 1)
                st_s[r, p, 1:2, 128 * s:128 * s + 128] = jnp.concatenate(lse + [blank], 1) * (1 / scale)
        st_b[r, me] = st_s[r, me]
        for p in along + across + [mate]:
            remote(st_s.at[r, p], st_b.at[r, me], st_send, st_recv.at[r], p)

    def ship_pair(k):
        buf = lax.rem(k, 2)
        r = pair_at(k)
        segs = pl.ds(2 * r, 2)
        arrived(stg.at[buf], box_own.at[buf])
        arrived(stg.at[buf], box_send.at[buf])
        arrived(stg.at[buf, 0], pair_d2d.at[buf])
        arrived(box.at[0, k], box_recv.at[k])

        def send_all(to):
            for src in range(2):
                for p in to:
                    remote(box.at[src, k, p], qd_b.at[segs, :, :, rows_of(me - core + src)], pair_send, row_recv.at[r], p)

        sent_by_me(send_all)

    pltpu.make_async_copy(ls_n, ls_v, ls_sem).start()
    fetch_keys(0)
    fetch(0)
    barrier = pltpu.get_barrier_semaphore()
    for p in along + across + [mate]:
        pl.semaphore_signal(barrier, inc=1, device_id=device(p), device_id_type=MESH)
    chunks = k_rows // CHUNK
    stage_keys(0, 2)
    pl.semaphore_wait(barrier, rest)
    ship_keys(0, 2)
    stage_keys(2, chunks - 2)
    ship_keys(2, chunks - 2)
    arrived(ls_v, ls_sem)

    @pl.loop(0, n_pairs)
    def _(k):
        stage_pair(k)

        @pl.when(k == 1)
        def _():
            forward_keys()

        @pl.when(k > 0)
        def _():
            ship_pair(k - 1)

    ship_pair(n_pairs - 1)

    @pl.loop(0, 2 * n_tiles)
    def _(i):
        dk_a[i] = jnp.zeros((head_dim, 128), F32)
        dv_a[i] = jnp.zeros((head_dim, 128), F32)

    unused = EARLY_SLOTS - 1
    q_t[unused] = jnp.zeros(q_t.shape[1:], BF16)
    do_t[unused] = jnp.zeros(do_t.shape[1:], BF16)
    dq_a[unused] = jnp.zeros(dq_a.shape[1:], F32)
    p_c[...] = jnp.zeros(p_c.shape, BF16)
    d_c[...] = jnp.zeros(d_c.shape, BF16)
    turn[1] = jnp.zeros(turn.shape[1:], BF16)
    aug[...] = jnp.zeros(aug.shape, BF16)
    place = lax.broadcasted_iota(jnp.int32, (head_dim, TILE), 0)
    for a in range(2):
        aug_k[a] = jnp.where((place < 6) & (lax.rem(place, 2) == 1 - a), -1.0, 0.0).astype(BF16)

    for a, land in enumerate((k_b, v_b)):
        arrived(land.at[pl.ds(0, rest * k_rows)], kv_recv.at[a])

    half = pl.ds(0, n_dev // 2)
    quarter = pl.ds(0, n_dev // 4)
    one = pl.ds(0, 1)
    for a in range(2):
        wait_sent(kv_s[a].at[half], kv_s[a].at[quarter], kv_send.at[a])
        arrived(kv_s[a].at[one], kv_d2d.at[a])
        arrived(kv_s[a], kv_mir.at[a])

    @pl.loop(0, n_tiles)
    def _(t):
        for b in range(2):
            rows = pl.ds(pl.multiple_of(t * TILE + b * 128, 128), 128)
            k_t[2 * t + b] = k_b[rows, :].T
            v_t[2 * t + b] = v_b[rows, :].T

    def tile_of(ref, t):
        return jnp.concatenate([ref[2 * t], ref[2 * t + 1]], 1)

    def products(items, old_slot, old_tile, masked=False, last=None):
        n = len(items)
        old = [(p_c[h], d_c[h]) for h in range(group)]
        old_turn = 1
        for w, item in enumerate(items):
            new = [None] * group
            new_turn = 1 if w == n - 1 else 0 if (n - 1 - w) % 2 else 2
            sums = {"V": None, "K": None}
            raw = {"S": [None] * group, "P": [None] * group}
            count = dict.fromkeys("SPVKQ", 0)
            kept = [turn[old_turn, h] for h in range(group)] if new_turn == old_turn else None
            for step in ORDER:
                h = count[step]
                count[step] += 1
                if step in "SP":
                    if item is None:
                        continue
                    j, slot, t = item
                    a = "SP".index(step)
                    rows = jnp.concatenate([qd_b[j, a, h], aug[slot, h]], 1)
                    cols = jnp.concatenate([tile_of((k_t, v_t)[a], t), aug_k[a]], 0)
                    raw[step][h] = dot(rows, cols, 1, 0)
                    if raw["S"][h] is not None and raw["P"][h] is not None:
                        p = jnp.exp2(raw["S"][h] * (scale * LOG2E))
                        if masked and w == n - 1:
                            visible = (lax.broadcasted_iota(jnp.int32, (TILE, TILE), 0)
                                       >= lax.broadcasted_iota(jnp.int32, (TILE, TILE), 1))
                            p = jnp.where(visible, p, 0.0)
                        ds = (p * raw["P"][h]).astype(BF16)
                        new[h] = (p.astype(BF16), ds)
                        turn[new_turn, h] = ds.T
                elif step == "Q":
                    right = turn[old_turn, h] if kept is None else kept[h]
                    dq_a[old_slot, h] += dot(tile_of(k_t, old_tile), right, 1, 0)
                else:
                    lanes = slice(h * TILE, (h + 1) * TILE)
                    left = (do_t if step == "V" else q_t)[old_slot, :, lanes]
                    part = dot(left, old[h]["VK".index(step)], 1, 0)
                    sums[step] = part if sums[step] is None else sums[step] + part
            for acc, total in ((dv_a, sums["V"]), (dk_a, sums["K"])):
                acc[2 * old_tile] += total[:, :128]
                acc[2 * old_tile + 1] += total[:, 128:]
            if item is None:
                return
            old, old_turn, old_slot, old_tile = new, new_turn, slot, t
        for h in range(group):
            p_c[h], d_c[h] = old[h]
        if last is not None:
            last()

    def await_pair(i):
        @pl.when((lax.rem(i, 2) == 0) & (i < n_segs))
        def _():
            pair = pair_at(lax.div(i, 2))
            arrived(qd_b.at[pl.ds(2 * pair, 2), :, :, pl.ds(0, rest * q_rows)], row_recv.at[pair])
            arrived(st_b.at[pair, pl.ds(0, rest)], st_recv.at[pair])

    def open_row(j, slot):
        pair, s = lax.div(j, 2), lax.rem(j, 2)
        q_t[slot] = qd_b[j, 0].reshape(group * TILE, head_dim).T
        do_t[slot] = qd_b[j, 1].reshape(group * TILE, head_dim).T
        dq_a[slot] = jnp.zeros((group, head_dim, TILE), F32)
        for b in range(n_dev):
            stats = st_b[pair, b, :, pl.ds(pl.multiple_of(s * 128, 128), 128)]
            hi = stats.astype(BF16).astype(F32)
            mid = (stats - hi).astype(BF16).astype(F32)
            parts = jnp.concatenate([hi, mid, (stats - hi) - mid, jnp.zeros((2, 128), F32)], 0).T.astype(BF16)
            for h in range(group):
                aug[slot, h, b * q_rows:(b + 1) * q_rows, 0:8] = parts[h * q_rows:(h + 1) * q_rows]

    def forward_row(j):
        arrived(mir_q.at[j], dq_mir_recv.at[j])

        def send_all(to):
            for p in to:
                remote(mir_q.at[j, :, rows_of(p)], dq_o.at[j, mate], dq_send, out_recv.at[0], p)

        sent_by_me(send_all)

    def round_row(j, slot):
        for h in range(group):
            qd_b[j, 0, h] = (dq_a[slot, h].T * scale).astype(BF16)

    def close_row(j, before):
        remote(qd_b.at[j, 0], mir_q.at[j], dq_mir, dq_mir_recv.at[j], mate)
        remote(qd_b.at[j, 0, :, rows_of(mate)], dq_o.at[j, me], dq_d2d, out_recv.at[0], mate)
        dq_o[j, me] = qd_b[j, 0, :, rows_of(me)]

        def send_all(to):
            for p in to:
                remote(qd_b.at[j, 0, :, rows_of(p)], dq_o.at[j, me], dq_send, out_recv.at[0], p)

        sent_by_me(send_all)

        @pl.when(before >= 0)
        def _():
            forward_row(before)

    flat_sums = [ref.reshape(2 * n_tiles * 128 // PIECE, PIECE, head_dim) for ref in (dk_a, dv_a)]
    flat_mirs = [ref.reshape(2 * n_tiles * 128 // PIECE, PIECE, head_dim) for ref in (mir_k, mir_v)]
    per_tile = TILE // PIECE

    def ship_tile(t, src_dev, mine):
        def part(p, n):
            owner = lax.div(p, pieces)
            src, dst = pl.ds(p, n), pl.ds(p - owner * pieces, n)
            on_chip = lax.div(owner, 2) == lax.div(me, 2)
            both = (lax.div(owner, inner) != outer_at) & (lax.div(lax.rem(owner, inner), 2) != lax.div(inner_at, 2))
            mine_to_send = jnp.where(both, 1, 0) == core
            for n_out, out in enumerate((dk_o, dv_o)):
                ref = (flat_sums if mine else flat_mirs)[n_out]
                if mine:
                    @pl.when(owner == me)
                    def _():
                        out[dst, src_dev] = ref[src]

                    @pl.when(owner == mate)
                    def _():
                        remote(ref.at[src], out.at[dst, src_dev], dkv_d2d.at[n_out], out_recv.at[1 + n_out], mate)

                @pl.when(jnp.logical_not(on_chip) & mine_to_send)
                def _():
                    remote(ref.at[src], out.at[dst, src_dev], dkv_send.at[n_out], out_recv.at[1 + n_out], owner)

        first = t * per_tile
        whole = lax.div(first, pieces) == lax.div(first + per_tile - 1, pieces)

        @pl.when(whole)
        def _():
            part(first, per_tile)

        @pl.when(jnp.logical_not(whole))
        def _():
            @pl.loop(0, per_tile)
            def _(i):
                part(first + i, 1)

    def close_tiles(lo, n, step, mir):
        @pl.loop(0, n)
        def _(w):
            t = lo + w * step
            for b in range(2):
                dk_a[2 * t + b] = dk_a[2 * t + b].T * scale
                dv_a[2 * t + b] = dv_a[2 * t + b].T
            for a, (src, dst) in enumerate(((dk_a, mir_k), (dv_a, mir_v))):
                remote(src.at[pl.ds(2 * t, 2)], dst.at[pl.ds(2 * t, 2)], dkv_mir.at[a], dkv_mir_recv.at[a, mir], mate)

    n_late = n_tiles - late_tile

    def column(dev, i):
        return lax.rem(dev + i, n_cols)

    def ship_column(dev, i, mine):
        @pl.loop(0, HALF)
        def _(w):
            ship_tile(column(dev, i) + w * n_cols, dev, mine)

    def ship_late(dev, n, mine):
        ship_tile(late_tile + lax.rem(n + dev, n_late), dev, mine)

    def forward_column(i):
        for a, ref in enumerate((mir_k, mir_v)):
            arrived(ref.at[pl.ds(0, 2 * HALF)], dkv_mir_recv.at[a, i])
        ship_column(mate, i, False)

    late_end = middle_row + late
    late_slot = EARLY_SLOTS + late - 1

    def slot_at(i):
        early_index = jnp.where(i < middle_row, i, i - late)
        return jnp.where((i >= middle_row) & (i < late_end), i - middle_row + EARLY_SLOTS,
                         lax.rem(early_index + EARLY_SLOTS, EARLY_SLOTS))

    await_pair(0)
    open_row(first_late - 1, 0)

    @pl.loop(0, n_segs)
    def _(i):
        j, slot = row_at(i), slot_at(i)
        before = jnp.where(i == 0, first_late, row_at(jnp.maximum(i - 1, 0)))
        early_before = (before < first_late) | (i == 0)
        old_slot = jnp.where(i == 0, unused, slot_at(i - 1))
        lo = jnp.where(j < first_late, 0, late_tile)
        closes = (i > 0) & early_before
        n = j + 1 - lo

        def tiles(t, n):
            return [(j, slot, t + w) for w in range(n)]

        def after(t):
            return jnp.where(t == lo, old_slot, slot), jnp.where(t == lo, before + 1, t - 1)

        @pl.loop(0, lax.div(n, WIDE))
        def _(c):
            t = lo + c * WIDE
            products(tiles(t, WIDE), *after(t))

        await_pair(i + 1)
        coming = jnp.minimum(i + 1, n_segs - 1)
        wide_end = lo + lax.div(n, WIDE) * WIDE
        for r in range(WIDE):
            @pl.when(lax.rem(n, WIDE) == r)
            def _():
                products(tiles(wide_end, r + 1), *after(wide_end), masked=True,
                         last=lambda: open_row(row_at(coming), slot_at(i + 1)))

        @pl.when(closes)
        def _():
            round_row(before, old_slot)
            close_row(before, jnp.where(i > 1, before + 1, -1))

        @pl.when(i == late_end)
        def _():
            close_tiles(late_tile, n_late, 1, n_cols)

        @pl.when(i == late_end + 1)
        def _():
            for a, ref in enumerate((mir_k, mir_v)):
                arrived(ref.at[pl.ds(0, 2 * n_late)], dkv_mir_recv.at[a, n_cols])

        @pl.when(i >= late_end)
        def _():
            turn_of = lax.div(i - late_end, 2)

            @pl.when(lax.rem(i, 2) == 0)
            def _():
                ship_late(me, turn_of, True)

            @pl.when(lax.rem(i, 2) == 1)
            def _():
                ship_late(mate, turn_of, False)

    @pl.loop(0, n_cols)
    def _(i):
        c = column(me, i)

        @pl.loop(0, late // 2)
        def _(pair):
            j = first_late + 2 * pair
            slot = 2 * pair + EARLY_SLOTS
            first = pair == 0
            middle = pair == late // 4
            last_tile = c + (HALF - 1) * n_cols
            products([(j + u, slot + u, c + w * n_cols) for u in range(2) for w in range(HALF)],
                     jnp.where(first, jnp.where(i == 0, slot_at(n_segs - 1), late_slot), slot - 1),
                     jnp.where(first, jnp.where(i == 0, 1, column(me, i + n_cols - 1) + (HALF - 1) * n_cols),
                               last_tile))

            @pl.when(first & (i == 0))
            def _():
                round_row(0, slot_at(n_segs - 1))
                close_row(0, 1)

            @pl.when(first & (i > 0))
            def _():
                close_tiles(column(me, i - 1), HALF, n_cols, i - 1)
                ship_column(me, i - 1, True)

            shipped = (n_segs - late_end) // 2

            @pl.when(first & (i < n_late - shipped))
            def _():
                ship_late(me, shipped + i, True)

            @pl.when(middle & (i > 0))
            def _():
                forward_column(i - 1)

            @pl.when(middle & (i < n_late - shipped))
            def _():
                ship_late(mate, shipped + i, False)

            @pl.when(i == n_cols - 1)
            def _():
                @pl.when(jnp.logical_not(first))
                def _():
                    round_row(j - 1, slot - 1)
                    close_row(j - 1, j - 2)

                round_row(j, slot)
                close_row(j, jnp.where(first, 0, j - 1))

    products([None], late_slot, column(me, n_cols - 1) + (HALF - 1) * n_cols)
    close_tiles(column(me, n_cols - 1), HALF, n_cols, n_cols - 1)
    round_row(n_segs - 1, late_slot)
    close_row(n_segs - 1, n_segs - 2)
    ship_column(me, n_cols - 1, True)
    forward_row(n_segs - 1)
    forward_column(n_cols - 1)

    wait_sent(box.at[0], box.at[0, :, half], pair_send)
    for a in range(2):
        wait_sent(mir_kv.at[a, half], mir_kv.at[a, quarter], kv_fwd.at[a])
    arrived(st_s.at[:, pl.ds(0, rest)], st_send)
    wait_sent(dq_o, dq_o.at[:, half], dq_send)
    arrived(dq_o.at[:, one], dq_d2d)
    arrived(mir_q, dq_mir)
    for a, (out, ref) in enumerate(((dk_o, dk_a), (dv_o, dv_a))):
        wait_sent(out, out.at[:, half], dkv_send.at[a])
        arrived(out.at[:, one], dkv_d2d.at[a])
        arrived(ref, dkv_mir.at[a])
    for n, ref in enumerate((dq_o, dk_o, dv_o)):
        arrived(ref.at[:, pl.ds(0, rest)], out_recv.at[n])


def ungroup_kernel(q_step, k_step, dq_i, dk_i, dv_i, dq_o, dk_o, dv_o, q_out, k_out, v_out, q_done, k_done, v_done):
    groups = ((dq_i, q_out, dq_o, q_step, q_done), (dk_i, k_out, dk_o, k_step, k_done), (dv_i, v_out, dv_o, k_step, v_done))

    for src, turned, dst, step, done in groups:
        rows, width = src.shape[-2], src.shape[-1]

        @pl.loop(0, src.shape[0] // step)
        def _(i):
            for u in range(step):
                at = pl.ds(pl.multiple_of((i * step + u) * rows, rows), rows)
                turned[at] = jnp.transpose(src[i * step + u].reshape(-1, rows, width), (1, 0, 2))
            part = pl.ds(i * step * rows, step * rows)
            pltpu.make_async_copy(turned.at[part], dst.at[part], done.at[i]).start()

    for src, turned, _, step, done in groups:
        rows = src.shape[-2]

        @pl.loop(0, src.shape[0] // step)
        def _(i):
            part = turned.at[pl.ds(i * step * rows, step * rows)]
            pltpu.make_async_copy(part, part, done.at[i]).wait()


def solution(mesh):
    outer, inner = mesh.shape["cp_outer"], mesh.shape["cp"]
    n_dev = outer * inner
    seq_spec = P(None, SEQ_AXES, "heads", None)
    stat_spec = P(None, SEQ_AXES, "heads")
    kv_spec = P(SEQ_AXES, "heads", None)

    def local_grads(q, k, v, o, do, lse):
        n_segs, q_rows, q_heads, head_dim = q.shape
        k_rows, kv_heads, _ = k.shape
        group = q_heads // kv_heads
        late = 8
        n_tiles = n_segs + 1
        n_pairs = n_segs // 2
        pieces = k_rows // PIECE
        keys = n_dev * k_rows

        def flat(x):
            return x.reshape(n_segs * q_rows, q_heads, head_dim)

        dims = (n_dev, inner, n_segs, group, q_rows, head_dim, k_rows, late)
        hbm = pl.BlockSpec(memory_space=pl.ANY)
        vmem = pltpu.VMEM
        key = vmem((keys, head_dim), BF16)
        key_t = vmem((2 * n_tiles, head_dim, 128), BF16)
        row_t = vmem((late + EARLY_SLOTS, head_dim, group * TILE), BF16)
        key_sum = vmem((2 * n_tiles, head_dim, 128), F32)
        stat = vmem((n_pairs, n_dev, 2, 256), F32)
        carried = vmem((group, TILE, TILE), BF16)
        dma = pltpu.SemaphoreType.DMA
        n_cols = (n_segs - late) // HALF
        q_out = vmem((n_segs, kv_heads, group, q_rows, head_dim), BF16)
        kv_out = vmem((pieces, kv_heads, PIECE, head_dim), F32)
        on_chip = pl.BlockSpec(memory_space=pltpu.VMEM)
        sums = jax.ShapeDtypeStruct((2 * n_tiles, 128, head_dim), F32)
        pair = (kv_heads, 2, 2, group, q_rows, head_dim)
        dq, dk, dv = pl.pallas_call(
            functools.partial(attn_kernel, dims),
            out_shape=(q_out, kv_out, kv_out,
                       jax.ShapeDtypeStruct((2, n_pairs) + pair, BF16),
                       jax.ShapeDtypeStruct((2, kv_heads, k_rows, head_dim), BF16),
                       jax.ShapeDtypeStruct((n_segs, group, TILE, head_dim), BF16), sums, sums),
            in_specs=[hbm] * 6,
            out_specs=(on_chip,) * 3 + (hbm,) * 5,
            scratch_shapes=[
                vmem((2, 3, 2 * q_rows, q_heads, head_dim), BF16),
                vmem((2, 2, CHUNK, kv_heads, head_dim), BF16),
                vmem((n_segs, q_heads, q_rows), F32),
                vmem((2,) + pair, BF16),
                vmem((kv_heads, 2, group, q_rows, head_dim), BF16),
                stat, vmem((n_segs, 2, group, TILE, head_dim), BF16), key, key, stat,
                key_t, key_t, row_t, row_t,
                vmem((late + EARLY_SLOTS, group, head_dim, TILE), F32),
                key_sum, key_sum,
                vmem((late + EARLY_SLOTS, group, TILE, head_dim), BF16), vmem((2, head_dim, TILE), BF16),
                carried, carried, vmem((3, group, TILE, TILE), BF16),
                dma((2, 3)), dma((2, 2)), dma, dma((2,)), dma((2,)), dma((n_pairs,)), dma, dma((2,)),
                dma((2,)), dma((2,)), dma((2,)), dma((2,)), dma((2,)), dma, dma, dma, dma, dma((n_segs,)),
                dma((2,)), dma((2,)), dma((2,)), dma((2, n_cols + 1)), dma((n_pairs,)), dma((2,)), dma((n_pairs,)),
                dma((3,))],
            compiler_params=pltpu.CompilerParams(
                collective_id=0, has_side_effects=True, vmem_limit_bytes=MAIN_VMEM),
            cost_estimate=pl.CostEstimate(flops=1680 * 5 * 2 * 256 * 256 * 128, bytes_accessed=64 << 20,
                                          transcendentals=1680 * 65536),
            name="attn_grads",
        )(flat(q), flat(do), flat(o), k, v, lse.transpose(0, 2, 1))[:3]

        q_step, k_step = 4, 3
        q_rows_out = jax.ShapeDtypeStruct((n_segs * q_rows, q_heads, head_dim), BF16)
        k_rows_out = jax.ShapeDtypeStruct((k_rows, kv_heads, head_dim), F32)
        q_sems, k_sems = dma((n_segs // q_step,)), dma((pieces // k_step,))
        q_turned, k_turned = vmem(q_rows_out.shape, BF16), vmem(k_rows_out.shape, F32)
        dq, dk, dv = pl.pallas_call(
            functools.partial(ungroup_kernel, q_step, k_step),
            out_shape=(q_rows_out, k_rows_out, k_rows_out),
            in_specs=[on_chip] * 3,
            out_specs=(hbm,) * 3,
            scratch_shapes=[q_turned, k_turned, k_turned, q_sems, k_sems, k_sems],
            compiler_params=pltpu.CompilerParams(vmem_limit_bytes=24 << 20),
            name="ungroup",
        )(dq, dk, dv)
        return dq.reshape(n_segs, q_rows, q_heads, head_dim), dk, dv

    return jax.shard_map(local_grads, mesh=mesh,
                         in_specs=(seq_spec, kv_spec, kv_spec, seq_spec, seq_spec, stat_spec),
                         out_specs=(seq_spec, kv_spec, kv_spec), check_vma=False)
```

```python
import functools

import jax
import jax.numpy as jnp
from jax import lax
from jax.experimental import pallas as pl
from jax.experimental.pallas import tpu as pltpu
from jax.sharding import PartitionSpec as P

MESH = pl.DeviceIdType.MESH
SEQ_AXES = ("cp_outer", "cp")
BF16 = jnp.bfloat16
F32 = jnp.float32
LOG2E = 1.4426950408889634
TILE = 256
WIDE = 8
HALF = 4
EARLY_SLOTS = 3
ORDER = "SVPKSQPVSKPQVKQ"
PIECE = 32
CHUNK = 96
MAIN_VMEM = 49 << 20


def dot(a, b, ca, cb):
    return lax.dot_general(a, b, (((ca,), (cb,)), ((), ())), preferred_element_type=F32)


def attn_kernel(dims, q_n, do_n, o_n, k_n, v_n, ls_n, dq_o, dk_o, dv_o, box, mir_kv, mir_q, mir_k, mir_v,
                nat, nat_k, ls_v, stg, o_s, st_s, qd_b, k_b, v_b, st_b,
                k_t, v_t, q_t, do_t, dq_a, dk_a, dv_a, aug, aug_k, p_c, d_c, turn,
                nat_sem, natk_sem, ls_sem, box_own, box_send, box_recv, pair_send, pair_d2d,
                kv_send, kv_fwd, kv_d2d, kv_mir, kv_mir_recv, st_send, dq_send, dq_d2d, dq_mir, dq_mir_recv,
                dkv_send, dkv_d2d, dkv_mir, dkv_mir_recv, row_recv, kv_recv, st_recv, out_recv):
    n_dev, inner, n_segs, group, q_rows, head_dim, k_rows, late = dims
    scale = head_dim ** -0.5
    outer_at, inner_at = lax.axis_index("cp_outer"), lax.axis_index("cp")
    me = outer_at * inner + inner_at
    core = lax.rem(inner_at, 2)
    mate = me + 1 - 2 * core
    n_pairs = n_segs // 2
    n_tiles = n_segs + 1
    first_late = n_segs - late
    late_tile = first_late
    n_cols = late_tile // HALF
    pieces = k_rows // PIECE
    rest = n_dev - 1
    middle_row = first_late // 2

    kv_s = [ref.reshape(n_dev, k_rows, head_dim) for ref in (k_t, v_t)]

    def chip_cores(flip_outer, flip_inner):
        y = 1 - outer_at if flip_outer else outer_at
        x = (inner - 2) - (inner_at - core) if flip_inner else inner_at - core
        return [y * inner + x + c for c in range(2)]

    along = chip_cores(False, True) + chip_cores(True, False)
    across = chip_cores(True, True)

    def sent_by_me(send_all):
        @pl.when(core == 0)
        def _():
            send_all(along)

        @pl.when(core == 1)
        def _():
            send_all(across)

    def rows_of(p):
        return pl.ds(pl.multiple_of(p * q_rows, q_rows), q_rows)

    def device(p):
        return (0, lax.div(p, inner), lax.rem(p, inner))

    def remote(src, dst, send_sem, recv_sem, p):
        pltpu.make_async_remote_copy(src_ref=src, dst_ref=dst, send_sem=send_sem, recv_sem=recv_sem,
                                     device_id=device(p), device_id_type=MESH).start()

    def arrived(ref, sem):
        pltpu.make_async_copy(ref, ref, sem).wait()

    def wait_sent(whole, half, sem):
        @pl.when(core == 0)
        def _():
            arrived(whole, sem)

        @pl.when(core == 1)
        def _():
            arrived(half, sem)

    def row_at(i):
        return jnp.where(i < middle_row, first_late - 1 - i,
                         jnp.where(i < middle_row + late, first_late - middle_row + i, n_segs - 1 - i))

    def pair_at(k):
        return lax.div(row_at(2 * k), 2)

    def fetch(k):
        r = pair_at(k)
        for a, src in enumerate((q_n, do_n, o_n)):
            pltpu.make_async_copy(src.at[pl.ds(r * 2 * q_rows, 2 * q_rows)], nat.at[lax.rem(k, 2), a],
                                  nat_sem.at[lax.rem(k, 2), a]).start()

    def fetch_keys(c):
        for a, src in enumerate((k_n, v_n)):
            pltpu.make_async_copy(src.at[pl.ds(c * CHUNK, CHUNK)], nat_k.at[lax.rem(c, 2), a],
                                  natk_sem.at[lax.rem(c, 2), a]).start()

    def send_keys(src, owner, lo, n, sem):
        rows = pl.ds(lo, n)
        dst = pl.ds(pl.multiple_of(owner * k_rows + lo, 32), n)

        def send_all(to):
            for p in to:
                for a, land in enumerate((k_b, v_b)):
                    remote(src[a].at[p, rows], land.at[dst], sem.at[a], kv_recv.at[a], p)

        sent_by_me(send_all)

    def stage_keys(first, n):
        @pl.loop(first, first + n)
        def _(c):
            buf = lax.rem(c, 2)
            rows = pl.ds(pl.multiple_of(c * CHUNK, CHUNK), CHUNK)
            dst = pl.ds(pl.multiple_of(me * k_rows + c * CHUNK, 32), CHUNK)
            for a in range(2):
                arrived(nat_k.at[buf, a], natk_sem.at[buf, a])

            @pl.when(c + 1 < k_rows // CHUNK)
            def _():
                fetch_keys(c + 1)

            for a, land in enumerate((k_b, v_b)):
                block = jnp.transpose(nat_k[buf, a], (1, 0, 2))
                kv_s[a][:, rows] = block
                land[dst, :] = kv_s[a][me, rows]

    def ship_keys(first, n):
        lo, rows = first * CHUNK, n * CHUNK
        send_keys(kv_s, me, lo, rows, kv_send)
        src = pl.ds(lo, rows)
        dst = pl.ds(pl.multiple_of(me * k_rows + lo, 32), rows)
        for a, land in enumerate((k_b, v_b)):
            remote(kv_s[a].at[mate, src], land.at[dst], kv_d2d.at[a], kv_recv.at[a], mate)
            remote(kv_s[a].at[:, src], mir_kv.at[a, :, src], kv_mir.at[a], kv_mir_recv.at[a], mate)

    def forward_keys():
        for a in range(2):
            arrived(mir_kv.at[a], kv_mir_recv.at[a])
        send_keys([mir_kv.at[a] for a in range(2)], mate, 0, k_rows, kv_fwd)

    def stage_pair(k):
        buf = lax.rem(k, 2)
        r = pair_at(k)
        for a in range(3):
            arrived(nat.at[buf, a], nat_sem.at[buf, a])

        @pl.when(k + 1 < n_pairs)
        def _():
            fetch(k + 1)

        for u in range(4):
            half = slice(16 * (u % 2), 16 * (u % 2) + 16)
            for a in range(3):
                block = jnp.transpose(nat[buf, a, 16 * u:16 * u + 16], (1, 0, 2)).reshape(n_dev, group, 16, head_dim)
                if a < 2:
                    stg[buf, :, u // 2, a, :, half] = block
                else:
                    o_s[:, u // 2, :, half] = block
        for s in range(2):
            qd_b[2 * r + s, :, :, rows_of(me)] = stg[buf, me, s]
        pltpu.make_async_copy(stg.at[buf], box.at[core, k], box_own.at[buf]).start()
        remote(stg.at[buf], box.at[core, k], box_send.at[buf], box_recv.at[k], mate)
        for u in range(2):
            j = row_at(2 * k + u)
            remote(stg.at[buf, mate, lax.rem(j, 2)], qd_b.at[j, :, :, rows_of(me)], pair_d2d.at[buf], row_recv.at[j], mate)

        ones = jnp.ones((8, head_dim), BF16)
        rows = group * q_rows
        blank = jnp.zeros((1, 128 - rows), F32)
        for p in range(n_dev):
            for s in range(2):
                prod = (stg[buf, p, s, 1].reshape(rows, head_dim).astype(F32)
                        * o_s[p, s].reshape(rows, head_dim).astype(F32))
                hi = prod.astype(BF16)
                prod = prod - hi.astype(F32)
                mid = prod.astype(BF16)
                low = (prod - mid.astype(F32)).astype(BF16)
                delta = (dot(ones, hi, 1, 1) + dot(ones, mid, 1, 1)) + dot(ones, low, 1, 1)
                lse = [ls_v[2 * r + s, p * group + h:p * group + h + 1, :] for h in range(group)]
                st_s[r, p, 0:1, 128 * s:128 * s + 128] = jnp.concatenate([delta[0:1], blank], 1)
                st_s[r, p, 1:2, 128 * s:128 * s + 128] = jnp.concatenate(lse + [blank], 1) * (1 / scale)
        st_b[r, me] = st_s[r, me]
        for p in along + across + [mate]:
            remote(st_s.at[r, p], st_b.at[r, me], st_send, st_recv.at[r], p)

    def ship_pair(k):
        buf = lax.rem(k, 2)
        arrived(stg.at[buf], box_own.at[buf])
        arrived(stg.at[buf], box_send.at[buf])
        arrived(stg.at[buf, 0], pair_d2d.at[buf])
        arrived(box.at[0, k], box_recv.at[k])

        def send_all(to):
            for u in range(2):
                j = row_at(2 * k + u)
                for src in range(2):
                    for p in to:
                        remote(box.at[src, k, p, lax.rem(j, 2)], qd_b.at[j, :, :, rows_of(me - core + src)],
                               pair_send, row_recv.at[j], p)

        sent_by_me(send_all)

    pltpu.make_async_copy(ls_n, ls_v, ls_sem).start()
    fetch_keys(0)
    fetch(0)
    barrier = pltpu.get_barrier_semaphore()
    for p in along + across + [mate]:
        pl.semaphore_signal(barrier, inc=1, device_id=device(p), device_id_type=MESH)
    chunks = k_rows // CHUNK
    stage_keys(0, 2)
    pl.semaphore_wait(barrier, rest)
    ship_keys(0, 2)
    stage_keys(2, chunks - 2)
    ship_keys(2, chunks - 2)
    arrived(ls_v, ls_sem)

    @pl.loop(0, n_pairs)
    def _(k):
        stage_pair(k)

        @pl.when(k == 1)
        def _():
            forward_keys()

        @pl.when(k > 0)
        def _():
            ship_pair(k - 1)

    ship_pair(n_pairs - 1)

    @pl.loop(0, 2 * n_tiles)
    def _(i):
        dk_a[i] = jnp.zeros((head_dim, 128), F32)
        dv_a[i] = jnp.zeros((head_dim, 128), F32)

    unused = EARLY_SLOTS - 1
    q_t[unused] = jnp.zeros(q_t.shape[1:], BF16)
    do_t[unused] = jnp.zeros(do_t.shape[1:], BF16)
    dq_a[unused] = jnp.zeros(dq_a.shape[1:], F32)
    p_c[...] = jnp.zeros(p_c.shape, BF16)
    d_c[...] = jnp.zeros(d_c.shape, BF16)
    turn[1] = jnp.zeros(turn.shape[1:], BF16)
    aug[...] = jnp.zeros(aug.shape, BF16)
    place = lax.broadcasted_iota(jnp.int32, (head_dim, TILE), 0)
    for a in range(2):
        aug_k[a] = jnp.where((place < 6) & (lax.rem(place, 2) == 1 - a), -1.0, 0.0).astype(BF16)

    for a, land in enumerate((k_b, v_b)):
        arrived(land.at[pl.ds(0, rest * k_rows)], kv_recv.at[a])

    half = pl.ds(0, n_dev // 2)
    quarter = pl.ds(0, n_dev // 4)
    one = pl.ds(0, 1)
    for a in range(2):
        wait_sent(kv_s[a].at[half], kv_s[a].at[quarter], kv_send.at[a])
        arrived(kv_s[a].at[one], kv_d2d.at[a])
        arrived(kv_s[a], kv_mir.at[a])

    @pl.loop(0, n_tiles)
    def _(t):
        for b in range(2):
            rows = pl.ds(pl.multiple_of(t * TILE + b * 128, 128), 128)
            k_t[2 * t + b] = k_b[rows, :].T
            v_t[2 * t + b] = v_b[rows, :].T

    def tile_of(ref, t):
        return jnp.concatenate([ref[2 * t], ref[2 * t + 1]], 1)

    def products(items, old_slot, old_tile, masked=False, last=None):
        n = len(items)
        old = [(p_c[h], d_c[h]) for h in range(group)]
        old_turn = 1
        for w, item in enumerate(items):
            new = [None] * group
            new_turn = 1 if w == n - 1 else 0 if (n - 1 - w) % 2 else 2
            sums = {"V": None, "K": None}
            raw = {"S": [None] * group, "P": [None] * group}
            count = dict.fromkeys("SPVKQ", 0)
            kept = [turn[old_turn, h] for h in range(group)] if new_turn == old_turn else None
            for step in ORDER:
                h = count[step]
                count[step] += 1
                if step in "SP":
                    if item is None:
                        continue
                    j, slot, t = item
                    a = "SP".index(step)
                    rows = jnp.concatenate([qd_b[j, a, h], aug[slot, h]], 1)
                    cols = jnp.concatenate([tile_of((k_t, v_t)[a], t), aug_k[a]], 0)
                    raw[step][h] = dot(rows, cols, 1, 0)
                    if raw["S"][h] is not None and raw["P"][h] is not None:
                        p = jnp.exp2(raw["S"][h] * (scale * LOG2E))
                        if masked and w == n - 1:
                            visible = (lax.broadcasted_iota(jnp.int32, (TILE, TILE), 0)
                                       >= lax.broadcasted_iota(jnp.int32, (TILE, TILE), 1))
                            p = jnp.where(visible, p, 0.0)
                        ds = (p * raw["P"][h]).astype(BF16)
                        new[h] = (p.astype(BF16), ds)
                        turn[new_turn, h] = ds.T
                elif step == "Q":
                    right = turn[old_turn, h] if kept is None else kept[h]
                    dq_a[old_slot, h] += dot(tile_of(k_t, old_tile), right, 1, 0)
                else:
                    lanes = slice(h * TILE, (h + 1) * TILE)
                    left = (do_t if step == "V" else q_t)[old_slot, :, lanes]
                    part = dot(left, old[h]["VK".index(step)], 1, 0)
                    sums[step] = part if sums[step] is None else sums[step] + part
            for acc, total in ((dv_a, sums["V"]), (dk_a, sums["K"])):
                acc[2 * old_tile] += total[:, :128]
                acc[2 * old_tile + 1] += total[:, 128:]
            if item is None:
                return
            old, old_turn, old_slot, old_tile = new, new_turn, slot, t
        for h in range(group):
            p_c[h], d_c[h] = old[h]
        if last is not None:
            last()

    def await_row(i):
        j = row_at(jnp.minimum(i, n_segs - 1))

        @pl.when(i < n_segs)
        def _():
            arrived(qd_b.at[j, :, :, pl.ds(0, rest * q_rows)], row_recv.at[j])

        @pl.when((lax.rem(i, 2) == 0) & (i < n_segs))
        def _():
            pair = lax.div(j, 2)
            arrived(st_b.at[pair, pl.ds(0, rest)], st_recv.at[pair])

    def open_row(j, slot):
        pair, s = lax.div(j, 2), lax.rem(j, 2)
        q_t[slot] = qd_b[j, 0].reshape(group * TILE, head_dim).T
        do_t[slot] = qd_b[j, 1].reshape(group * TILE, head_dim).T
        dq_a[slot] = jnp.zeros((group, head_dim, TILE), F32)
        for b in range(n_dev):
            stats = st_b[pair, b, :, pl.ds(pl.multiple_of(s * 128, 128), 128)]
            hi = stats.astype(BF16).astype(F32)
            mid = (stats - hi).astype(BF16).astype(F32)
            parts = jnp.concatenate([hi, mid, (stats - hi) - mid, jnp.zeros((2, 128), F32)], 0).T.astype(BF16)
            for h in range(group):
                aug[slot, h, b * q_rows:(b + 1) * q_rows, 0:8] = parts[h * q_rows:(h + 1) * q_rows]

    def forward_row(j):
        arrived(mir_q.at[j], dq_mir_recv.at[j])

        def send_all(to):
            for p in to:
                remote(mir_q.at[j, :, rows_of(p)], dq_o.at[j, mate], dq_send, out_recv.at[0], p)

        sent_by_me(send_all)

    def round_row(j, slot):
        for h in range(group):
            qd_b[j, 0, h] = (dq_a[slot, h] * scale).astype(BF16).T

    def close_row(j, before):
        remote(qd_b.at[j, 0], mir_q.at[j], dq_mir, dq_mir_recv.at[j], mate)
        remote(qd_b.at[j, 0, :, rows_of(mate)], dq_o.at[j, me], dq_d2d, out_recv.at[0], mate)
        dq_o[j, me] = qd_b[j, 0, :, rows_of(me)]

        def send_all(to):
            for p in to:
                remote(qd_b.at[j, 0, :, rows_of(p)], dq_o.at[j, me], dq_send, out_recv.at[0], p)

        sent_by_me(send_all)

        @pl.when(before >= 0)
        def _():
            forward_row(before)

    flat_sums = [ref.reshape(2 * n_tiles * 128 // PIECE, PIECE, head_dim) for ref in (dk_a, dv_a)]
    flat_mirs = [ref.reshape(2 * n_tiles * 128 // PIECE, PIECE, head_dim) for ref in (mir_k, mir_v)]
    per_tile = TILE // PIECE

    def ship_tile(t, src_dev, mine):
        def part(p, n):
            owner = lax.div(p, pieces)
            src, dst = pl.ds(p, n), pl.ds(p - owner * pieces, n)
            on_chip = lax.div(owner, 2) == lax.div(me, 2)
            both = (lax.div(owner, inner) != outer_at) & (lax.div(lax.rem(owner, inner), 2) != lax.div(inner_at, 2))
            mine_to_send = jnp.where(both, 1, 0) == core
            for n_out, out in enumerate((dk_o, dv_o)):
                ref = (flat_sums if mine else flat_mirs)[n_out]
                if mine:
                    @pl.when(owner == me)
                    def _():
                        out[dst, src_dev] = ref[src]

                    @pl.when(owner == mate)
                    def _():
                        remote(ref.at[src], out.at[dst, src_dev], dkv_d2d.at[n_out], out_recv.at[1 + n_out], mate)

                @pl.when(jnp.logical_not(on_chip) & mine_to_send)
                def _():
                    remote(ref.at[src], out.at[dst, src_dev], dkv_send.at[n_out], out_recv.at[1 + n_out], owner)

        first = t * per_tile
        whole = lax.div(first, pieces) == lax.div(first + per_tile - 1, pieces)

        @pl.when(whole)
        def _():
            part(first, per_tile)

        @pl.when(jnp.logical_not(whole))
        def _():
            @pl.loop(0, per_tile)
            def _(i):
                part(first + i, 1)

    def close_tiles(lo, n, step, mir):
        @pl.loop(0, n)
        def _(w):
            t = lo + w * step
            for b in range(2):
                dk_a[2 * t + b] = dk_a[2 * t + b].T * scale
                dv_a[2 * t + b] = dv_a[2 * t + b].T
            for a, (src, dst) in enumerate(((dk_a, mir_k), (dv_a, mir_v))):
                remote(src.at[pl.ds(2 * t, 2)], dst.at[pl.ds(2 * t, 2)], dkv_mir.at[a], dkv_mir_recv.at[a, mir], mate)

    n_late = n_tiles - late_tile

    def column(dev, i):
        return lax.rem(dev + i, n_cols)

    def ship_column(dev, i, mine):
        @pl.loop(0, HALF)
        def _(w):
            ship_tile(column(dev, i) + w * n_cols, dev, mine)

    def ship_late(dev, n, mine):
        ship_tile(late_tile + lax.rem(n + dev, n_late), dev, mine)

    def forward_column(i):
        for a, ref in enumerate((mir_k, mir_v)):
            arrived(ref.at[pl.ds(0, 2 * HALF)], dkv_mir_recv.at[a, i])
        ship_column(mate, i, False)

    late_end = middle_row + late
    late_slot = EARLY_SLOTS + late - 1

    def slot_at(i):
        early_index = jnp.where(i < middle_row, i, i - late)
        return jnp.where((i >= middle_row) & (i < late_end), i - middle_row + EARLY_SLOTS,
                         lax.rem(early_index + EARLY_SLOTS, EARLY_SLOTS))

    await_row(0)
    open_row(first_late - 1, 0)

    @pl.loop(0, n_segs)
    def _(i):
        j, slot = row_at(i), slot_at(i)
        before = jnp.where(i == 0, first_late, row_at(jnp.maximum(i - 1, 0)))
        early_before = (before < first_late) | (i == 0)
        old_slot = jnp.where(i == 0, unused, slot_at(i - 1))
        lo = jnp.where(j < first_late, 0, late_tile)
        closes = (i > 0) & early_before
        n = j + 1 - lo

        def tiles(t, n):
            return [(j, slot, t + w) for w in range(n)]

        def after(t):
            return jnp.where(t == lo, old_slot, slot), jnp.where(t == lo, before + 1, t - 1)

        @pl.loop(0, lax.div(n, WIDE))
        def _(c):
            t = lo + c * WIDE
            products(tiles(t, WIDE), *after(t))

        await_row(i + 1)
        coming = jnp.minimum(i + 1, n_segs - 1)
        wide_end = lo + lax.div(n, WIDE) * WIDE
        for r in range(WIDE):
            @pl.when(lax.rem(n, WIDE) == r)
            def _():
                products(tiles(wide_end, r + 1), *after(wide_end), masked=True,
                         last=lambda: open_row(row_at(coming), slot_at(i + 1)))

        @pl.when(closes)
        def _():
            round_row(before, old_slot)
            close_row(before, jnp.where(i > 1, before + 1, -1))

        @pl.when(i == late_end)
        def _():
            close_tiles(late_tile, n_late, 1, n_cols)

        @pl.when(i == late_end + 1)
        def _():
            for a, ref in enumerate((mir_k, mir_v)):
                arrived(ref.at[pl.ds(0, 2 * n_late)], dkv_mir_recv.at[a, n_cols])

        @pl.when(i >= late_end)
        def _():
            turn_of = lax.div(i - late_end, 2)

            @pl.when(lax.rem(i, 2) == 0)
            def _():
                ship_late(me, turn_of, True)

            @pl.when(lax.rem(i, 2) == 1)
            def _():
                ship_late(mate, turn_of, False)

    @pl.loop(0, n_cols)
    def _(i):
        c = column(me, i)

        @pl.loop(0, late // 2)
        def _(pair):
            j = first_late + 2 * pair
            slot = 2 * pair + EARLY_SLOTS
            first = pair == 0
            middle = pair == late // 4
            last_tile = c + (HALF - 1) * n_cols
            products([(j + u, slot + u, c + w * n_cols) for u in range(2) for w in range(HALF)],
                     jnp.where(first, jnp.where(i == 0, slot_at(n_segs - 1), late_slot), slot - 1),
                     jnp.where(first, jnp.where(i == 0, 1, column(me, i + n_cols - 1) + (HALF - 1) * n_cols),
                               last_tile))

            @pl.when(first & (i == 0))
            def _():
                round_row(0, slot_at(n_segs - 1))
                close_row(0, 1)

            @pl.when(first & (i > 0))
            def _():
                close_tiles(column(me, i - 1), HALF, n_cols, i - 1)
                ship_column(me, i - 1, True)

            shipped = (n_segs - late_end) // 2

            @pl.when(first & (i < n_late - shipped))
            def _():
                ship_late(me, shipped + i, True)

            @pl.when(middle & (i > 0))
            def _():
                forward_column(i - 1)

            @pl.when(middle & (i < n_late - shipped))
            def _():
                ship_late(mate, shipped + i, False)

            @pl.when(i == n_cols - 1)
            def _():
                @pl.when(jnp.logical_not(first))
                def _():
                    round_row(j - 1, slot - 1)
                    close_row(j - 1, j - 2)

                round_row(j, slot)
                close_row(j, jnp.where(first, 0, j - 1))

    products([None], late_slot, column(me, n_cols - 1) + (HALF - 1) * n_cols)
    close_tiles(column(me, n_cols - 1), HALF, n_cols, n_cols - 1)
    round_row(n_segs - 1, late_slot)
    close_row(n_segs - 1, n_segs - 2)
    ship_column(me, n_cols - 1, True)
    forward_row(n_segs - 1)
    forward_column(n_cols - 1)

    wait_sent(box.at[0], box.at[0, :, half], pair_send)
    for a in range(2):
        wait_sent(mir_kv.at[a, half], mir_kv.at[a, quarter], kv_fwd.at[a])
    arrived(st_s.at[:, pl.ds(0, rest)], st_send)
    wait_sent(dq_o, dq_o.at[:, half], dq_send)
    arrived(dq_o.at[:, one], dq_d2d)
    arrived(mir_q, dq_mir)
    for a, (out, ref) in enumerate(((dk_o, dk_a), (dv_o, dv_a))):
        wait_sent(out, out.at[:, half], dkv_send.at[a])
        arrived(out.at[:, one], dkv_d2d.at[a])
        arrived(ref, dkv_mir.at[a])
    for n, ref in enumerate((dq_o, dk_o, dv_o)):
        arrived(ref.at[:, pl.ds(0, rest)], out_recv.at[n])


def ungroup_kernel(q_step, k_step, dq_i, dk_i, dv_i, dq_o, dk_o, dv_o, q_out, k_out, v_out, q_done, k_done, v_done):
    groups = ((dq_i, q_out, dq_o, q_step, q_done), (dk_i, k_out, dk_o, k_step, k_done), (dv_i, v_out, dv_o, k_step, v_done))

    for src, turned, dst, step, done in groups:
        rows, width = src.shape[-2], src.shape[-1]

        @pl.loop(0, src.shape[0] // step)
        def _(i):
            for u in range(step):
                at = pl.ds(pl.multiple_of((i * step + u) * rows, rows), rows)
                turned[at] = jnp.transpose(src[i * step + u].reshape(-1, rows, width), (1, 0, 2))
            part = pl.ds(i * step * rows, step * rows)
            pltpu.make_async_copy(turned.at[part], dst.at[part], done.at[i]).start()

    for src, turned, _, step, done in groups:
        rows = src.shape[-2]

        @pl.loop(0, src.shape[0] // step)
        def _(i):
            part = turned.at[pl.ds(i * step * rows, step * rows)]
            pltpu.make_async_copy(part, part, done.at[i]).wait()


def solution(mesh):
    outer, inner = mesh.shape["cp_outer"], mesh.shape["cp"]
    n_dev = outer * inner
    seq_spec = P(None, SEQ_AXES, "heads", None)
    stat_spec = P(None, SEQ_AXES, "heads")
    kv_spec = P(SEQ_AXES, "heads", None)

    def local_grads(q, k, v, o, do, lse):
        n_segs, q_rows, q_heads, head_dim = q.shape
        k_rows, kv_heads, _ = k.shape
        group = q_heads // kv_heads
        late = 8
        n_tiles = n_segs + 1
        n_pairs = n_segs // 2
        pieces = k_rows // PIECE
        keys = n_dev * k_rows

        def flat(x):
            return x.reshape(n_segs * q_rows, q_heads, head_dim)

        dims = (n_dev, inner, n_segs, group, q_rows, head_dim, k_rows, late)
        hbm = pl.BlockSpec(memory_space=pl.ANY)
        vmem = pltpu.VMEM
        key = vmem((keys, head_dim), BF16)
        key_t = vmem((2 * n_tiles, head_dim, 128), BF16)
        row_t = vmem((late + EARLY_SLOTS, head_dim, group * TILE), BF16)
        key_sum = vmem((2 * n_tiles, head_dim, 128), F32)
        stat = vmem((n_pairs, n_dev, 2, 256), F32)
        carried = vmem((group, TILE, TILE), BF16)
        dma = pltpu.SemaphoreType.DMA
        n_cols = (n_segs - late) // HALF
        q_out = vmem((n_segs, kv_heads, group, q_rows, head_dim), BF16)
        kv_out = vmem((pieces, kv_heads, PIECE, head_dim), F32)
        on_chip = pl.BlockSpec(memory_space=pltpu.VMEM)
        sums = jax.ShapeDtypeStruct((2 * n_tiles, 128, head_dim), F32)
        pair = (kv_heads, 2, 2, group, q_rows, head_dim)
        dq, dk, dv = pl.pallas_call(
            functools.partial(attn_kernel, dims),
            out_shape=(q_out, kv_out, kv_out,
                       jax.ShapeDtypeStruct((2, n_pairs) + pair, BF16),
                       jax.ShapeDtypeStruct((2, kv_heads, k_rows, head_dim), BF16),
                       jax.ShapeDtypeStruct((n_segs, group, TILE, head_dim), BF16), sums, sums),
            in_specs=[hbm] * 6,
            out_specs=(on_chip,) * 3 + (hbm,) * 5,
            scratch_shapes=[
                vmem((2, 3, 2 * q_rows, q_heads, head_dim), BF16),
                vmem((2, 2, CHUNK, kv_heads, head_dim), BF16),
                vmem((n_segs, q_heads, q_rows), F32),
                vmem((2,) + pair, BF16),
                vmem((kv_heads, 2, group, q_rows, head_dim), BF16),
                stat, vmem((n_segs, 2, group, TILE, head_dim), BF16), key, key, stat,
                key_t, key_t, row_t, row_t,
                vmem((late + EARLY_SLOTS, group, head_dim, TILE), F32),
                key_sum, key_sum,
                vmem((late + EARLY_SLOTS, group, TILE, head_dim), BF16), vmem((2, head_dim, TILE), BF16),
                carried, carried, vmem((3, group, TILE, TILE), BF16),
                dma((2, 3)), dma((2, 2)), dma, dma((2,)), dma((2,)), dma((n_pairs,)), dma, dma((2,)),
                dma((2,)), dma((2,)), dma((2,)), dma((2,)), dma((2,)), dma, dma, dma, dma, dma((n_segs,)),
                dma((2,)), dma((2,)), dma((2,)), dma((2, n_cols + 1)), dma((n_segs,)), dma((2,)), dma((n_pairs,)),
                dma((3,))],
            compiler_params=pltpu.CompilerParams(
                collective_id=0, has_side_effects=True, vmem_limit_bytes=MAIN_VMEM),
            cost_estimate=pl.CostEstimate(flops=1680 * 5 * 2 * 256 * 256 * 128, bytes_accessed=64 << 20,
                                          transcendentals=1680 * 65536),
            name="attn_grads",
        )(flat(q), flat(do), flat(o), k, v, lse.transpose(0, 2, 1))[:3]

        q_step, k_step = 4, 3
        q_rows_out = jax.ShapeDtypeStruct((n_segs * q_rows, q_heads, head_dim), BF16)
        k_rows_out = jax.ShapeDtypeStruct((k_rows, kv_heads, head_dim), F32)
        q_sems, k_sems = dma((n_segs // q_step,)), dma((pieces // k_step,))
        q_turned, k_turned = vmem(q_rows_out.shape, BF16), vmem(k_rows_out.shape, F32)
        dq, dk, dv = pl.pallas_call(
            functools.partial(ungroup_kernel, q_step, k_step),
            out_shape=(q_rows_out, k_rows_out, k_rows_out),
            in_specs=[on_chip] * 3,
            out_specs=(hbm,) * 3,
            scratch_shapes=[q_turned, k_turned, k_turned, q_sems, k_sems, k_sems],
            compiler_params=pltpu.CompilerParams(vmem_limit_bytes=24 << 20),
            name="ungroup",
        )(dq, dk, dv)
        return dq.reshape(n_segs, q_rows, q_heads, head_dim), dk, dv

    return jax.shard_map(local_grads, mesh=mesh,
                         in_specs=(seq_spec, kv_spec, kv_spec, seq_spec, seq_spec, stat_spec),
                         out_specs=(seq_spec, kv_spec, kv_spec), check_vma=False)
```

```python
import functools

import jax
import jax.numpy as jnp
from jax import lax
from jax.experimental import pallas as pl
from jax.experimental.pallas import tpu as pltpu
from jax.sharding import PartitionSpec as P

MESH = pl.DeviceIdType.MESH
SEQ_AXES = ("cp_outer", "cp")
BF16 = jnp.bfloat16
F32 = jnp.float32
LOG2E = 1.4426950408889634
TILE = 256
WIDE = 8
HALF = 4
EARLY_SLOTS = 3
ORDER = "SVPKSQPVSKPQVKQ"
PIECE = 32
CHUNK = 96
MAIN_VMEM = 49 << 20


def dot(a, b, ca, cb):
    return lax.dot_general(a, b, (((ca,), (cb,)), ((), ())), preferred_element_type=F32)


def attn_kernel(dims, q_n, do_n, o_n, k_n, v_n, ls_n, dq_o, dk_o, dv_o, box, mir_kv, mir_q, mir_k, mir_v,
                nat, nat_k, ls_v, stg, o_s, st_s, qd_b, k_b, v_b, st_b,
                k_t, v_t, q_t, do_t, dq_a, dk_a, dv_a, aug, aug_k, p_c, d_c, turn,
                nat_sem, natk_sem, ls_sem, box_own, box_send, box_recv, pair_send, pair_d2d,
                kv_send, kv_fwd, kv_d2d, kv_mir, kv_mir_recv, st_send, dq_send, dq_d2d, dq_mir, dq_mir_recv,
                dkv_send, dkv_d2d, dkv_mir, dkv_mir_recv, row_recv, kv_recv, st_recv, out_recv):
    n_dev, inner, n_segs, group, q_rows, head_dim, k_rows, late = dims
    scale = head_dim ** -0.5
    outer_at, inner_at = lax.axis_index("cp_outer"), lax.axis_index("cp")
    me = outer_at * inner + inner_at
    core = lax.rem(inner_at, 2)
    mate = me + 1 - 2 * core
    n_pairs = n_segs // 2
    n_tiles = n_segs + 1
    first_late = n_segs - late
    late_tile = first_late
    n_cols = late_tile // HALF
    pieces = k_rows // PIECE
    rest = n_dev - 1
    middle_row = first_late // 2

    kv_s = [ref.reshape(n_dev, k_rows, head_dim) for ref in (k_t, v_t)]

    def chip_cores(flip_outer, flip_inner):
        y = 1 - outer_at if flip_outer else outer_at
        x = (inner - 2) - (inner_at - core) if flip_inner else inner_at - core
        return [y * inner + x + c for c in range(2)]

    along = chip_cores(False, True) + chip_cores(True, False)
    across = chip_cores(True, True)

    along_chips, across_chips = [along[0], along[2]], [across[0]]

    def each_chip(for_mate, act):
        @pl.when(core == (1 if for_mate else 0))
        def _():
            for p in along_chips:
                act(p)

        @pl.when(core == (0 if for_mate else 1))
        def _():
            for p in across_chips:
                act(p)

    def sent_by_me(send_all):
        @pl.when(core == 0)
        def _():
            send_all(along)

        @pl.when(core == 1)
        def _():
            send_all(across)

    def rows_of(p):
        return pl.ds(pl.multiple_of(p * q_rows, q_rows), q_rows)

    def device(p):
        return (0, lax.div(p, inner), lax.rem(p, inner))

    def remote(src, dst, send_sem, recv_sem, p):
        pltpu.make_async_remote_copy(src_ref=src, dst_ref=dst, send_sem=send_sem, recv_sem=recv_sem,
                                     device_id=device(p), device_id_type=MESH).start()

    def arrived(ref, sem):
        pltpu.make_async_copy(ref, ref, sem).wait()

    def wait_sent(whole, half, sem, whole_on=0):
        @pl.when(core == whole_on)
        def _():
            arrived(whole, sem)

        @pl.when(core == 1 - whole_on)
        def _():
            arrived(half, sem)

    def row_at(i):
        return jnp.where(i < middle_row, first_late - 1 - i,
                         jnp.where(i < middle_row + late, first_late - middle_row + i, n_segs - 1 - i))

    def pair_at(k):
        return lax.div(row_at(2 * k), 2)

    def fetch(k):
        r = pair_at(k)
        for a, src in enumerate((q_n, do_n, o_n)):
            pltpu.make_async_copy(src.at[pl.ds(r * 2 * q_rows, 2 * q_rows)], nat.at[lax.rem(k, 2), a],
                                  nat_sem.at[lax.rem(k, 2), a]).start()

    def fetch_keys(c):
        for a, src in enumerate((k_n, v_n)):
            pltpu.make_async_copy(src.at[pl.ds(c * CHUNK, CHUNK)], nat_k.at[lax.rem(c, 2), a],
                                  natk_sem.at[lax.rem(c, 2), a]).start()

    def send_keys(src, owner, lo, n, sem):
        rows = pl.ds(lo, n)
        dst = pl.ds(pl.multiple_of(owner * k_rows + lo, 32), n)

        def send_all(to):
            for p in to:
                for a, land in enumerate((k_b, v_b)):
                    remote(src[a].at[p, rows], land.at[dst], sem.at[a], kv_recv.at[a], p)

        sent_by_me(send_all)

    def stage_keys(first, n):
        @pl.loop(first, first + n)
        def _(c):
            buf = lax.rem(c, 2)
            rows = pl.ds(pl.multiple_of(c * CHUNK, CHUNK), CHUNK)
            dst = pl.ds(pl.multiple_of(me * k_rows + c * CHUNK, 32), CHUNK)
            for a in range(2):
                arrived(nat_k.at[buf, a], natk_sem.at[buf, a])

            @pl.when(c + 1 < k_rows // CHUNK)
            def _():
                fetch_keys(c + 1)

            for a, land in enumerate((k_b, v_b)):
                block = jnp.transpose(nat_k[buf, a], (1, 0, 2))
                kv_s[a][:, rows] = block
                land[dst, :] = kv_s[a][me, rows]

    def ship_keys(first, n):
        lo, rows = first * CHUNK, n * CHUNK
        send_keys(kv_s, me, lo, rows, kv_send)
        src = pl.ds(lo, rows)
        dst = pl.ds(pl.multiple_of(me * k_rows + lo, 32), rows)
        for a, land in enumerate((k_b, v_b)):
            remote(kv_s[a].at[mate, src], land.at[dst], kv_d2d.at[a], kv_recv.at[a], mate)
            each_chip(True, lambda p: remote(kv_s[a].at[pl.ds(p, 2), src], mir_kv.at[a, pl.ds(p, 2), src],
                                             kv_mir.at[a], kv_mir_recv.at[a], mate))

    def forward_keys():
        for a in range(2):
            wait_sent(mir_kv.at[a, pl.ds(0, n_dev // 2)], mir_kv.at[a, pl.ds(0, n_dev // 4)], kv_mir_recv.at[a])
        send_keys([mir_kv.at[a] for a in range(2)], mate, 0, k_rows, kv_fwd)

    def stage_pair(k):
        buf = lax.rem(k, 2)
        r = pair_at(k)
        for a in range(3):
            arrived(nat.at[buf, a], nat_sem.at[buf, a])

        @pl.when(k + 1 < n_pairs)
        def _():
            fetch(k + 1)

        for u in range(4):
            half = slice(16 * (u % 2), 16 * (u % 2) + 16)
            for a in range(3):
                block = jnp.transpose(nat[buf, a, 16 * u:16 * u + 16], (1, 0, 2)).reshape(n_dev, group, 16, head_dim)
                if a < 2:
                    stg[buf, :, u // 2, a, :, half] = block
                else:
                    o_s[:, u // 2, :, half] = block
        for s in range(2):
            qd_b[2 * r + s, :, :, rows_of(me)] = stg[buf, me, s]
        each_chip(True, lambda p: remote(stg.at[buf, pl.ds(p, 2)], box.at[core, k, pl.ds(p, 2)],
                                         box_send.at[buf], box_recv.at[k], mate))
        each_chip(False, lambda p: pltpu.make_async_copy(stg.at[buf, pl.ds(p, 2)], box.at[core, k, pl.ds(p, 2)],
                                                         box_own.at[buf]).start())
        for u in range(2):
            j = row_at(2 * k + u)
            remote(stg.at[buf, mate, lax.rem(j, 2)], qd_b.at[j, :, :, rows_of(me)], pair_d2d.at[buf], row_recv.at[j], mate)

        ones = jnp.ones((8, head_dim), BF16)
        rows = group * q_rows
        blank = jnp.zeros((1, 128 - rows), F32)
        for p in range(n_dev):
            for s in range(2):
                prod = (stg[buf, p, s, 1].reshape(rows, head_dim).astype(F32)
                        * o_s[p, s].reshape(rows, head_dim).astype(F32))
                hi = prod.astype(BF16)
                prod = prod - hi.astype(F32)
                mid = prod.astype(BF16)
                low = (prod - mid.astype(F32)).astype(BF16)
                delta = (dot(ones, hi, 1, 1) + dot(ones, mid, 1, 1)) + dot(ones, low, 1, 1)
                lse = [ls_v[2 * r + s, p * group + h:p * group + h + 1, :] for h in range(group)]
                st_s[r, p, 0:1, 128 * s:128 * s + 128] = jnp.concatenate([delta[0:1], blank], 1)
                st_s[r, p, 1:2, 128 * s:128 * s + 128] = jnp.concatenate(lse + [blank], 1) * (1 / scale)
        st_b[r, me] = st_s[r, me]
        for p in along + across + [mate]:
            remote(st_s.at[r, p], st_b.at[r, me], st_send, st_recv.at[r], p)

    def ship_pair(k):
        buf = lax.rem(k, 2)
        four, two = pl.ds(0, n_dev // 2), pl.ds(0, n_dev // 4)
        wait_sent(stg.at[buf, four], stg.at[buf, two], box_own.at[buf])
        wait_sent(stg.at[buf, four], stg.at[buf, two], box_send.at[buf], 1)
        arrived(stg.at[buf, 0], pair_d2d.at[buf])
        wait_sent(box.at[0, k, four], box.at[0, k, two], box_recv.at[k])

        def send_all(to):
            for u in range(2):
                j = row_at(2 * k + u)
                for src in range(2):
                    for p in to:
                        remote(box.at[src, k, p, lax.rem(j, 2)], qd_b.at[j, :, :, rows_of(me - core + src)],
                               pair_send, row_recv.at[j], p)

        sent_by_me(send_all)

    pltpu.make_async_copy(ls_n, ls_v, ls_sem).start()
    fetch_keys(0)
    fetch(0)
    barrier = pltpu.get_barrier_semaphore()
    for p in along + across + [mate]:
        pl.semaphore_signal(barrier, inc=1, device_id=device(p), device_id_type=MESH)
    chunks = k_rows // CHUNK
    stage_keys(0, 2)
    pl.semaphore_wait(barrier, rest)
    ship_keys(0, 2)
    stage_keys(2, chunks - 2)
    ship_keys(2, chunks - 2)
    arrived(ls_v, ls_sem)

    @pl.loop(0, n_pairs)
    def _(k):
        stage_pair(k)

        @pl.when(k == 1)
        def _():
            forward_keys()

        @pl.when(k > 0)
        def _():
            ship_pair(k - 1)

    ship_pair(n_pairs - 1)

    @pl.loop(0, 2 * n_tiles)
    def _(i):
        dk_a[i] = jnp.zeros((head_dim, 128), F32)
        dv_a[i] = jnp.zeros((head_dim, 128), F32)

    unused = EARLY_SLOTS - 1
    q_t[unused] = jnp.zeros(q_t.shape[1:], BF16)
    do_t[unused] = jnp.zeros(do_t.shape[1:], BF16)
    dq_a[unused] = jnp.zeros(dq_a.shape[1:], F32)
    p_c[...] = jnp.zeros(p_c.shape, BF16)
    d_c[...] = jnp.zeros(d_c.shape, BF16)
    turn[1] = jnp.zeros(turn.shape[1:], BF16)
    aug[...] = jnp.zeros(aug.shape, BF16)
    place = lax.broadcasted_iota(jnp.int32, (head_dim, TILE), 0)
    for a in range(2):
        aug_k[a] = jnp.where((place < 6) & (lax.rem(place, 2) == 1 - a), -1.0, 0.0).astype(BF16)

    for a, land in enumerate((k_b, v_b)):
        arrived(land.at[pl.ds(0, rest * k_rows)], kv_recv.at[a])

    half = pl.ds(0, n_dev // 2)
    quarter = pl.ds(0, n_dev // 4)
    one = pl.ds(0, 1)
    for a in range(2):
        wait_sent(kv_s[a].at[half], kv_s[a].at[quarter], kv_send.at[a])
        arrived(kv_s[a].at[one], kv_d2d.at[a])
        wait_sent(kv_s[a].at[half], kv_s[a].at[quarter], kv_mir.at[a], 1)

    @pl.loop(0, n_tiles)
    def _(t):
        for b in range(2):
            rows = pl.ds(pl.multiple_of(t * TILE + b * 128, 128), 128)
            k_t[2 * t + b] = k_b[rows, :].T
            v_t[2 * t + b] = v_b[rows, :].T

    def tile_of(ref, t):
        return jnp.concatenate([ref[2 * t], ref[2 * t + 1]], 1)

    def products(items, old_slot, old_tile, masked=False, last=None):
        n = len(items)
        old = [(p_c[h], d_c[h]) for h in range(group)]
        old_turn = 1
        for w, item in enumerate(items):
            new = [None] * group
            new_turn = 1 if w == n - 1 else 0 if (n - 1 - w) % 2 else 2
            sums = {"V": None, "K": None}
            raw = {"S": [None] * group, "P": [None] * group}
            count = dict.fromkeys("SPVKQ", 0)
            kept = [turn[old_turn, h] for h in range(group)] if new_turn == old_turn else None
            for step in ORDER:
                h = count[step]
                count[step] += 1
                if step in "SP":
                    if item is None:
                        continue
                    j, slot, t = item
                    a = "SP".index(step)
                    rows = jnp.concatenate([qd_b[j, a, h], aug[slot, h]], 1)
                    cols = jnp.concatenate([tile_of((k_t, v_t)[a], t), aug_k[a]], 0)
                    raw[step][h] = dot(rows, cols, 1, 0)
                    if raw["S"][h] is not None and raw["P"][h] is not None:
                        p = jnp.exp2(raw["S"][h] * (scale * LOG2E))
                        if masked and w == n - 1:
                            visible = (lax.broadcasted_iota(jnp.int32, (TILE, TILE), 0)
                                       >= lax.broadcasted_iota(jnp.int32, (TILE, TILE), 1))
                            p = jnp.where(visible, p, 0.0)
                        ds = (p * raw["P"][h]).astype(BF16)
                        new[h] = (p.astype(BF16), ds)
                        turn[new_turn, h] = ds.T
                elif step == "Q":
                    right = turn[old_turn, h] if kept is None else kept[h]
                    dq_a[old_slot, h] += dot(tile_of(k_t, old_tile), right, 1, 0)
                else:
                    lanes = slice(h * TILE, (h + 1) * TILE)
                    left = (do_t if step == "V" else q_t)[old_slot, :, lanes]
                    part = dot(left, old[h]["VK".index(step)], 1, 0)
                    sums[step] = part if sums[step] is None else sums[step] + part
            for acc, total in ((dv_a, sums["V"]), (dk_a, sums["K"])):
                acc[2 * old_tile] += total[:, :128]
                acc[2 * old_tile + 1] += total[:, 128:]
            if item is None:
                return
            old, old_turn, old_slot, old_tile = new, new_turn, slot, t
        for h in range(group):
            p_c[h], d_c[h] = old[h]
        if last is not None:
            last()

    def await_row(i):
        j = row_at(jnp.minimum(i, n_segs - 1))

        @pl.when(i < n_segs)
        def _():
            arrived(qd_b.at[j, :, :, pl.ds(0, rest * q_rows)], row_recv.at[j])

        @pl.when((lax.rem(i, 2) == 0) & (i < n_segs))
        def _():
            pair = lax.div(j, 2)
            arrived(st_b.at[pair, pl.ds(0, rest)], st_recv.at[pair])

    def open_row(j, slot):
        pair, s = lax.div(j, 2), lax.rem(j, 2)
        q_t[slot] = qd_b[j, 0].reshape(group * TILE, head_dim).T
        do_t[slot] = qd_b[j, 1].reshape(group * TILE, head_dim).T
        dq_a[slot] = jnp.zeros((group, head_dim, TILE), F32)
        for b in range(n_dev):
            stats = st_b[pair, b, :, pl.ds(pl.multiple_of(s * 128, 128), 128)]
            hi = stats.astype(BF16).astype(F32)
            mid = (stats - hi).astype(BF16).astype(F32)
            parts = jnp.concatenate([hi, mid, (stats - hi) - mid, jnp.zeros((2, 128), F32)], 0).T.astype(BF16)
            for h in range(group):
                aug[slot, h, b * q_rows:(b + 1) * q_rows, 0:8] = parts[h * q_rows:(h + 1) * q_rows]

    def forward_row(j):
        wait_sent(mir_q.at[j, :, pl.ds(0, 4 * q_rows)], mir_q.at[j, :, pl.ds(0, 2 * q_rows)], dq_mir_recv.at[j])

        def send_all(to):
            for p in to:
                remote(mir_q.at[j, :, rows_of(p)], dq_o.at[j, mate], dq_send, out_recv.at[0], p)

        sent_by_me(send_all)

    def round_row(j, slot):
        for h in range(group):
            qd_b[j, 0, h] = (dq_a[slot, h] * scale).astype(BF16).T

    def close_row(j, before):
        def hand_over(p):
            rows = pl.ds(pl.multiple_of(p * q_rows, 2 * q_rows), 2 * q_rows)
            remote(qd_b.at[j, 0, :, rows], mir_q.at[j, :, rows], dq_mir, dq_mir_recv.at[j], mate)

        each_chip(True, hand_over)
        remote(qd_b.at[j, 0, :, rows_of(mate)], dq_o.at[j, me], dq_d2d, out_recv.at[0], mate)
        dq_o[j, me] = qd_b[j, 0, :, rows_of(me)]

        def send_all(to):
            for p in to:
                remote(qd_b.at[j, 0, :, rows_of(p)], dq_o.at[j, me], dq_send, out_recv.at[0], p)

        sent_by_me(send_all)

        @pl.when(before >= 0)
        def _():
            forward_row(before)

    flat_sums = [ref.reshape(2 * n_tiles * 128 // PIECE, PIECE, head_dim) for ref in (dk_a, dv_a)]
    flat_mirs = [ref.reshape(2 * n_tiles * 128 // PIECE, PIECE, head_dim) for ref in (mir_k, mir_v)]
    per_tile = TILE // PIECE

    def ship_tile(t, src_dev, mine):
        def part(p, n):
            owner = lax.div(p, pieces)
            src, dst = pl.ds(p, n), pl.ds(p - owner * pieces, n)
            on_chip = lax.div(owner, 2) == lax.div(me, 2)
            both = (lax.div(owner, inner) != outer_at) & (lax.div(lax.rem(owner, inner), 2) != lax.div(inner_at, 2))
            mine_to_send = jnp.where(both, 1, 0) == core
            for n_out, out in enumerate((dk_o, dv_o)):
                ref = (flat_sums if mine else flat_mirs)[n_out]
                if mine:
                    @pl.when(owner == me)
                    def _():
                        out[dst, src_dev] = ref[src]

                    @pl.when(owner == mate)
                    def _():
                        remote(ref.at[src], out.at[dst, src_dev], dkv_d2d.at[n_out], out_recv.at[1 + n_out], mate)

                @pl.when(jnp.logical_not(on_chip) & mine_to_send)
                def _():
                    remote(ref.at[src], out.at[dst, src_dev], dkv_send.at[n_out], out_recv.at[1 + n_out], owner)

        first = t * per_tile
        whole = lax.div(first, pieces) == lax.div(first + per_tile - 1, pieces)

        @pl.when(whole)
        def _():
            part(first, per_tile)

        @pl.when(jnp.logical_not(whole))
        def _():
            @pl.loop(0, per_tile)
            def _(i):
                part(first + i, 1)

    def close_tiles(lo, n, step, mir):
        @pl.loop(0, n)
        def _(w):
            t = lo + w * step
            for b in range(2):
                dk_a[2 * t + b] = dk_a[2 * t + b].T * scale
                dv_a[2 * t + b] = dv_a[2 * t + b].T
            for a, (src, dst) in enumerate(((dk_a, mir_k), (dv_a, mir_v))):
                remote(src.at[pl.ds(2 * t, 2)], dst.at[pl.ds(2 * t, 2)], dkv_mir.at[a], dkv_mir_recv.at[a, mir], mate)

    n_late = n_tiles - late_tile

    def column(dev, i):
        return lax.rem(dev + i, n_cols)

    def ship_column(dev, i, mine):
        @pl.loop(0, HALF)
        def _(w):
            ship_tile(column(dev, i) + w * n_cols, dev, mine)

    def ship_late(dev, n, mine):
        ship_tile(late_tile + lax.rem(n + dev, n_late), dev, mine)

    def forward_column(i):
        for a, ref in enumerate((mir_k, mir_v)):
            arrived(ref.at[pl.ds(0, 2 * HALF)], dkv_mir_recv.at[a, i])
        ship_column(mate, i, False)

    late_end = middle_row + late
    late_slot = EARLY_SLOTS + late - 1

    def slot_at(i):
        early_index = jnp.where(i < middle_row, i, i - late)
        return jnp.where((i >= middle_row) & (i < late_end), i - middle_row + EARLY_SLOTS,
                         lax.rem(early_index + EARLY_SLOTS, EARLY_SLOTS))

    await_row(0)
    open_row(first_late - 1, 0)

    @pl.loop(0, n_segs)
    def _(i):
        j, slot = row_at(i), slot_at(i)
        before = jnp.where(i == 0, first_late, row_at(jnp.maximum(i - 1, 0)))
        early_before = (before < first_late) | (i == 0)
        old_slot = jnp.where(i == 0, unused, slot_at(i - 1))
        lo = jnp.where(j < first_late, 0, late_tile)
        closes = (i > 0) & early_before
        n = j + 1 - lo

        def tiles(t, n):
            return [(j, slot, t + w) for w in range(n)]

        def after(t):
            return jnp.where(t == lo, old_slot, slot), jnp.where(t == lo, before + 1, t - 1)

        @pl.loop(0, lax.div(n, WIDE))
        def _(c):
            t = lo + c * WIDE
            products(tiles(t, WIDE), *after(t))

        await_row(i + 1)
        coming = jnp.minimum(i + 1, n_segs - 1)
        wide_end = lo + lax.div(n, WIDE) * WIDE
        for r in range(WIDE):
            @pl.when(lax.rem(n, WIDE) == r)
            def _():
                products(tiles(wide_end, r + 1), *after(wide_end), masked=True,
                         last=lambda: open_row(row_at(coming), slot_at(i + 1)))

        @pl.when(closes)
        def _():
            round_row(before, old_slot)
            close_row(before, jnp.where(i > 1, before + 1, -1))

        @pl.when(i == late_end)
        def _():
            close_tiles(late_tile, n_late, 1, n_cols)

        @pl.when(i == late_end + 1)
        def _():
            for a, ref in enumerate((mir_k, mir_v)):
                arrived(ref.at[pl.ds(0, 2 * n_late)], dkv_mir_recv.at[a, n_cols])

        @pl.when(i >= late_end)
        def _():
            turn_of = lax.div(i - late_end, 2)

            @pl.when(lax.rem(i, 2) == 0)
            def _():
                ship_late(me, turn_of, True)

            @pl.when(lax.rem(i, 2) == 1)
            def _():
                ship_late(mate, turn_of, False)

    @pl.loop(0, n_cols)
    def _(i):
        c = column(me, i)

        @pl.loop(0, late // 2)
        def _(pair):
            j = first_late + 2 * pair
            slot = 2 * pair + EARLY_SLOTS
            first = pair == 0
            middle = pair == late // 4
            last_tile = c + (HALF - 1) * n_cols
            products([(j + u, slot + u, c + w * n_cols) for u in range(2) for w in range(HALF)],
                     jnp.where(first, jnp.where(i == 0, slot_at(n_segs - 1), late_slot), slot - 1),
                     jnp.where(first, jnp.where(i == 0, 1, column(me, i + n_cols - 1) + (HALF - 1) * n_cols),
                               last_tile))

            @pl.when(first & (i == 0))
            def _():
                round_row(0, slot_at(n_segs - 1))
                close_row(0, 1)

            @pl.when(first & (i > 0))
            def _():
                close_tiles(column(me, i - 1), HALF, n_cols, i - 1)
                ship_column(me, i - 1, True)

            shipped = (n_segs - late_end) // 2

            @pl.when(first & (i < n_late - shipped))
            def _():
                ship_late(me, shipped + i, True)

            @pl.when(middle & (i > 0))
            def _():
                forward_column(i - 1)

            @pl.when(middle & (i < n_late - shipped))
            def _():
                ship_late(mate, shipped + i, False)

            @pl.when(i == n_cols - 1)
            def _():
                @pl.when(jnp.logical_not(first))
                def _():
                    round_row(j - 1, slot - 1)
                    close_row(j - 1, j - 2)

                round_row(j, slot)
                close_row(j, jnp.where(first, 0, j - 1))

    products([None], late_slot, column(me, n_cols - 1) + (HALF - 1) * n_cols)
    close_tiles(column(me, n_cols - 1), HALF, n_cols, n_cols - 1)
    round_row(n_segs - 1, late_slot)
    close_row(n_segs - 1, n_segs - 2)
    ship_column(me, n_cols - 1, True)
    forward_row(n_segs - 1)
    forward_column(n_cols - 1)

    wait_sent(box.at[0], box.at[0, :, half], pair_send)
    for a in range(2):
        wait_sent(mir_kv.at[a, half], mir_kv.at[a, quarter], kv_fwd.at[a])
    arrived(st_s.at[:, pl.ds(0, rest)], st_send)
    wait_sent(dq_o, dq_o.at[:, half], dq_send)
    arrived(dq_o.at[:, one], dq_d2d)
    wait_sent(mir_q.at[:, :, pl.ds(0, 4 * q_rows)], mir_q.at[:, :, pl.ds(0, 2 * q_rows)], dq_mir, 1)
    for a, (out, ref) in enumerate(((dk_o, dk_a), (dv_o, dv_a))):
        wait_sent(out, out.at[:, half], dkv_send.at[a])
        arrived(out.at[:, one], dkv_d2d.at[a])
        arrived(ref, dkv_mir.at[a])
    for n, ref in enumerate((dq_o, dk_o, dv_o)):
        arrived(ref.at[:, pl.ds(0, rest)], out_recv.at[n])


def ungroup_kernel(q_step, k_step, dq_i, dk_i, dv_i, dq_o, dk_o, dv_o, q_out, k_out, v_out, q_done, k_done, v_done):
    groups = ((dq_i, q_out, dq_o, q_step, q_done), (dk_i, k_out, dk_o, k_step, k_done), (dv_i, v_out, dv_o, k_step, v_done))

    for src, turned, dst, step, done in groups:
        rows, width = src.shape[-2], src.shape[-1]

        @pl.loop(0, src.shape[0] // step)
        def _(i):
            for u in range(step):
                at = pl.ds(pl.multiple_of((i * step + u) * rows, rows), rows)
                turned[at] = jnp.transpose(src[i * step + u].reshape(-1, rows, width), (1, 0, 2))
            part = pl.ds(i * step * rows, step * rows)
            pltpu.make_async_copy(turned.at[part], dst.at[part], done.at[i]).start()

    for src, turned, _, step, done in groups:
        rows = src.shape[-2]

        @pl.loop(0, src.shape[0] // step)
        def _(i):
            part = turned.at[pl.ds(i * step * rows, step * rows)]
            pltpu.make_async_copy(part, part, done.at[i]).wait()


def solution(mesh):
    outer, inner = mesh.shape["cp_outer"], mesh.shape["cp"]
    n_dev = outer * inner
    seq_spec = P(None, SEQ_AXES, "heads", None)
    stat_spec = P(None, SEQ_AXES, "heads")
    kv_spec = P(SEQ_AXES, "heads", None)

    def local_grads(q, k, v, o, do, lse):
        n_segs, q_rows, q_heads, head_dim = q.shape
        k_rows, kv_heads, _ = k.shape
        group = q_heads // kv_heads
        late = 8
        n_tiles = n_segs + 1
        n_pairs = n_segs // 2
        pieces = k_rows // PIECE
        keys = n_dev * k_rows

        def flat(x):
            return x.reshape(n_segs * q_rows, q_heads, head_dim)

        dims = (n_dev, inner, n_segs, group, q_rows, head_dim, k_rows, late)
        hbm = pl.BlockSpec(memory_space=pl.ANY)
        vmem = pltpu.VMEM
        key = vmem((keys, head_dim), BF16)
        key_t = vmem((2 * n_tiles, head_dim, 128), BF16)
        row_t = vmem((late + EARLY_SLOTS, head_dim, group * TILE), BF16)
        key_sum = vmem((2 * n_tiles, head_dim, 128), F32)
        stat = vmem((n_pairs, n_dev, 2, 256), F32)
        carried = vmem((group, TILE, TILE), BF16)
        dma = pltpu.SemaphoreType.DMA
        n_cols = (n_segs - late) // HALF
        q_out = vmem((n_segs, kv_heads, group, q_rows, head_dim), BF16)
        kv_out = vmem((pieces, kv_heads, PIECE, head_dim), F32)
        on_chip = pl.BlockSpec(memory_space=pltpu.VMEM)
        sums = jax.ShapeDtypeStruct((2 * n_tiles, 128, head_dim), F32)
        pair = (kv_heads, 2, 2, group, q_rows, head_dim)
        dq, dk, dv = pl.pallas_call(
            functools.partial(attn_kernel, dims),
            out_shape=(q_out, kv_out, kv_out,
                       jax.ShapeDtypeStruct((2, n_pairs) + pair, BF16),
                       jax.ShapeDtypeStruct((2, kv_heads, k_rows, head_dim), BF16),
                       jax.ShapeDtypeStruct((n_segs, group, TILE, head_dim), BF16), sums, sums),
            in_specs=[hbm] * 6,
            out_specs=(on_chip,) * 3 + (hbm,) * 5,
            scratch_shapes=[
                vmem((2, 3, 2 * q_rows, q_heads, head_dim), BF16),
                vmem((2, 2, CHUNK, kv_heads, head_dim), BF16),
                vmem((n_segs, q_heads, q_rows), F32),
                vmem((2,) + pair, BF16),
                vmem((kv_heads, 2, group, q_rows, head_dim), BF16),
                stat, vmem((n_segs, 2, group, TILE, head_dim), BF16), key, key, stat,
                key_t, key_t, row_t, row_t,
                vmem((late + EARLY_SLOTS, group, head_dim, TILE), F32),
                key_sum, key_sum,
                vmem((late + EARLY_SLOTS, group, TILE, head_dim), BF16), vmem((2, head_dim, TILE), BF16),
                carried, carried, vmem((3, group, TILE, TILE), BF16),
                dma((2, 3)), dma((2, 2)), dma, dma((2,)), dma((2,)), dma((n_pairs,)), dma, dma((2,)),
                dma((2,)), dma((2,)), dma((2,)), dma((2,)), dma((2,)), dma, dma, dma, dma, dma((n_segs,)),
                dma((2,)), dma((2,)), dma((2,)), dma((2, n_cols + 1)), dma((n_segs,)), dma((2,)), dma((n_pairs,)),
                dma((3,))],
            compiler_params=pltpu.CompilerParams(
                collective_id=0, has_side_effects=True, vmem_limit_bytes=MAIN_VMEM),
            cost_estimate=pl.CostEstimate(flops=1680 * 5 * 2 * 256 * 256 * 128, bytes_accessed=64 << 20,
                                          transcendentals=1680 * 65536),
            name="attn_grads",
        )(flat(q), flat(do), flat(o), k, v, lse.transpose(0, 2, 1))[:3]

        q_step, k_step = 4, 3
        q_rows_out = jax.ShapeDtypeStruct((n_segs * q_rows, q_heads, head_dim), BF16)
        k_rows_out = jax.ShapeDtypeStruct((k_rows, kv_heads, head_dim), F32)
        q_sems, k_sems = dma((n_segs // q_step,)), dma((pieces // k_step,))
        q_turned, k_turned = vmem(q_rows_out.shape, BF16), vmem(k_rows_out.shape, F32)
        dq, dk, dv = pl.pallas_call(
            functools.partial(ungroup_kernel, q_step, k_step),
            out_shape=(q_rows_out, k_rows_out, k_rows_out),
            in_specs=[on_chip] * 3,
            out_specs=(hbm,) * 3,
            scratch_shapes=[q_turned, k_turned, k_turned, q_sems, k_sems, k_sems],
            compiler_params=pltpu.CompilerParams(vmem_limit_bytes=24 << 20),
            name="ungroup",
        )(dq, dk, dv)
        return dq.reshape(n_segs, q_rows, q_heads, head_dim), dk, dv

    return jax.shard_map(local_grads, mesh=mesh,
                         in_specs=(seq_spec, kv_spec, kv_spec, seq_spec, seq_spec, stat_spec),
                         out_specs=(seq_spec, kv_spec, kv_spec), check_vma=False)
```

```python
import functools

import jax
import jax.numpy as jnp
from jax import lax
from jax.experimental import pallas as pl
from jax.experimental.pallas import tpu as pltpu
from jax.sharding import PartitionSpec as P

MESH = pl.DeviceIdType.MESH
SEQ_AXES = ("cp_outer", "cp")
BF16 = jnp.bfloat16
F32 = jnp.float32
LOG2E = 1.4426950408889634
TILE = 256
WIDE = 8
HALF = 4
EARLY_SLOTS = 3
ORDER = "SVPKSQPVSKPQVKQ"
PIECE = 32
CHUNK = 96
MAIN_VMEM = 49 << 20


def dot(a, b, ca, cb):
    return lax.dot_general(a, b, (((ca,), (cb,)), ((), ())), preferred_element_type=F32)


def attn_kernel(dims, q_n, do_n, o_n, k_n, v_n, ls_n, dq_o, dk_o, dv_o, box, mir_kv, mir_q, mir_k, mir_v,
                nat, nat_k, ls_v, stg, o_s, st_s, qd_b, k_b, v_b, st_b,
                k_t, v_t, q_t, do_t, dq_a, dk_a, dv_a, aug, aug_k, p_c, d_c, turn,
                nat_sem, natk_sem, ls_sem, box_own, box_send, box_recv, pair_send, pair_d2d,
                kv_send, kv_fwd, kv_d2d, kv_mir, kv_mir_recv, st_send, dq_send, dq_d2d, dq_mir, dq_mir_recv,
                dkv_send, dkv_d2d, dkv_mir, dkv_mir_recv, row_recv, kv_recv, st_recv, out_recv):
    n_dev, inner, n_segs, group, q_rows, head_dim, k_rows, late = dims
    scale = head_dim ** -0.5
    outer_at, inner_at = lax.axis_index("cp_outer"), lax.axis_index("cp")
    me = outer_at * inner + inner_at
    core = lax.rem(inner_at, 2)
    mate = me + 1 - 2 * core
    n_pairs = n_segs // 2
    n_tiles = n_segs + 1
    first_late = n_segs - late
    late_tile = first_late
    n_cols = late_tile // HALF
    pieces = k_rows // PIECE
    rest = n_dev - 1
    middle_row = first_late // 2

    kv_s = [ref.reshape(n_dev, k_rows, head_dim) for ref in (k_t, v_t)]

    role = 1 - core

    def chip_cores(flip_outer, flip_inner):
        y = 1 - outer_at if flip_outer else outer_at
        x = (inner - 2) - (inner_at - core) if flip_inner else inner_at - core
        return [y * inner + x + c for c in range(2)]

    along = chip_cores(False, True) + chip_cores(True, False)
    across = chip_cores(True, True)

    along_chips, across_chips = [along[0], along[2]], [across[0]]

    def each_chip(for_mate, act):
        @pl.when(role == (1 if for_mate else 0))
        def _():
            for p in along_chips:
                act(p)

        @pl.when(role == (0 if for_mate else 1))
        def _():
            for p in across_chips:
                act(p)

    def sent_by_me(send_all):
        @pl.when(role == 0)
        def _():
            send_all(along)

        @pl.when(role == 1)
        def _():
            send_all(across)

    def rows_of(p):
        return pl.ds(pl.multiple_of(p * q_rows, q_rows), q_rows)

    def device(p):
        return (0, lax.div(p, inner), lax.rem(p, inner))

    def remote(src, dst, send_sem, recv_sem, p):
        pltpu.make_async_remote_copy(src_ref=src, dst_ref=dst, send_sem=send_sem, recv_sem=recv_sem,
                                     device_id=device(p), device_id_type=MESH).start()

    def arrived(ref, sem):
        pltpu.make_async_copy(ref, ref, sem).wait()

    def wait_sent(whole, half, sem, whole_on=0):
        @pl.when(role == whole_on)
        def _():
            arrived(whole, sem)

        @pl.when(role == 1 - whole_on)
        def _():
            arrived(half, sem)

    def row_at(i):
        return jnp.where(i < middle_row, first_late - 1 - i,
                         jnp.where(i < middle_row + late, first_late - middle_row + i, n_segs - 1 - i))

    def pair_at(k):
        return lax.div(row_at(2 * k), 2)

    def fetch(k):
        r = pair_at(k)
        for a, src in enumerate((q_n, do_n, o_n)):
            pltpu.make_async_copy(src.at[pl.ds(r * 2 * q_rows, 2 * q_rows)], nat.at[lax.rem(k, 2), a],
                                  nat_sem.at[lax.rem(k, 2), a]).start()

    def fetch_keys(c):
        for a, src in enumerate((k_n, v_n)):
            pltpu.make_async_copy(src.at[pl.ds(c * CHUNK, CHUNK)], nat_k.at[lax.rem(c, 2), a],
                                  natk_sem.at[lax.rem(c, 2), a]).start()

    def send_keys(src, owner, lo, n, sem):
        rows = pl.ds(lo, n)
        dst = pl.ds(pl.multiple_of(owner * k_rows + lo, 32), n)

        def send_all(to):
            for p in to:
                for a, land in enumerate((k_b, v_b)):
                    remote(src[a].at[p, rows], land.at[dst], sem.at[a], kv_recv.at[a], p)

        sent_by_me(send_all)

    def stage_keys(first, n):
        @pl.loop(first, first + n)
        def _(c):
            buf = lax.rem(c, 2)
            rows = pl.ds(pl.multiple_of(c * CHUNK, CHUNK), CHUNK)
            dst = pl.ds(pl.multiple_of(me * k_rows + c * CHUNK, 32), CHUNK)
            for a in range(2):
                arrived(nat_k.at[buf, a], natk_sem.at[buf, a])

            @pl.when(c + 1 < k_rows // CHUNK)
            def _():
                fetch_keys(c + 1)

            for a, land in enumerate((k_b, v_b)):
                block = jnp.transpose(nat_k[buf, a], (1, 0, 2))
                kv_s[a][:, rows] = block
                land[dst, :] = kv_s[a][me, rows]

    def ship_keys(first, n):
        lo, rows = first * CHUNK, n * CHUNK
        send_keys(kv_s, me, lo, rows, kv_send)
        src = pl.ds(lo, rows)
        dst = pl.ds(pl.multiple_of(me * k_rows + lo, 32), rows)
        for a, land in enumerate((k_b, v_b)):
            remote(kv_s[a].at[mate, src], land.at[dst], kv_d2d.at[a], kv_recv.at[a], mate)
            each_chip(True, lambda p: remote(kv_s[a].at[pl.ds(p, 2), src], mir_kv.at[a, pl.ds(p, 2), src],
                                             kv_mir.at[a], kv_mir_recv.at[a], mate))

    def forward_keys():
        for a in range(2):
            wait_sent(mir_kv.at[a, pl.ds(0, n_dev // 2)], mir_kv.at[a, pl.ds(0, n_dev // 4)], kv_mir_recv.at[a])
        send_keys([mir_kv.at[a] for a in range(2)], mate, 0, k_rows, kv_fwd)

    def stage_pair(k):
        buf = lax.rem(k, 2)
        r = pair_at(k)
        for a in range(3):
            arrived(nat.at[buf, a], nat_sem.at[buf, a])

        @pl.when(k + 1 < n_pairs)
        def _():
            fetch(k + 1)

        for u in range(4):
            half = slice(16 * (u % 2), 16 * (u % 2) + 16)
            for a in range(3):
                block = jnp.transpose(nat[buf, a, 16 * u:16 * u + 16], (1, 0, 2)).reshape(n_dev, group, 16, head_dim)
                if a < 2:
                    stg[buf, :, u // 2, a, :, half] = block
                else:
                    o_s[:, u // 2, :, half] = block
        for s in range(2):
            qd_b[2 * r + s, :, :, rows_of(me)] = stg[buf, me, s]
        each_chip(True, lambda p: remote(stg.at[buf, pl.ds(p, 2)], box.at[core, k, pl.ds(p, 2)],
                                         box_send.at[buf], box_recv.at[k], mate))
        each_chip(False, lambda p: pltpu.make_async_copy(stg.at[buf, pl.ds(p, 2)], box.at[core, k, pl.ds(p, 2)],
                                                         box_own.at[buf]).start())
        for u in range(2):
            j = row_at(2 * k + u)
            remote(stg.at[buf, mate, lax.rem(j, 2)], qd_b.at[j, :, :, rows_of(me)], pair_d2d.at[buf], row_recv.at[j], mate)

        ones = jnp.ones((8, head_dim), BF16)
        rows = group * q_rows
        blank = jnp.zeros((1, 128 - rows), F32)
        for p in range(n_dev):
            for s in range(2):
                prod = (stg[buf, p, s, 1].reshape(rows, head_dim).astype(F32)
                        * o_s[p, s].reshape(rows, head_dim).astype(F32))
                hi = prod.astype(BF16)
                prod = prod - hi.astype(F32)
                mid = prod.astype(BF16)
                low = (prod - mid.astype(F32)).astype(BF16)
                delta = (dot(ones, hi, 1, 1) + dot(ones, mid, 1, 1)) + dot(ones, low, 1, 1)
                lse = [ls_v[2 * r + s, p * group + h:p * group + h + 1, :] for h in range(group)]
                st_s[r, p, 0:1, 128 * s:128 * s + 128] = jnp.concatenate([delta[0:1], blank], 1)
                st_s[r, p, 1:2, 128 * s:128 * s + 128] = jnp.concatenate(lse + [blank], 1) * (1 / scale)
        st_b[r, me] = st_s[r, me]
        for p in along + across + [mate]:
            remote(st_s.at[r, p], st_b.at[r, me], st_send, st_recv.at[r], p)

    def ship_pair(k):
        buf = lax.rem(k, 2)
        four, two = pl.ds(0, n_dev // 2), pl.ds(0, n_dev // 4)
        wait_sent(stg.at[buf, four], stg.at[buf, two], box_own.at[buf])
        wait_sent(stg.at[buf, four], stg.at[buf, two], box_send.at[buf], 1)
        arrived(stg.at[buf, 0], pair_d2d.at[buf])
        wait_sent(box.at[0, k, four], box.at[0, k, two], box_recv.at[k])

        def send_all(to):
            for u in range(2):
                j = row_at(2 * k + u)
                for src in range(2):
                    for p in to:
                        remote(box.at[src, k, p, lax.rem(j, 2)], qd_b.at[j, :, :, rows_of(me - core + src)],
                               pair_send, row_recv.at[j], p)

        sent_by_me(send_all)

    pltpu.make_async_copy(ls_n, ls_v, ls_sem).start()
    fetch_keys(0)
    fetch(0)
    barrier = pltpu.get_barrier_semaphore()
    for p in along + across + [mate]:
        pl.semaphore_signal(barrier, inc=1, device_id=device(p), device_id_type=MESH)
    chunks = k_rows // CHUNK
    stage_keys(0, 1)
    pl.semaphore_wait(barrier, rest)
    ship_keys(0, 1)
    stage_keys(1, chunks - 1)
    ship_keys(1, chunks - 1)
    arrived(ls_v, ls_sem)

    @pl.loop(0, n_pairs)
    def _(k):
        stage_pair(k)

        @pl.when(k == 1)
        def _():
            forward_keys()

        @pl.when(k > 0)
        def _():
            ship_pair(k - 1)

    ship_pair(n_pairs - 1)

    @pl.loop(0, 2 * n_tiles)
    def _(i):
        dk_a[i] = jnp.zeros((head_dim, 128), F32)
        dv_a[i] = jnp.zeros((head_dim, 128), F32)

    unused = EARLY_SLOTS - 1
    q_t[unused] = jnp.zeros(q_t.shape[1:], BF16)
    do_t[unused] = jnp.zeros(do_t.shape[1:], BF16)
    dq_a[unused] = jnp.zeros(dq_a.shape[1:], F32)
    p_c[...] = jnp.zeros(p_c.shape, BF16)
    d_c[...] = jnp.zeros(d_c.shape, BF16)
    turn[1] = jnp.zeros(turn.shape[1:], BF16)
    aug[...] = jnp.zeros(aug.shape, BF16)
    place = lax.broadcasted_iota(jnp.int32, (head_dim, TILE), 0)
    for a in range(2):
        aug_k[a] = jnp.where((place < 6) & (lax.rem(place, 2) == 1 - a), -1.0, 0.0).astype(BF16)

    for a, land in enumerate((k_b, v_b)):
        arrived(land.at[pl.ds(0, rest * k_rows)], kv_recv.at[a])

    half = pl.ds(0, n_dev // 2)
    quarter = pl.ds(0, n_dev // 4)
    one = pl.ds(0, 1)
    for a in range(2):
        wait_sent(kv_s[a].at[half], kv_s[a].at[quarter], kv_send.at[a])
        arrived(kv_s[a].at[one], kv_d2d.at[a])
        wait_sent(kv_s[a].at[half], kv_s[a].at[quarter], kv_mir.at[a], 1)

    @pl.loop(0, n_tiles)
    def _(t):
        for b in range(2):
            rows = pl.ds(pl.multiple_of(t * TILE + b * 128, 128), 128)
            k_t[2 * t + b] = k_b[rows, :].T
            v_t[2 * t + b] = v_b[rows, :].T

    def tile_of(ref, t):
        return jnp.concatenate([ref[2 * t], ref[2 * t + 1]], 1)

    def products(items, old_slot, old_tile, masked=False, last=None):
        n = len(items)
        old = [(p_c[h], d_c[h]) for h in range(group)]
        old_turn = 1
        for w, item in enumerate(items):
            new = [None] * group
            new_turn = 1 if w == n - 1 else 0 if (n - 1 - w) % 2 else 2
            sums = {"V": None, "K": None}
            raw = {"S": [None] * group, "P": [None] * group}
            count = dict.fromkeys("SPVKQ", 0)
            kept = [turn[old_turn, h] for h in range(group)] if new_turn == old_turn else None
            for step in ORDER:
                h = count[step]
                count[step] += 1
                if step in "SP":
                    if item is None:
                        continue
                    j, slot, t = item
                    a = "SP".index(step)
                    rows = jnp.concatenate([qd_b[j, a, h], aug[slot, h]], 1)
                    cols = jnp.concatenate([tile_of((k_t, v_t)[a], t), aug_k[a]], 0)
                    raw[step][h] = dot(rows, cols, 1, 0)
                    if raw["S"][h] is not None and raw["P"][h] is not None:
                        p = jnp.exp2(raw["S"][h] * (scale * LOG2E))
                        if masked and w == n - 1:
                            visible = (lax.broadcasted_iota(jnp.int32, (TILE, TILE), 0)
                                       >= lax.broadcasted_iota(jnp.int32, (TILE, TILE), 1))
                            p = jnp.where(visible, p, 0.0)
                        ds = (p * raw["P"][h]).astype(BF16)
                        new[h] = (p.astype(BF16), ds)
                        turn[new_turn, h] = ds.T
                elif step == "Q":
                    right = turn[old_turn, h] if kept is None else kept[h]
                    dq_a[old_slot, h] += dot(tile_of(k_t, old_tile), right, 1, 0)
                else:
                    lanes = slice(h * TILE, (h + 1) * TILE)
                    left = (do_t if step == "V" else q_t)[old_slot, :, lanes]
                    part = dot(left, old[h]["VK".index(step)], 1, 0)
                    sums[step] = part if sums[step] is None else sums[step] + part
            for acc, total in ((dv_a, sums["V"]), (dk_a, sums["K"])):
                acc[2 * old_tile] += total[:, :128]
                acc[2 * old_tile + 1] += total[:, 128:]
            if item is None:
                return
            old, old_turn, old_slot, old_tile = new, new_turn, slot, t
        for h in range(group):
            p_c[h], d_c[h] = old[h]
        if last is not None:
            last()

    def await_row(i):
        j = row_at(jnp.minimum(i, n_segs - 1))

        @pl.when(i < n_segs)
        def _():
            arrived(qd_b.at[j, :, :, pl.ds(0, rest * q_rows)], row_recv.at[j])

        @pl.when((lax.rem(i, 2) == 0) & (i < n_segs))
        def _():
            pair = lax.div(j, 2)
            arrived(st_b.at[pair, pl.ds(0, rest)], st_recv.at[pair])

    def open_row(j, slot):
        pair, s = lax.div(j, 2), lax.rem(j, 2)
        q_t[slot] = qd_b[j, 0].reshape(group * TILE, head_dim).T
        do_t[slot] = qd_b[j, 1].reshape(group * TILE, head_dim).T
        dq_a[slot] = jnp.zeros((group, head_dim, TILE), F32)
        for b in range(n_dev):
            stats = st_b[pair, b, :, pl.ds(pl.multiple_of(s * 128, 128), 128)]
            hi = stats.astype(BF16).astype(F32)
            mid = (stats - hi).astype(BF16).astype(F32)
            parts = jnp.concatenate([hi, mid, (stats - hi) - mid, jnp.zeros((2, 128), F32)], 0).T.astype(BF16)
            for h in range(group):
                aug[slot, h, b * q_rows:(b + 1) * q_rows, 0:8] = parts[h * q_rows:(h + 1) * q_rows]

    def forward_row(j):
        wait_sent(mir_q.at[j, :, pl.ds(0, 4 * q_rows)], mir_q.at[j, :, pl.ds(0, 2 * q_rows)], dq_mir_recv.at[j])

        def send_all(to):
            for p in to:
                remote(mir_q.at[j, :, rows_of(p)], dq_o.at[j, mate], dq_send, out_recv.at[0], p)

        sent_by_me(send_all)

    def round_row(j, slot):
        for h in range(group):
            qd_b[j, 0, h] = (dq_a[slot, h] * scale).astype(BF16).T

    def close_row(j, before):
        def hand_over(p):
            rows = pl.ds(pl.multiple_of(p * q_rows, 2 * q_rows), 2 * q_rows)
            remote(qd_b.at[j, 0, :, rows], mir_q.at[j, :, rows], dq_mir, dq_mir_recv.at[j], mate)

        each_chip(True, hand_over)
        remote(qd_b.at[j, 0, :, rows_of(mate)], dq_o.at[j, me], dq_d2d, out_recv.at[0], mate)
        dq_o[j, me] = qd_b[j, 0, :, rows_of(me)]

        def send_all(to):
            for p in to:
                remote(qd_b.at[j, 0, :, rows_of(p)], dq_o.at[j, me], dq_send, out_recv.at[0], p)

        sent_by_me(send_all)

        @pl.when(before >= 0)
        def _():
            forward_row(before)

    flat_sums = [ref.reshape(2 * n_tiles * 128 // PIECE, PIECE, head_dim) for ref in (dk_a, dv_a)]
    flat_mirs = [ref.reshape(2 * n_tiles * 128 // PIECE, PIECE, head_dim) for ref in (mir_k, mir_v)]
    per_tile = TILE // PIECE

    def ship_tile(t, src_dev, mine):
        def part(p, n):
            owner = lax.div(p, pieces)
            src, dst = pl.ds(p, n), pl.ds(p - owner * pieces, n)
            on_chip = lax.div(owner, 2) == lax.div(me, 2)
            both = (lax.div(owner, inner) != outer_at) & (lax.div(lax.rem(owner, inner), 2) != lax.div(inner_at, 2))
            mine_to_send = jnp.where(both, 1, 0) == role
            for n_out, out in enumerate((dk_o, dv_o)):
                ref = (flat_sums if mine else flat_mirs)[n_out]
                if mine:
                    @pl.when(owner == me)
                    def _():
                        out[dst, src_dev] = ref[src]

                    @pl.when(owner == mate)
                    def _():
                        remote(ref.at[src], out.at[dst, src_dev], dkv_d2d.at[n_out], out_recv.at[1 + n_out], mate)

                @pl.when(jnp.logical_not(on_chip) & mine_to_send)
                def _():
                    remote(ref.at[src], out.at[dst, src_dev], dkv_send.at[n_out], out_recv.at[1 + n_out], owner)

        first = t * per_tile
        whole = lax.div(first, pieces) == lax.div(first + per_tile - 1, pieces)

        @pl.when(whole)
        def _():
            part(first, per_tile)

        @pl.when(jnp.logical_not(whole))
        def _():
            @pl.loop(0, per_tile)
            def _(i):
                part(first + i, 1)

    def close_tiles(lo, n, step, mir):
        @pl.loop(0, n)
        def _(w):
            t = lo + w * step
            for b in range(2):
                dk_a[2 * t + b] = dk_a[2 * t + b].T * scale
                dv_a[2 * t + b] = dv_a[2 * t + b].T
            for a, (src, dst) in enumerate(((dk_a, mir_k), (dv_a, mir_v))):
                remote(src.at[pl.ds(2 * t, 2)], dst.at[pl.ds(2 * t, 2)], dkv_mir.at[a], dkv_mir_recv.at[a, mir], mate)

    n_late = n_tiles - late_tile

    def column(dev, i):
        return lax.rem(dev + i, n_cols)

    def ship_column(dev, i, mine):
        @pl.loop(0, HALF)
        def _(w):
            ship_tile(column(dev, i) + w * n_cols, dev, mine)

    def ship_late(dev, n, mine):
        ship_tile(late_tile + lax.rem(n + dev, n_late), dev, mine)

    def forward_column(i):
        for a, ref in enumerate((mir_k, mir_v)):
            arrived(ref.at[pl.ds(0, 2 * HALF)], dkv_mir_recv.at[a, i])
        ship_column(mate, i, False)

    late_end = middle_row + late
    late_slot = EARLY_SLOTS + late - 1

    def slot_at(i):
        early_index = jnp.where(i < middle_row, i, i - late)
        return jnp.where((i >= middle_row) & (i < late_end), i - middle_row + EARLY_SLOTS,
                         lax.rem(early_index + EARLY_SLOTS, EARLY_SLOTS))

    await_row(0)
    open_row(first_late - 1, 0)

    @pl.loop(0, n_segs)
    def _(i):
        j, slot = row_at(i), slot_at(i)
        before = jnp.where(i == 0, first_late, row_at(jnp.maximum(i - 1, 0)))
        early_before = (before < first_late) | (i == 0)
        old_slot = jnp.where(i == 0, unused, slot_at(i - 1))
        lo = jnp.where(j < first_late, 0, late_tile)
        closes = (i > 0) & early_before
        n = j + 1 - lo

        def tiles(t, n):
            return [(j, slot, t + w) for w in range(n)]

        def after(t):
            return jnp.where(t == lo, old_slot, slot), jnp.where(t == lo, before + 1, t - 1)

        @pl.loop(0, lax.div(n, WIDE))
        def _(c):
            t = lo + c * WIDE
            products(tiles(t, WIDE), *after(t))

        await_row(i + 1)
        coming = jnp.minimum(i + 1, n_segs - 1)
        wide_end = lo + lax.div(n, WIDE) * WIDE
        for r in range(WIDE):
            @pl.when(lax.rem(n, WIDE) == r)
            def _():
                products(tiles(wide_end, r + 1), *after(wide_end), masked=True,
                         last=lambda: open_row(row_at(coming), slot_at(i + 1)))

        @pl.when(closes)
        def _():
            round_row(before, old_slot)
            close_row(before, jnp.where(i > 1, before + 1, -1))

        @pl.when(i == late_end)
        def _():
            close_tiles(late_tile, n_late, 1, n_cols)

        @pl.when(i == late_end + 1)
        def _():
            for a, ref in enumerate((mir_k, mir_v)):
                arrived(ref.at[pl.ds(0, 2 * n_late)], dkv_mir_recv.at[a, n_cols])

        @pl.when(i >= late_end)
        def _():
            turn_of = lax.div(i - late_end, 2)

            @pl.when(lax.rem(i, 2) == 0)
            def _():
                ship_late(me, turn_of, True)

            @pl.when(lax.rem(i, 2) == 1)
            def _():
                ship_late(mate, turn_of, False)

    @pl.loop(0, n_cols)
    def _(i):
        c = column(me, i)

        @pl.loop(0, late // 2)
        def _(pair):
            j = first_late + 2 * pair
            slot = 2 * pair + EARLY_SLOTS
            first = pair == 0
            middle = pair == late // 4
            last_tile = c + (HALF - 1) * n_cols
            products([(j + u, slot + u, c + w * n_cols) for u in range(2) for w in range(HALF)],
                     jnp.where(first, jnp.where(i == 0, slot_at(n_segs - 1), late_slot), slot - 1),
                     jnp.where(first, jnp.where(i == 0, 1, column(me, i + n_cols - 1) + (HALF - 1) * n_cols),
                               last_tile))

            @pl.when(first & (i == 0))
            def _():
                round_row(0, slot_at(n_segs - 1))
                close_row(0, 1)

            @pl.when(first & (i > 0))
            def _():
                close_tiles(column(me, i - 1), HALF, n_cols, i - 1)
                ship_column(me, i - 1, True)

            shipped = (n_segs - late_end) // 2

            @pl.when(first & (i < n_late - shipped))
            def _():
                ship_late(me, shipped + i, True)

            @pl.when(middle & (i > 0))
            def _():
                forward_column(i - 1)

            @pl.when(middle & (i < n_late - shipped))
            def _():
                ship_late(mate, shipped + i, False)

            @pl.when(i == n_cols - 1)
            def _():
                @pl.when(jnp.logical_not(first))
                def _():
                    round_row(j - 1, slot - 1)
                    close_row(j - 1, j - 2)

                round_row(j, slot)
                close_row(j, jnp.where(first, 0, j - 1))

    products([None], late_slot, column(me, n_cols - 1) + (HALF - 1) * n_cols)
    close_tiles(column(me, n_cols - 1), HALF, n_cols, n_cols - 1)
    round_row(n_segs - 1, late_slot)
    close_row(n_segs - 1, n_segs - 2)
    ship_column(me, n_cols - 1, True)
    forward_row(n_segs - 1)
    forward_column(n_cols - 1)

    wait_sent(box.at[0], box.at[0, :, half], pair_send)
    for a in range(2):
        wait_sent(mir_kv.at[a, half], mir_kv.at[a, quarter], kv_fwd.at[a])
    arrived(st_s.at[:, pl.ds(0, rest)], st_send)
    wait_sent(dq_o, dq_o.at[:, half], dq_send)
    arrived(dq_o.at[:, one], dq_d2d)
    wait_sent(mir_q.at[:, :, pl.ds(0, 4 * q_rows)], mir_q.at[:, :, pl.ds(0, 2 * q_rows)], dq_mir, 1)
    for a, (out, ref) in enumerate(((dk_o, dk_a), (dv_o, dv_a))):
        wait_sent(out, out.at[:, half], dkv_send.at[a])
        arrived(out.at[:, one], dkv_d2d.at[a])
        arrived(ref, dkv_mir.at[a])
    for n, ref in enumerate((dq_o, dk_o, dv_o)):
        arrived(ref.at[:, pl.ds(0, rest)], out_recv.at[n])


def ungroup_kernel(q_step, k_step, dq_i, dk_i, dv_i, dq_o, dk_o, dv_o, q_out, k_out, v_out, q_done, k_done, v_done):
    groups = ((dq_i, q_out, dq_o, q_step, q_done), (dk_i, k_out, dk_o, k_step, k_done), (dv_i, v_out, dv_o, k_step, v_done))

    for src, turned, dst, step, done in groups:
        rows, width = src.shape[-2], src.shape[-1]

        @pl.loop(0, src.shape[0] // step)
        def _(i):
            for u in range(step):
                at = pl.ds(pl.multiple_of((i * step + u) * rows, rows), rows)
                turned[at] = jnp.transpose(src[i * step + u].reshape(-1, rows, width), (1, 0, 2))
            part = pl.ds(i * step * rows, step * rows)
            pltpu.make_async_copy(turned.at[part], dst.at[part], done.at[i]).start()

    for src, turned, _, step, done in groups:
        rows = src.shape[-2]

        @pl.loop(0, src.shape[0] // step)
        def _(i):
            part = turned.at[pl.ds(i * step * rows, step * rows)]
            pltpu.make_async_copy(part, part, done.at[i]).wait()


def solution(mesh):
    outer, inner = mesh.shape["cp_outer"], mesh.shape["cp"]
    n_dev = outer * inner
    seq_spec = P(None, SEQ_AXES, "heads", None)
    stat_spec = P(None, SEQ_AXES, "heads")
    kv_spec = P(SEQ_AXES, "heads", None)

    def local_grads(q, k, v, o, do, lse):
        n_segs, q_rows, q_heads, head_dim = q.shape
        k_rows, kv_heads, _ = k.shape
        group = q_heads // kv_heads
        late = 8
        n_tiles = n_segs + 1
        n_pairs = n_segs // 2
        pieces = k_rows // PIECE
        keys = n_dev * k_rows

        def flat(x):
            return x.reshape(n_segs * q_rows, q_heads, head_dim)

        dims = (n_dev, inner, n_segs, group, q_rows, head_dim, k_rows, late)
        hbm = pl.BlockSpec(memory_space=pl.ANY)
        vmem = pltpu.VMEM
        key = vmem((keys, head_dim), BF16)
        key_t = vmem((2 * n_tiles, head_dim, 128), BF16)
        row_t = vmem((late + EARLY_SLOTS, head_dim, group * TILE), BF16)
        key_sum = vmem((2 * n_tiles, head_dim, 128), F32)
        stat = vmem((n_pairs, n_dev, 2, 256), F32)
        carried = vmem((group, TILE, TILE), BF16)
        dma = pltpu.SemaphoreType.DMA
        n_cols = (n_segs - late) // HALF
        q_out = vmem((n_segs, kv_heads, group, q_rows, head_dim), BF16)
        kv_out = vmem((pieces, kv_heads, PIECE, head_dim), F32)
        on_chip = pl.BlockSpec(memory_space=pltpu.VMEM)
        sums = jax.ShapeDtypeStruct((2 * n_tiles, 128, head_dim), F32)
        pair = (kv_heads, 2, 2, group, q_rows, head_dim)
        dq, dk, dv = pl.pallas_call(
            functools.partial(attn_kernel, dims),
            out_shape=(q_out, kv_out, kv_out,
                       jax.ShapeDtypeStruct((2, n_pairs) + pair, BF16),
                       jax.ShapeDtypeStruct((2, kv_heads, k_rows, head_dim), BF16),
                       jax.ShapeDtypeStruct((n_segs, group, TILE, head_dim), BF16), sums, sums),
            in_specs=[hbm] * 6,
            out_specs=(on_chip,) * 3 + (hbm,) * 5,
            scratch_shapes=[
                vmem((2, 3, 2 * q_rows, q_heads, head_dim), BF16),
                vmem((2, 2, CHUNK, kv_heads, head_dim), BF16),
                vmem((n_segs, q_heads, q_rows), F32),
                vmem((2,) + pair, BF16),
                vmem((kv_heads, 2, group, q_rows, head_dim), BF16),
                stat, vmem((n_segs, 2, group, TILE, head_dim), BF16), key, key, stat,
                key_t, key_t, row_t, row_t,
                vmem((late + EARLY_SLOTS, group, head_dim, TILE), F32),
                key_sum, key_sum,
                vmem((late + EARLY_SLOTS, group, TILE, head_dim), BF16), vmem((2, head_dim, TILE), BF16),
                carried, carried, vmem((3, group, TILE, TILE), BF16),
                dma((2, 3)), dma((2, 2)), dma, dma((2,)), dma((2,)), dma((n_pairs,)), dma, dma((2,)),
                dma((2,)), dma((2,)), dma((2,)), dma((2,)), dma((2,)), dma, dma, dma, dma, dma((n_segs,)),
                dma((2,)), dma((2,)), dma((2,)), dma((2, n_cols + 1)), dma((n_segs,)), dma((2,)), dma((n_pairs,)),
                dma((3,))],
            compiler_params=pltpu.CompilerParams(
                collective_id=0, has_side_effects=True, vmem_limit_bytes=MAIN_VMEM),
            cost_estimate=pl.CostEstimate(flops=1680 * 5 * 2 * 256 * 256 * 128, bytes_accessed=64 << 20,
                                          transcendentals=1680 * 65536),
            name="attn_grads",
        )(flat(q), flat(do), flat(o), k, v, lse.transpose(0, 2, 1))[:3]

        q_step, k_step = 4, 3
        q_rows_out = jax.ShapeDtypeStruct((n_segs * q_rows, q_heads, head_dim), BF16)
        k_rows_out = jax.ShapeDtypeStruct((k_rows, kv_heads, head_dim), F32)
        q_sems, k_sems = dma((n_segs // q_step,)), dma((pieces // k_step,))
        q_turned, k_turned = vmem(q_rows_out.shape, BF16), vmem(k_rows_out.shape, F32)
        dq, dk, dv = pl.pallas_call(
            functools.partial(ungroup_kernel, q_step, k_step),
            out_shape=(q_rows_out, k_rows_out, k_rows_out),
            in_specs=[on_chip] * 3,
            out_specs=(hbm,) * 3,
            scratch_shapes=[q_turned, k_turned, k_turned, q_sems, k_sems, k_sems],
            compiler_params=pltpu.CompilerParams(vmem_limit_bytes=24 << 20),
            name="ungroup",
        )(dq, dk, dv)
        return dq.reshape(n_segs, q_rows, q_heads, head_dim), dk, dv

    return jax.shard_map(local_grads, mesh=mesh,
                         in_specs=(seq_spec, kv_spec, kv_spec, seq_spec, seq_spec, stat_spec),
                         out_specs=(seq_spec, kv_spec, kv_spec), check_vma=False)
```
